32 devices in a mesh: dp: 8 (over z, x), tensor: 4 (over y, core).
Axes of the slice: x: 2, y: 2, z: 4, core: 2. Of those that a mesh axis runs over, the one named last changes fastest.
Arguments:
- tokens: bfloat16 [64, 258, 768], P('dp'), may hold values from -6 to 6
- metadata: int32 [64], P('dp'), may hold values 0 or 1
- cotangent: bfloat16 [64, 258, 768], P('dp'), may hold values from -6 to 6
- w_query: bfloat16 [768, 768], P(None, 'tensor'), may hold values from -0.21875 to 0.21875
- w_key: bfloat16 [768, 768], P(None, 'tensor'), may hold values from -0.21875 to 0.21875
- w_value: bfloat16 [768, 768], P(None, 'tensor'), may hold values from -0.21875 to 0.21875
- w_out: bfloat16 [768, 768], P('tensor'), may hold values from -1.75 to 1.75
- b_query: float32 [768], P('tensor'), may hold values from -1.5 to 1.5
- b_value: float32 [768], P('tensor'), may hold values from -1.5 to 1.5
- b_out: float32 [768], replicated, may hold values from -1.5 to 1.5
- w_up: bfloat16 [768, 3072], P(None, 'tensor'), may hold values from -0.21875 to 0.21875
- b_up: float32 [3072], P('tensor'), may hold values from -1.5 to 1.5
- w_down: bfloat16 [3072, 768], P('tensor'), may hold values from -0.21875 to 0.21875
- b_down: float32 [768], replicated, may hold values from -1.5 to 1.5
- gain_one: float32 [768], replicated, may hold values from 0.25 to 1.75
- shift_one: float32 [768], replicated, may hold values from -1.5 to 1.5
- gain_two: float32 [768], replicated, may hold values from 0.25 to 1.75
- shift_two: float32 [768], replicated, may hold values from -1.5 to 1.5
Outputs:
- layer_out: bfloat16 [64, 258, 768], P('dp')
- grad_tokens: float32 [64, 258, 768], P('dp')
- grad_w_query: float32 [768, 768], P(None, 'tensor')
- grad_w_key: float32 [768, 768], P(None, 'tensor')
- grad_w_value: float32 [768, 768], P(None, 'tensor')
- grad_w_out: float32 [768, 768], P('tensor')
- grad_b_query: float32 [768], P('tensor')
- grad_b_value: float32 [768], P('tensor')
- grad_b_out: float32 [768], replicated
- grad_w_up: float32 [768, 3072], P(None, 'tensor')
- grad_b_up: float32 [3072], P('tensor')
- grad_w_down: float32 [3072, 768], P('tensor')
- grad_b_down: float32 [768], replicated
- grad_gain_one: float32 [768], replicated
- grad_shift_one: float32 [768], replicated
- grad_gain_two: float32 [768], replicated
- grad_shift_two: float32 [768], replicated
The draws below stay inside these ranges and needn't reach their ends.
All inputs are finite; a program needn't handle non-finite values. No bound on the sum of `metadata` on one device may be relied on, other than what follows from the above.
Results may differ from the reference program's by a relative error of at most 0.012.
Values sent between devices are 32-bit elements; how exact they have to be, the bound alone decides.
A program may use at most 192 MiB of HBM per device.

```python
import math
import jax
import jax.numpy as jnp
from jax import lax

D = 768
HEADS = 12
HEAD_DIM = 64
FF = 3072
LENGTH = 258
SAMPLES = 64
N_DP = 8


def plant(values, key, least, largest):
    longest = values.shape.index(max(values.shape))
    spots = []
    for shift in (0, 1):
        where = [jax.random.randint(jax.random.fold_in(key, axis), (), 0, length) for axis, length in enumerate(values.shape)]
        where[longest] = (where[longest] + shift) % values.shape[longest]
        spots.append(tuple(where))
    return values.at[spots[0]].set(least).at[spots[1]].set(largest)


def steps_of(own_key, shape, shards, least, top_value):
    loudness, own = 1.0, jax.random.fold_in(own_key, 6)
    for dim, shards_of in shards:
        steps = jnp.exp(jax.random.uniform(jax.random.fold_in(own, dim), (shards_of,), jnp.float32, least / len(shards), top_value / len(shards)))
        loudness = loudness * jnp.repeat(steps, shape[dim] // shards_of).reshape([-1 if axis == dim else 1 for axis in range(len(shape))])
    return loudness


def scatter_about(key, shape, spread, bound, pieces=(), kind=jnp.bfloat16):
    level = steps_of(key, shape, pieces, -0.22, 0.18) if pieces else 1.0
    entries = jax.random.normal(key, shape, jnp.float32) * spread * level
    return jnp.minimum(jnp.maximum(entries, -bound), bound).astype(kind)


def setup_inputs(seed: int = 0) -> dict:
    seeds = jax.random.split(jax.random.key(seed), 19)
    tokens = scatter_about(seeds[0], (SAMPLES, LENGTH, D), 1.0, 6.0, ((0, 8),))
    metadata = plant((jax.random.randint(seeds[1], (SAMPLES,), 0, 4) < 3).astype(jnp.int32), jax.random.fold_in(seeds[1], 1), 0, 1)
    cotangent = scatter_about(seeds[2], (SAMPLES, LENGTH, D), 1.0, 6.0, ((0, 8),))
    w_query = scatter_about(seeds[3], (D, D), D ** -0.5, 0.21875, ((1, 4),))
    w_key = scatter_about(seeds[4], (D, D), D ** -0.5, 0.21875, ((1, 4),))
    w_value = scatter_about(seeds[5], (D, D), D ** -0.5, 0.21875, ((1, 4),))
    w_out = scatter_about(seeds[6], (D, D), (max(D // 64, 4)) ** -0.5, 1.75, ((0, 4),))
    b_query = scatter_about(seeds[7], (D,), 0.3, 1.5, ((0, 4),), jnp.float32)
    b_value = scatter_about(seeds[8], (D,), 0.3, 1.5, ((0, 4),), jnp.float32)
    b_out = scatter_about(seeds[9], (D,), 0.3, 1.5, (), jnp.float32)
    w_up = scatter_about(seeds[10], (D, FF), D ** -0.5, 0.21875, ((1, 4),))
    b_up = scatter_about(seeds[11], (FF,), 0.3, 1.5, ((0, 4),), jnp.float32)
    w_down = scatter_about(seeds[12], (FF, D), (FF // 4) ** -0.5, 0.21875, ((0, 4),))
    b_down = scatter_about(seeds[13], (D,), 0.3, 1.5, (), jnp.float32)
    gain_one = jnp.clip(1.0 + 0.15 * jax.random.normal(seeds[14], (D,), jnp.float32), 0.25, 1.75)
    shift_one = scatter_about(seeds[15], (D,), 0.3, 1.5, (), jnp.float32)
    gain_two = jnp.clip(1.0 + 0.15 * jax.random.normal(seeds[16], (D,), jnp.float32), 0.25, 1.75)
    shift_two = scatter_about(seeds[17], (D,), 0.3, 1.5, (), jnp.float32)
    return {"tokens": tokens, "metadata": metadata, "cotangent": cotangent, "w_query": w_query, "w_key": w_key, "w_value": w_value, "w_out": w_out, "b_query": b_query, "b_value": b_value, "b_out": b_out, "w_up": w_up, "b_up": b_up, "w_down": w_down, "b_down": b_down, "gain_one": gain_one, "shift_one": shift_one, "gain_two": gain_two, "shift_two": shift_two}


@jax.custom_vjp
def low(v):
    return lax.optimization_barrier(v.astype(jnp.bfloat16)).astype(jnp.float32)

@jax.custom_vjp
def reduced_backward(v):
    return v

def low_keep(v):
    return (low(v), None)

def low_pass(kept, grad):
    return (grad,)

def back_keep(v):
    return (v, None)

def back_low(kept, grad):
    return (low(grad),)
low.defvjp(low_keep, low_pass)
reduced_backward.defvjp(back_keep, back_low)
NORM_EPSILON = 1e-05
MATMUL_ACCURACY = lax.Precision.HIGHEST

def layer_norm(source_tokens, gain, shift):
    average = lax.optimization_barrier(jnp.mean(source_tokens, -1, keepdims=True))
    mean_removed = source_tokens - average
    variance = lax.optimization_barrier(jnp.mean(mean_removed * mean_removed, -1, keepdims=True))
    return mean_removed * lax.rsqrt(variance + NORM_EPSILON) * gain + shift

def project(source_tokens, weight_matrix):
    return jnp.einsum('mao,oq->maq', source_tokens, weight_matrix, precision=MATMUL_ACCURACY)

def block(inputs, weights):
    w_query, w_key, w_value, w_out, b_query, b_value, b_out, w_up, b_up, w_down, b_down, gain_one, shift_one, gain_two, shift_two = weights
    groups = inputs.shape[0]
    length = inputs.shape[1]
    normed = low(layer_norm(inputs, gain_one, shift_one))
    queries = low(reduced_backward(project(normed, w_query) + b_query)).reshape(groups, length, HEADS, HEAD_DIM)
    key_rows = low(reduced_backward(project(normed, w_key))).reshape(groups, length, HEADS, HEAD_DIM)
    values = low(reduced_backward(project(normed, w_value) + b_value)).reshape(groups, length, HEADS, HEAD_DIM)
    score_scale = 1.0 / math.sqrt(HEAD_DIM)
    scores = reduced_backward(jnp.einsum('sqhc,skhc->shqk', queries, key_rows, precision=MATMUL_ACCURACY) * score_scale)
    attn_probs = low(jax.nn.softmax(scores, axis=-1))
    mixture = jnp.einsum('shqk,skhc->sqhc', attn_probs, values, precision=MATMUL_ACCURACY).reshape(groups, length, D)
    mixture = low(reduced_backward(mixture))
    branch = reduced_backward(project(mixture, w_out) + b_out)
    middle = inputs + branch
    normed_two = low(layer_norm(middle, gain_two, shift_two))
    hidden = reduced_backward(project(normed_two, w_up) + b_up)
    active = low(jax.nn.gelu(hidden, approximate=False))
    branch_two = reduced_backward(project(active, w_down) + b_down)
    return middle + branch_two

def reference(tokens, metadata, cotangent, w_query, w_key, w_value, w_out, b_query, b_value, b_out, w_up, b_up, w_down, b_down, gain_one, shift_one, gain_two, shift_two):
    position = jnp.arange(LENGTH)
    keep_mask = jnp.where(position[None, :] == 1, metadata[:, None].astype(jnp.float32), jnp.float32(1.0))
    params = tuple((array.astype(jnp.float32) for array in (w_query, w_key, w_value, w_out, b_query, b_value, b_out, w_up, b_up, w_down, b_down, gain_one, shift_one, gain_two, shift_two)))

    def forward(inputs, weights):
        masked = inputs * keep_mask[:, :, None]
        grouped = masked.reshape(N_DP, SAMPLES // N_DP, LENGTH, D)

        def one_group(group_in):
            return block(group_in, weights)
        result = lax.map(jax.checkpoint(one_group), grouped)
        return result.reshape(SAMPLES, LENGTH, D)
    outputs, pull_back = jax.vjp(forward, tokens.astype(jnp.float32), params)
    grad_in, grads = pull_back(cotangent.astype(jnp.float32))
    return (outputs.astype(jnp.bfloat16), grad_in, grads[0], grads[1], grads[2], grads[3], grads[4], grads[5], grads[6], grads[7], grads[8], grads[9], grads[10], grads[11], grads[12], grads[13], grads[14])
```

```python
import math

import jax
import jax.numpy as jnp
from jax import lax
from jax.experimental import pallas as pl
from jax.experimental.pallas import tpu as pltpu
from jax.sharding import PartitionSpec as P

HEAD_DIM = 64
EPS = 1e-05
MESH = pl.DeviceIdType.MESH
f32 = jnp.float32
bf16 = jnp.bfloat16
VMEM_LIMIT = 61 << 20
TAIL_P = 0.24
TAIL = (
    0.08952743306829739,
    0.15551359433427508,
    -0.15404885518029288,
    0.6255903019940591,
    -0.6460706945688248,
    0.5545739487327468,
    -0.12508572868970558,
)
INV_SQRT_2PI = 1.0 / math.sqrt(2.0 * math.pi)
HALF_LOG2E = -0.5 / math.log(2.0)


def mm(a, b):
    return lax.dot_general(a, b, (((1,), (0,)), ((), ())), preferred_element_type=f32)


def mmt(a, b):
    return lax.dot_general(a, b, (((1,), (1,)), ((), ())), preferred_element_type=f32)


def tmm(a, b):
    return lax.dot_general(a, b, (((0,), (0,)), ((), ())), preferred_element_type=f32)


def loop(n, fn):
    def body(i, carry):
        fn(i)
        return carry

    lax.fori_loop(0, n, body, 0)


def al(i, step):
    return pl.ds(pl.multiple_of(i * step, step), step)


def centred(x):
    d = x.shape[-1]
    mu = jnp.sum(x, -1, keepdims=True) * (1.0 / d)
    xm = x - mu
    var = jnp.sum(xm * xm, -1, keepdims=True) * (1.0 / d)
    r = lax.rsqrt(var + EPS)
    return xm * r, r


def gelu_pair(v):
    d = 1.0 + TAIL_P * jnp.abs(v)
    t = pltpu.reciprocal(d, approx=True)
    t = t * (2.0 - d * t)
    e = jnp.exp2(HALF_LOG2E * (v * v))
    acc = TAIL[6] * t + TAIL[5]
    for k in range(4, -1, -1):
        acc = acc * t + TAIL[k]
    q = (acc * t) * e
    cdf = jnp.where(v < 0, q, 1.0 - q)
    return v * cdf, cdf + (v * e) * INV_SQRT_2PI


def fold8(x):
    return jnp.sum(x.reshape(x.shape[0] // 8, 8, x.shape[1]), 0)


class Dims:
    def __init__(self, tokens, w_up, n_t):
        self.samples, self.length, self.d = tokens.shape
        self.ns = self.samples // 2
        self.r = -(-self.length // 16) * 16
        self.rows = self.ns * self.r
        self.f = w_up.shape[1]
        self.ff = self.f * n_t
        self.n_t = n_t
        self.heads = self.d // HEAD_DIM
        self.pairs = self.heads // 2
        self.hw = self.d // n_t


def masked_input(tok, meta, r0, ch, R):
    x = tok[pl.ds(r0, ch), :].astype(f32)
    samp = (r0 + (ch - 2)) // R
    rows = lax.broadcasted_iota(jnp.int32, (ch, 1), 0) + r0
    keep = jnp.where(rows == samp * R + 1, meta[samp].astype(f32), 1.0)
    return x, keep


CH = 64


def forward_body(dm, y, meta, tok, cot, wqkv, wo, wup, wdn, vec, p_hbm, normed, q8, kk, vv, mixt, n2, gp, mid, lout, dwd, act, pbuf, psem):
    R, D, NS = dm.r, dm.d, dm.ns
    g1, s1, g2, s2 = (vec[i : i + 1, :] for i in range(4))
    bo, bd, bq, bv = (vec[i : i + 1, :] for i in range(4, 8))
    nt = D // 256

    def ln1(i):
        r0 = pl.multiple_of(i * CH, CH)
        x, keep = masked_input(tok, meta, r0, CH, R)
        xh, _ = centred(x * keep)
        normed[pl.ds(r0, CH), :] = (xh * g1 + s1).astype(bf16)

    loop(dm.rows // CH, ln1)

    def qkv(s):
        rs = al(s, R)
        n = normed[rs, :]
        for j in range(nt):
            c = slice(j * 256, j * 256 + 256)
            q8[rs, c] = (mmt(n, wqkv[c, :]) + bq[:, c]).astype(bf16) * jnp.bfloat16(0.125)
            kk[rs, c] = mmt(n, wqkv[D + j * 256 : D + j * 256 + 256, :]).astype(bf16)
            vv[rs, c] = (mmt(n, wqkv[2 * D + j * 256 : 2 * D + j * 256 + 256, :]) + bv[:, c]).astype(bf16)

    loop(NS, qkv)
    lane = lax.broadcasted_iota(jnp.int32, (1, 128), 1)
    masks = (lane < HEAD_DIM, lane >= HEAD_DIM)
    tail = R - 16
    live = lax.broadcasted_iota(jnp.int32, (16, 1), 0) < dm.length - tail

    def p_copy(i):
        slot = lax.rem(i, 2)
        return pltpu.make_async_copy(pbuf.at[slot], p_hbm.at[i], psem.at[slot])

    def attn(i):
        s, p = i // dm.pairs, lax.rem(i, dm.pairs)
        slot = lax.rem(i, 2)
        rs, cs = al(s, R), al(p, 128)

        @pl.when(i >= 2)
        def _():
            p_copy(i - 2).wait()

        q, k, v = q8[rs, cs], kk[rs, cs], vv[rs, cs]
        for h in range(2):
            st = mmt(jnp.where(masks[h], k, jnp.bfloat16(0)), q)
            sa = st[:tail]
            sb = jnp.where(live, st[tail:], -1e30)
            m = jnp.maximum(jnp.max(sa, 0, keepdims=True), jnp.max(sb, 0, keepdims=True))
            ea, eb = jnp.exp(sa - m), jnp.exp(sb - m)
            inv = 1.0 / (jnp.sum(ea, 0, keepdims=True) + jnp.sum(eb, 0, keepdims=True))
            pbuf[slot, h, :tail, :] = (ea * inv).astype(bf16)
            pbuf[slot, h, tail:, :] = (eb * inv).astype(bf16)
            o = tmm(v, pbuf[slot, h])
            hr = pl.ds(pl.multiple_of(p * 128 + h * HEAD_DIM, HEAD_DIM), HEAD_DIM)
            mixt[s, hr, :] = o[h * HEAD_DIM : (h + 1) * HEAD_DIM].astype(bf16)
        p_copy(i).start()

    total = NS * dm.pairs
    loop(total, attn)
    p_copy(total - 2).wait()
    p_copy(total - 1).wait()

    def outp(s):
        rs = al(s, R)
        a = mixt[s]
        for j in range(nt):
            c = slice(j * 256, j * 256 + 256)
            mid[rs, c] = tmm(a, wo[:, c])

    loop(NS, outp)

    def ln2(i):
        r0 = pl.multiple_of(i * CH, CH)
        x, keep = masked_input(tok, meta, r0, CH, R)
        m = x * keep + (mid[pl.ds(r0, CH), :] + bo)
        mid[pl.ds(r0, CH), :] = m
        xh, _ = centred(m)
        n2[pl.ds(r0, CH), :] = (xh * g2 + s2).astype(bf16)

    loop(dm.rows // CH, ln2)
    ft = dm.f // 256

    def mlp(i):
        s, j = i // (dm.ff // 256), lax.rem(i, dm.ff // 256)
        rs = al(s, R)
        sh, cs = j // ft, al(lax.rem(j, ft), 256)
        h = mm(n2[rs, :], wup[sh, :, cs]) + vec[pl.ds(8 + sh, 1), cs]
        a, g = gelu_pair(h)
        act[rs, al(j, 256)] = a.astype(bf16)
        gp[rs, al(j, 256)] = g.astype(bf16)

    loop(NS * (dm.ff // 256), mlp)

    def dwdn(i):
        sh, j = i // ft, lax.rem(i, ft)
        for n in range(nt):
            c = slice(n * 256, n * 256 + 256)
            dwd[sh, al(j, 256), c] = tmm(act[:, al(2 * y * ft + i, 256)], cot[:, c])

    loop(2 * ft, dwdn)

    def mlp2(s):
        rs = al(s, R)
        for j in range(nt):
            c = slice(j * 256, j * 256 + 256)
            lout[rs, c] = mid[rs, c] + (mm(act[rs, :], wdn[:, c]) + bd[:, c])

    loop(NS, mlp2)


def backward_body(dm, y, meta, tok, cot, wqkv, wo, wup, wdn, vec, p_hbm, normed, q8, kk, vv, mixt, n2, gp, mid, gml, gmix, dqt, gn, dwu, dwa, acc, pbuf, psem):
    R, D, NS = dm.r, dm.d, dm.ns
    nt, ft = D // 256, dm.f // 256
    g1, g2 = vec[0:1, :], vec[2:3, :]
    acc[...] = jnp.zeros_like(acc)

    def ghid(i):
        s, j = i // (dm.ff // 256), lax.rem(i, dm.ff // 256)
        rs, cs = al(s, R), al(j, 256)
        ga = mmt(cot[rs, :], wdn[cs, :])
        gp[rs, cs] = (ga * gp[rs, cs].astype(f32)).astype(bf16)

    loop(NS * (dm.ff // 256), ghid)

    def gnorm2(s):
        rs = al(s, R)
        for j in range(nt):
            c = slice(j * 256, j * 256 + 256)
            tot = None
            for sh in range(dm.n_t):
                t = mmt(gp[rs, sh * dm.f : (sh + 1) * dm.f], wup[sh, c, :])
                tot = t if tot is None else tot + t
            gn[rs, c] = tot

    loop(NS, gnorm2)

    def ln2b(i):
        rs = pl.ds(pl.multiple_of(i * CH, CH), CH)
        xh, r = centred(mid[rs, :])
        go = gn[rs, :]
        co = cot[rs, :].astype(f32)
        g = go * g2
        gx = g * xh
        gm = co + r * (g - jnp.sum(g, -1, keepdims=True) * (1.0 / D) - xh * (jnp.sum(gx, -1, keepdims=True) * (1.0 / D)))
        mid[rs, :] = gm
        gl = gm.astype(bf16)
        gml[rs, :] = gl
        acc[0] += fold8(co)
        acc[1] += fold8(gl.astype(f32))
        acc[4] += fold8(go * xh)
        acc[5] += fold8(go)

    loop(dm.rows // CH, ln2b)

    def gmixf(s):
        rs = al(s, R)
        for j in range(nt):
            c = slice(j * 256, j * 256 + 256)
            gmix[rs, c] = mmt(gml[rs, :], wo[c, :]).astype(bf16)

    loop(NS, gmixf)

    def dwup(i):
        sh, j = i // nt, lax.rem(i, nt)
        for n in range(ft):
            dwu[sh, al(j, 256), n * 256 : n * 256 + 256] = tmm(n2[:, al(j, 256)], gp[:, al((2 * y + sh) * ft + n, 256)])

    loop(2 * nt, dwup)
    ones = jnp.ones((8, dm.rows), bf16)
    for sh in range(2):
        acc[6 + sh, :, : dm.f] = mm(ones, gp[:, al(2 * y + sh, dm.f)]) * 0.125
    hw = dm.hw
    own = al(y, 2 * hw)

    def over_samples(fn):
        tot = None
        for s in range(NS):
            t = fn(s)
            tot = t if tot is None else tot + t
        return tot

    for n in range(nt):
        c = slice(n * 256, n * 256 + 256)
        t = over_samples(lambda s: mm(mixt[s, own, :], gml[s * R : s * R + R, c]))
        for sh in range(2):
            dwa[sh, 3 * hw : 4 * hw, c] = t[sh * hw : (sh + 1) * hw]

    lane = lax.broadcasted_iota(jnp.int32, (1, 128), 1)
    masks = (lane < HEAD_DIM, lane >= HEAD_DIM)
    total = NS * dm.pairs

    def p_copy(i):
        slot = lax.rem(i, 2)
        return pltpu.make_async_copy(p_hbm.at[i], pbuf.at[slot], psem.at[slot])

    p_copy(0).start()

    def attn(i):
        s, p = i // dm.pairs, lax.rem(i, dm.pairs)
        slot = lax.rem(i, 2)
        rs, cs = al(s, R), al(p, 128)

        @pl.when(i + 1 < total)
        def _():
            p_copy(i + 1).start()

        p_copy(i).wait()
        q, k, v, do = q8[rs, cs], kk[rs, cs], vv[rs, cs], gmix[rs, cs]
        dv, dk = [], []
        for h in range(2):
            pt = pbuf[slot, h]
            pf = pt.astype(f32)
            dp = mmt(jnp.where(masks[h], v, jnp.bfloat16(0)), do)
            dsum = jnp.sum(pf * dp, 0, keepdims=True)
            ds = (pf * (dp - dsum)).astype(bf16)
            dv.append(mm(pt, do))
            dk.append(mm(ds, q))
            o = tmm(k, ds)
            hr = pl.ds(pl.multiple_of(p * 128 + h * HEAD_DIM, HEAD_DIM), HEAD_DIM)
            dqt[s, hr, :] = (o[h * HEAD_DIM : (h + 1) * HEAD_DIM] * 0.125).astype(bf16)
        kk[rs, cs] = jnp.where(masks[0], dk[0], dk[1]).astype(bf16)
        vv[rs, cs] = jnp.where(masks[0], dv[0], dv[1]).astype(bf16)

    loop(total, attn)

    for n in range(nt):
        c = slice(n * 256, n * 256 + 256)
        t = over_samples(lambda s: mm(dqt[s, own, :], normed[s * R : s * R + R, c]))
        tk = tmm(kk[:, own], normed[:, c])
        tv = tmm(vv[:, own], normed[:, c])
        for sh in range(2):
            h = slice(sh * hw, (sh + 1) * hw)
            dwa[sh, 0:hw, c] = t[h]
            dwa[sh, hw : 2 * hw, c] = tk[h]
            dwa[sh, 2 * hw : 3 * hw, c] = tv[h]
    onesr = jnp.ones((8, R), bf16)
    acc[8, :, 0 : 2 * hw] = over_samples(lambda s: mmt(onesr, dqt[s, own, :])) * 0.125
    acc[9, :, 0 : 2 * hw] = mm(ones, vv[:, own]) * 0.125

    def gnorm1(s):
        rs = al(s, R)
        for j in range(nt):
            c = slice(j * 256, j * 256 + 256)
            gn[rs, c] = tmm(dqt[s], wqkv[0:D, c]) + mm(kk[rs, :], wqkv[D : 2 * D, c]) + mm(vv[rs, :], wqkv[2 * D : 3 * D, c])

    loop(NS, gnorm1)

    def ln1b(i):
        r0 = pl.multiple_of(i * CH, CH)
        rs = pl.ds(r0, CH)
        x, keep = masked_input(tok, meta, r0, CH, R)
        xh, r = centred(x * keep)
        go = gn[rs, :]
        g = go * g1
        gx = g * xh
        gi = r * (g - jnp.sum(g, -1, keepdims=True) * (1.0 / D) - xh * (jnp.sum(gx, -1, keepdims=True) * (1.0 / D)))
        mid[rs, :] = (mid[rs, :] + gi) * keep
        acc[2] += fold8(go * xh)
        acc[3] += fold8(go)

    loop(dm.rows // CH, ln1b)
    tot = jnp.sum(acc[...], 1)
    for sh in range(2):
        dwa[sh, D : D + 6, :] = tot[0:6]
        dwa[sh, D + 6 : D + 7, :] = tot[6 + sh : 7 + sh]
        dwa[sh, D + 7 : D + 8, 0:hw] = tot[8:9, sh * hw : (sh + 1) * hw]
        dwa[sh, D + 7 : D + 8, hw : 2 * hw] = tot[9:10, sh * hw : (sh + 1) * hw]


V = pl.BlockSpec(memory_space=pltpu.VMEM)
ANY = pl.BlockSpec(memory_space=pl.ANY)
SM = pl.BlockSpec(memory_space=pltpu.SMEM)


def forward_call(dm, meta, tok, cot, wqkv, wo, wup, wdn, vec):
    M, D = dm.rows, dm.d
    sds = jax.ShapeDtypeStruct
    total = dm.ns * dm.pairs

    def kern(meta, tok, cot, wqkv, wo, wup, wdn, vec, p_hbm, normed, q8, kk, vv, mixt, n2, gp, mid, lout, dwd, act, pbuf, psem):
        y = lax.axis_index("tensor") // 2
        forward_body(dm, y, meta, tok, cot, wqkv, wo, wup, wdn, vec, p_hbm, normed, q8, kk, vv, mixt, n2, gp, mid, lout, dwd, act, pbuf, psem)

    row = sds((M, D), bf16)
    return pl.pallas_call(
        kern,
        out_shape=[sds((total, 2, dm.r, dm.r), bf16), row, row, row, row, sds((dm.ns, D, dm.r), bf16), row, sds((M, dm.ff), bf16), sds((M, D), f32), sds((M, D), f32), sds((2, dm.f, D), f32)],
        in_specs=[SM] + [V] * 7,
        out_specs=[ANY] + [V] * 10,
        scratch_shapes=[pltpu.VMEM((M, dm.ff), bf16), pltpu.VMEM((2, 2, dm.r, dm.r), bf16), pltpu.SemaphoreType.DMA((2,))],
        compiler_params=pltpu.CompilerParams(vmem_limit_bytes=VMEM_LIMIT),
        name="forward",
    )(meta, tok, cot, wqkv, wo, wup, wdn, vec)


def backward_call(dm, meta, tok, cot, wqkv, wo, wup, wdn, vec, saved):
    M, D = dm.rows, dm.d
    sds = jax.ShapeDtypeStruct
    p_hbm, normed, q8, kk, vv, mixt, n2, gp, mid = saved

    def kern(meta, tok, cot, wqkv, wo, wup, wdn, vec, normed, q8, mixt, n2, p_hbm, kk_h, vv_h, gp_h, mid_h, gtok, dwu, dwa, kk, vv, gp, gml, gmix, dqt, gn, acc, pbuf, psem, lsem):
        y = lax.axis_index("tensor") // 2
        cps = [pltpu.make_async_copy(a, b, lsem.at[i]) for i, (a, b) in enumerate(((gp_h, gp), (kk_h, kk), (vv_h, vv), (mid_h, gtok)))]
        for c in cps:
            c.start()
        for c in cps:
            c.wait()
        backward_body(dm, y, meta, tok, cot, wqkv, wo, wup, wdn, vec, p_hbm, normed, q8, kk, vv, mixt, n2, gp, gtok, gml, gmix, dqt, gn, dwu, dwa, acc, pbuf, psem)

    row = pltpu.VMEM((M, D), bf16)
    return pl.pallas_call(
        kern,
        out_shape=[sds((M, D), f32), sds((2, D, dm.f), f32), sds((2, D + 16, D), f32)],
        in_specs=[SM] + [V] * 11 + [ANY] * 5,
        out_specs=[V] * 3,
        scratch_shapes=[row, row, pltpu.VMEM((M, dm.ff), bf16), row, row, pltpu.VMEM((dm.ns, D, dm.r), bf16), pltpu.VMEM((M, D), f32), pltpu.VMEM((10, 8, D), f32), pltpu.VMEM((2, 2, dm.r, dm.r), bf16), pltpu.SemaphoreType.DMA((2,)), pltpu.SemaphoreType.DMA((4,))],
        compiler_params=pltpu.CompilerParams(vmem_limit_bytes=VMEM_LIMIT),
        name="backward",
    )(meta, tok, cot, wqkv, wo, wup, wdn, vec, normed, q8, mixt, n2, p_hbm, kk, vv, gp, mid)


def shards(tokens, metadata, cotangent, w_query, w_key, w_value, w_out, b_query, b_value, b_out, w_up, b_up, w_down, b_down, gain_one, shift_one, gain_two, shift_two, n_dp, n_t):
    dm = Dims(tokens, w_up, n_t)
    D, hw = dm.d, dm.hw
    core = lax.rem(lax.axis_index("tensor"), 2)
    y = lax.axis_index("tensor") // 2
    mine = core * dm.ns

    def take(a):
        a = lax.dynamic_slice_in_dim(a, mine, dm.ns, 0)
        return jnp.pad(a, ((0, 0), (0, dm.r - dm.length), (0, 0))).reshape(dm.rows, D)

    tok, cot = take(tokens), take(cotangent)
    meta = lax.dynamic_slice_in_dim(metadata, mine, dm.ns, 0)
    bias = jnp.zeros((16, D), f32).at[0, : dm.f].set(b_up).at[1, :hw].set(b_query).at[1, hw : 2 * hw].set(b_value)
    own = jnp.concatenate([w_query.T.astype(f32), w_key.T.astype(f32), w_value.T.astype(f32), w_out.astype(f32), w_up.astype(f32), w_down.astype(f32), bias])
    g = lax.all_gather(own, "tensor")
    wq, wk, wv, wo = (g[:, i * hw : (i + 1) * hw].reshape(D, D).astype(bf16) for i in range(4))
    wqkv = jnp.concatenate([wq, wk, wv])
    wup = g[:, D : 2 * D].astype(bf16)
    wdn = g[:, 2 * D : 3 * D].reshape(dm.ff, D).astype(bf16)
    gb = g[:, 3 * D :]
    vec = jnp.concatenate([jnp.stack([gain_one, shift_one, gain_two, shift_two, b_out, b_down, gb[:, 1, :hw].reshape(D), gb[:, 1, hw : 2 * hw].reshape(D)]), gb[:, 0]])
    *saved, lout, dwd = forward_call(dm, meta, tok, cot, wqkv, wo, wup, wdn, vec)
    gtok, dwu, dwa = backward_call(dm, meta, tok, cot, wqkv, wo, wup, wdn, vec, saved)

    nt2 = n_t // 2
    sib = [[2 * i, 2 * i + 1] for i in range(nt2)]
    out2 = lax.all_gather(jnp.stack([lout, gtok]), "tensor", axis_index_groups=sib)
    lo, gt = (out2[:, i].reshape(dm.samples, dm.r, D)[:, : dm.length] for i in range(2))
    dw = jnp.concatenate([dwd, dwu, dwa], 1)
    dw = lax.psum_scatter(dw, "tensor", axis_index_groups=sib, scatter_dimension=0)
    dw = lax.psum(dw[...], "dp")
    dw = dw.reshape(3 * D + 16, D)
    d_, u_, a_ = dw[:D], dw[D : 2 * D], dw[2 * D :]
    sm = a_[D:]
    return (
        lo.astype(bf16),
        gt,
        a_[0:hw].T,
        a_[hw : 2 * hw].T,
        a_[2 * hw : 3 * hw].T,
        a_[3 * hw : 4 * hw],
        sm[7, :hw],
        sm[7, hw : 2 * hw],
        sm[1],
        u_,
        sm[6],
        d_,
        sm[0],
        sm[2],
        sm[3],
        sm[4],
        sm[5],
    )


def solution(mesh):
    n_dp, n_t = mesh.shape["dp"], mesh.shape["tensor"]
    rows, cols, vec, rep = P("dp", None, None), P(None, "tensor"), P("tensor"), P()
    srow = P("tensor", None)

    def run(*args):
        return shards(*args, n_dp=n_dp, n_t=n_t)

    return jax.shard_map(
        run,
        mesh=mesh,
        in_specs=(rows, P("dp"), rows, cols, cols, cols, srow, vec, vec, rep, cols, vec, srow, rep, rep, rep, rep, rep),
        out_specs=(rows, rows, cols, cols, cols, srow, vec, vec, rep, cols, vec, srow, rep, rep, rep, rep, rep),
        check_vma=False,
    )
```

```python
import math

import jax
import jax.numpy as jnp
from jax import lax
from jax.experimental import pallas as pl
from jax.experimental.pallas import tpu as pltpu
from jax.sharding import PartitionSpec as P

HEAD_DIM = 64
EPS = 1e-05
MESH = pl.DeviceIdType.MESH
f32 = jnp.float32
bf16 = jnp.bfloat16
VMEM_LIMIT = 61 << 20
RING = 8
CH = 64
TAIL_P = 0.24
TAIL = (
    0.08952743306829739,
    0.15551359433427508,
    -0.15404885518029288,
    0.6255903019940591,
    -0.6460706945688248,
    0.5545739487327468,
    -0.12508572868970558,
)
INV_SQRT_2PI = 1.0 / math.sqrt(2.0 * math.pi)
HALF_LOG2E = -0.5 / math.log(2.0)


def mm(a, b):
    return lax.dot_general(a, b, (((1,), (0,)), ((), ())), preferred_element_type=f32)


def mmt(a, b):
    return lax.dot_general(a, b, (((1,), (1,)), ((), ())), preferred_element_type=f32)


def tmm(a, b):
    return lax.dot_general(a, b, (((0,), (0,)), ((), ())), preferred_element_type=f32)


def loop(n, fn):
    def body(i, carry):
        fn(i)
        return carry

    lax.fori_loop(0, n, body, 0)


def al(i, step):
    return pl.ds(pl.multiple_of(i * step, step), step)


def centred(x):
    d = x.shape[-1]
    mu = jnp.sum(x, -1, keepdims=True) * (1.0 / d)
    xm = x - mu
    var = jnp.sum(xm * xm, -1, keepdims=True) * (1.0 / d)
    r = lax.rsqrt(var + EPS)
    return xm * r, r


def gelu_pair(v):
    d = 1.0 + TAIL_P * jnp.abs(v)
    t = pltpu.reciprocal(d, approx=True)
    t = t * (2.0 - d * t)
    e = jnp.exp2(HALF_LOG2E * (v * v))
    acc = TAIL[6] * t + TAIL[5]
    for k in range(4, -1, -1):
        acc = acc * t + TAIL[k]
    q = (acc * t) * e
    cdf = jnp.where(v < 0, q, 1.0 - q)
    return v * cdf, cdf + (v * e) * INV_SQRT_2PI


def fold8(x):
    return jnp.sum(x.reshape(x.shape[0] // 8, 8, x.shape[1]), 0)


class Dims:
    def __init__(self, tokens, w_up, n_t):
        self.samples, self.length, self.d = tokens.shape
        self.ns = self.samples // 2
        self.r = -(-self.length // 16) * 16
        self.rows = self.ns * self.r
        self.f = w_up.shape[1]
        self.ff = self.f * n_t
        self.n_t = n_t
        self.heads = self.d // HEAD_DIM
        self.pairs = self.heads // 2
        self.hw = self.d // n_t


class Links:
    def __init__(self, n_dp):
        self.n_dp = n_dp
        self.dp = lax.axis_index("dp")
        self.t = lax.axis_index("tensor")
        self.y, self.c = self.t // 2, lax.rem(self.t, 2)
        self.z, self.x = self.dp // 2, lax.rem(self.dp, 2)
        self.length = n_dp // 2
        self.sib = (self.dp, 2 * self.y + 1 - self.c)
        self.ypart = (self.dp, 2 * (1 - self.y) + self.c)
        self.t_sib = 2 * self.y + 1 - self.c
        self.t_y = 2 * (1 - self.y) + self.c
        self.t_ysib = 2 * (1 - self.y) + 1 - self.c
        g = lax.rem(self.dp, RING)
        half = RING // 2
        zz, xx = g // 2, lax.rem(g, 2)
        self.pos = jnp.where(xx == 0, zz, RING - 1 - zz)
        base = self.dp - g

        def at(pos):
            pos = lax.rem(pos + RING, RING)
            local = jnp.where(pos < half, 2 * pos, 2 * (RING - 1 - pos) + 1)
            return (base + local, self.t)

        self.step = 1 - 2 * self.c
        self.ahead, self.behind = at(self.pos + self.step), at(self.pos - self.step)

    def piece(self, offset):
        return lax.rem(self.pos + offset * self.step + RING, RING)


def rcopy(src, dst, ssem, rsem, dev):
    return pltpu.make_async_remote_copy(src_ref=src, dst_ref=dst, send_sem=ssem, recv_sem=rsem, device_id=dev, device_id_type=MESH)


def enter(devs):
    bar = pltpu.get_barrier_semaphore()
    for d in devs:
        pl.semaphore_signal(bar, inc=1, device_id=d, device_id_type=MESH)
    pl.semaphore_wait(bar, len(devs))


class Gather:
    def __init__(self, ln, src, out, direct, ssem, rsem):
        self.ln, self.src, self.out, self.direct = ln, src, out, direct
        self.ssem, self.rsem = ssem, rsem
        self.rows = src.shape[0]
        self.piece_rows = (self.rows - direct) // RING

    def at(self, ref, offset):
        return ref.at[pl.ds(pl.multiple_of(self.direct + self.ln.piece(offset) * self.piece_rows, 8), self.piece_rows)]

    def copy(self, src, dst, k, dev):
        return rcopy(src, dst, self.ssem.at[k], self.rsem.at[k], dev)

    def landed(self, view, k):
        rcopy(view, view, self.ssem.at[k], self.rsem.at[k], self.ln.sib).wait_recv()

    def spread_y(self):
        return self.copy(self.at(self.src, 0), self.at(self.out.at[self.ln.t], 0), 0, self.ln.ypart)

    def direct_y(self):
        d = pl.ds(0, self.direct)
        return self.copy(self.src.at[d], self.out.at[self.ln.t].at[d], 1, self.ln.ypart)

    def whole_sib(self):
        return self.copy(self.src, self.out.at[self.ln.t], 2, self.ln.sib)

    def start_y(self):
        self.spread_y().start()
        self.direct_y().start()

    def start_sib(self):
        self.whole_sib().start()

    def wait_sib(self):
        self.landed(self.out.at[self.ln.t_sib], 2)

    def to_sib(self, offset):
        v = self.at(self.out.at[self.ln.t_y], offset)
        return self.copy(v, v, 11 + 4 + offset, self.ln.sib)

    def direct_sib(self):
        v = self.out.at[self.ln.t_y].at[pl.ds(0, self.direct)]
        return self.copy(v, v, 10, self.ln.sib)

    def ring_ahead(self, s):
        v = self.at(self.out.at[self.ln.t_y], -s)
        return self.copy(v, v, 3 + s, self.ln.ahead)

    def ring_behind(self, s):
        v = self.at(self.out.at[self.ln.t_y], s)
        return self.copy(v, v, 7 + s, self.ln.behind)

    def tick(self, i):
        ln, out = self.ln, self.out.at[self.ln.t_y]
        if i == 0:
            self.landed(self.at(out, 0), 0)
            self.ring_ahead(0).start()
            self.ring_behind(0).start()
            self.to_sib(0).start()
            return
        s = i - 1
        self.landed(self.at(out, -s - 1), 3 + s)
        if s < 3:
            self.ring_ahead(s + 1).start()
            self.landed(self.at(out, s + 1), 7 + s)
            if s < 2:
                self.ring_behind(s + 1).start()
        self.to_sib(-s - 1).start()
        if s < 3:
            self.to_sib(s + 1).start()
        if i == 4:
            self.landed(out.at[pl.ds(0, self.direct)], 1)
            self.direct_sib().start()

    def finish(self):
        ln, out = self.ln, self.out.at[self.ln.t_ysib]
        for offset in range(-4, 4):
            v = out.at[pl.ds(pl.multiple_of(self.direct + lax.rem(ln.pos - offset * ln.step + RING, RING) * self.piece_rows, 8), self.piece_rows)]
            self.landed(v, 11 + 4 + offset)
        self.landed(out.at[pl.ds(0, self.direct)], 10)

    def drain(self):
        cps = [self.spread_y(), self.direct_y(), self.whole_sib(), self.direct_sib()]
        cps += [self.ring_ahead(s) for s in range(4)] + [self.ring_behind(s) for s in range(3)]
        cps += [self.to_sib(o) for o in range(-4, 4)]
        for cp in cps:
            cp.wait_send()


GATHER_SEMS = 19


def keep_of(meta, base, s, r0, n):
    rows = lax.broadcasted_iota(jnp.int32, (n, 1), 0) + r0
    return jnp.where(rows == 1, meta[base + s].astype(f32), 1.0)


def row_chunks(dm):
    out, r = [], 0
    while r < dm.r:
        n = min(CH, dm.r - r)
        out.append((r, n))
        r += n
    return out


def forward_kernel(dm, n_dp, *refs):
    (meta, wq, wk, wv, wo_s, wup_s, wdn_s, bias, g1_r, s1_r, g2_r, s2_r, bo_r, tokens, cotan) = refs[:15]
    (ga, gu, n32, p_hbm, o_wqkv, o_wo, o_bias, o_tok, o_cot, o_normed, o_q8, o_kk, o_vv, o_mixt, o_n2, o_act, o_gp, o_mid, d_own, d_sib) = refs[15:35]
    (tok3, cot3, tok, cot, wqkv, wo, wup, normed, q8, kk, vv, mixt, n2, act, gp, mid, dwd, pbuf, tmp, bbuf, bqv) = refs[35:56]
    psem, tsem, lsem, osem, ssa, rsa, ssu, rsu, ssd, rsd = refs[56:]
    R, D, NS, hw, f = dm.r, dm.d, dm.ns, dm.hw, dm.f
    ln = Links(n_dp)
    y, c, t = ln.y, ln.c, ln.t
    base = c * NS

    def row(ref):
        return ref[...].reshape(1, D)

    loads = []
    for s in range(NS):
        loads.append(pltpu.make_async_copy(tokens.at[base + s], tok3.at[s], lsem.at[s]))
    for s in range(NS):
        loads.append(pltpu.make_async_copy(cotan.at[base + s], cot3.at[s], lsem.at[NS + s]))
    for cp in loads:
        cp.start()
    outs = []

    def put(src, dst):
        cp = pltpu.make_async_copy(src, dst, osem.at[len(outs)])
        cp.start()
        outs.append(cp)

    mid[0:16, :] = bias[...]
    bbuf[t] = bias[...]
    for i, w in enumerate((wq, wk, wv)):
        wt = w[...].astype(f32).T
        mid[16 + i * hw : 16 + (i + 1) * hw, :] = wt
        wqkv[pl.ds(pl.multiple_of(i * D + t * hw, 16), hw), :] = wt.astype(bf16)
    mid[16 + 3 * hw : 16 + 4 * hw, :] = wo_s[...].astype(f32)
    wo[al(t, hw), :] = wo_s[...]
    enter((ln.ypart, ln.sib, ln.ahead, ln.behind))
    g_a = Gather(ln, mid.at[pl.ds(0, D + 16)], ga, 16 + D // 3, ssa, rsa)
    g_u = Gather(ln, dwd.at[0], gu, D // 3, ssu, rsu)
    g_a.start_y()
    g_a.start_sib()

    def widen(i):
        rs = al(i, 64)
        dwd[0, rs, :] = wup_s[rs, :].astype(f32)
        dwd[1, rs, :] = wdn_s[rs, :].astype(f32)
        wup[c, rs, :] = wup_s[rs, :]

    loop(f // 64, widen)
    put(dwd.at[1], n32)
    g_u.start_sib()

    for cp in loads:
        cp.wait()
    g1, s1, g2, s2, bo = (row(r) for r in (g1_r, s1_r, g2_r, s2_r, bo_r))
    full = dm.length // 16 * 16

    def pad_rows(s):
        for src, dst in ((tok3, tok), (cot3, cot)):
            for r in range(0, full, 64):
                n = min(64, full - r)
                dst[pl.ds(pl.multiple_of(s * R + r, 16), n), :] = src[s, r : r + n, :]
            last = pl.ds(pl.multiple_of(s * R + full, 16), R - full)
            dst[last, :] = jnp.zeros((R - full, D), bf16)
            if dm.length > full:
                dst[pl.ds(pl.multiple_of(s * R + full, 16), dm.length - full), :] = src[s, full : dm.length, :]

    loop(NS, pad_rows)
    put(tok, o_tok)
    put(cot, o_cot)

    def ln1(s):
        for r, n in row_chunks(dm):
            rs = pl.ds(pl.multiple_of(s * R + r, 16), n)
            x = tok[rs, :].astype(f32)
            if r == 0:
                x = x * keep_of(meta, base, s, r, n)
            xh, _ = centred(x)
            normed[rs, :] = (xh * g1 + s1).astype(bf16)

    loop(NS, ln1)
    put(normed, o_normed)

    def fetch(src, k):
        cp = pltpu.make_async_copy(src, tmp.at[k], tsem.at[k])
        cp.start()
        return cp

    def take_a(tp):
        dsts = [(wqkv, i * D + tp * hw) for i in range(3)] + [(wo, tp * hw)]
        cb = pltpu.make_async_copy(ga.at[tp, pl.ds(0, 16)], bbuf.at[tp], tsem.at[2])
        cb.start()
        cps = [fetch(ga.at[tp, pl.ds(16, hw)], 0)]
        for i, (ref, r0) in enumerate(dsts):
            if i < 3:
                cps.append(fetch(ga.at[tp, pl.ds(16 + (i + 1) * hw, hw)], (i + 1) % 2))
            cps[i].wait()
            ref[pl.ds(pl.multiple_of(r0, 16), hw), :] = tmp[i % 2].astype(bf16)
        cb.wait()

    lane = lax.broadcasted_iota(jnp.int32, (1, 128), 1)
    masks = (lane < HEAD_DIM, lane >= HEAD_DIM)
    hp = dm.pairs // 2
    tail = R - 16
    live = lax.broadcasted_iota(jnp.int32, (16, 1), 0) < dm.length - tail

    def project(hf):
        for i in range(2):
            b = bbuf[2 * hf + i]
            bqv[0:1, i * hw : (i + 1) * hw] = b[1:2, 0:hw]
            bqv[1:2, i * hw : (i + 1) * hw] = b[1:2, hw : 2 * hw]
        cs = al(hf, 2 * hw)

        def one(s):
            rs = al(s, R)
            n = normed[rs, :]
            w = [wqkv[pl.ds(pl.multiple_of(i * D + hf * 2 * hw, 128), 2 * hw), :] for i in range(3)]
            q8[rs, cs] = (mmt(n, w[0]) + bqv[0:1, : 2 * hw]).astype(bf16) * jnp.bfloat16(0.125)
            kk[rs, cs] = mmt(n, w[1]).astype(bf16)
            vv[rs, cs] = (mmt(n, w[2]) + bqv[1:2, : 2 * hw]).astype(bf16)

        loop(NS, one)

    def p_copy(hf, i):
        slot = lax.rem(i, 2)
        return pltpu.make_async_copy(pbuf.at[slot], p_hbm.at[(i // hp) * dm.pairs + hf * hp + lax.rem(i, hp)], psem.at[slot])

    def attend(hf, ticks):
        total = NS * hp

        def one(i):
            s, p = i // hp, hf * hp + lax.rem(i, hp)
            slot = lax.rem(i, 2)
            rs, cs = al(s, R), al(p, 128)
            for k, fn in ticks:
                pl.when(i == k)(fn)

            @pl.when(i >= 2)
            def _():
                p_copy(hf, i - 2).wait()

            q, k, v = q8[rs, cs], kk[rs, cs], vv[rs, cs]
            for h in range(2):
                st = mmt(jnp.where(masks[h], k, jnp.bfloat16(0)), q)
                sa = st[:tail]
                sb = jnp.where(live, st[tail:], -1e30)
                m = jnp.maximum(jnp.max(sa, 0, keepdims=True), jnp.max(sb, 0, keepdims=True))
                ea, eb = jnp.exp(sa - m), jnp.exp(sb - m)
                inv = 1.0 / (jnp.sum(ea, 0, keepdims=True) + jnp.sum(eb, 0, keepdims=True))
                pbuf[slot, h, :tail, :] = (ea * inv).astype(bf16)
                pbuf[slot, h, tail:, :] = (eb * inv).astype(bf16)
                o = tmm(v, pbuf[slot, h])
                hr = pl.ds(pl.multiple_of(p * 128 + h * HEAD_DIM, HEAD_DIM), HEAD_DIM)
                mixt[s, hr, :] = o[h * HEAD_DIM : (h + 1) * HEAD_DIM].astype(bf16)
            p_copy(hf, i).start()

        loop(total, one)
        p_copy(hf, total - 2).wait()
        p_copy(hf, total - 1).wait()

    g_a.wait_sib()
    take_a(ln.t_sib)
    project(y)
    g_a.tick(0)
    attend(y, [(2, lambda: g_a.tick(1)), (10, lambda: g_a.tick(2))])
    g_a.tick(3)
    g_a.tick(4)
    g_u.start_y()
    g_a.finish()
    take_a(ln.t_y)
    take_a(ln.t_ysib)
    put(wqkv, o_wqkv)
    put(wo, o_wo)
    put(bbuf, o_bias)
    project(1 - y)
    put(q8, o_q8)
    put(kk, o_kk)
    put(vv, o_vv)
    g_u.tick(0)
    attend(1 - y, [(2, lambda: g_u.tick(1)), (10, lambda: g_u.tick(2))])
    put(mixt, o_mixt)
    g_a.drain()

    def outp(s):
        rs = al(s, R)
        mid[rs, :] = tmm(mixt[s], wo[...])

    loop(NS, outp)

    def ln2(s):
        for r, n in row_chunks(dm):
            rs = pl.ds(pl.multiple_of(s * R + r, 16), n)
            x = tok[rs, :].astype(f32)
            if r == 0:
                x = x * keep_of(meta, base, s, r, n)
            m = x + (mid[rs, :] + bo)
            mid[rs, :] = m
            xh, _ = centred(m)
            n2[rs, :] = (xh * g2 + s2).astype(bf16)

    loop(NS, ln2)
    put(mid, o_mid)
    put(n2, o_n2)
    g_u.tick(3)
    g_u.wait_sib()
    cps = [fetch(gu.at[ln.t_sib, pl.ds(0, hw)], 0)]
    for i in range(4):
        if i < 3:
            cps.append(fetch(gu.at[ln.t_sib, pl.ds((i + 1) * hw, hw)], (i + 1) % 2))
        cps[i].wait()
        wup[1 - c, i * hw : (i + 1) * hw, :] = tmp[i % 2].astype(bf16)
    ft = f // 256

    def mlp(i):
        s, j = i // (2 * ft), lax.rem(i, 2 * ft)
        rs, sh, cs = al(s, R), j // ft, al(lax.rem(j, ft), 256)
        h = mm(n2[rs, :], wup[sh, :, cs]) + bbuf[2 * y + sh, 0:1, cs]
        a, g = gelu_pair(h)
        act[rs, al(j, 256)] = a.astype(bf16)
        gp[rs, al(j, 256)] = g.astype(bf16)

    loop(NS * 2 * ft, mlp)
    put(act, o_act)
    put(gp, o_gp)
    g_u.tick(4)
    g_u.finish()
    g_u.drain()
    outs[0].wait()

    def dwdn(i):
        sh, j = i // ft, lax.rem(i, ft)
        dwd[sh, al(j, 256), :] = tmm(act[:, al(i, 256)], cot[...])

    loop(2 * ft, dwdn)
    put(dwd.at[c], d_own)
    cp = rcopy(dwd.at[1 - c], d_sib, ssd.at[0], rsd.at[0], ln.sib)
    cp.start()
    cp.wait()
    for cp in outs[1:]:
        cp.wait()


V = pl.BlockSpec(memory_space=pltpu.VMEM)
ANY = pl.BlockSpec(memory_space=pl.ANY)
SM = pl.BlockSpec(memory_space=pltpu.SMEM)


def forward_call(dm, n_dp, small, big):
    M, D, f = dm.rows, dm.d, dm.f
    sds, vm, dma = jax.ShapeDtypeStruct, pltpu.VMEM, pltpu.SemaphoreType.DMA
    row = sds((M, D), bf16)
    wide = sds((M, 2 * f), bf16)
    sq = sds((D, f), f32)
    outs = [sds((dm.n_t, D + 16, D), f32), sds((dm.n_t, D, f), f32), sds((f, D), f32), sds((dm.ns * dm.pairs, 2, dm.r, dm.r), bf16), sds((3 * D, D), bf16), sds((D, D), bf16), sds((dm.n_t, 16, D), f32)]
    outs += [row] * 6 + [sds((dm.ns, D, dm.r), bf16), row, wide, wide, sds((M, D), f32), sds((f, D), f32), sds((f, D), f32)]
    scratch = [vm((dm.ns, dm.length, D), bf16)] * 2 + [vm((M, D), bf16)] * 2 + [vm((3 * D, D), bf16), vm((D, D), bf16), vm((2, D, f), bf16)]
    scratch += [vm((M, D), bf16)] * 4 + [vm((dm.ns, D, dm.r), bf16), vm((M, D), bf16), vm((M, 2 * f), bf16), vm((M, 2 * f), bf16), vm((M, D), f32), vm((2, f, D), f32)]
    scratch += [vm((2, 2, dm.r, dm.r), bf16), vm((2, dm.hw, D), f32), vm((dm.n_t, 16, D), f32), vm((8, D), f32)]
    scratch += [dma((2,)), dma((3,)), dma((2 * dm.ns,)), dma((20,)), dma((GATHER_SEMS,)), dma((GATHER_SEMS,)), dma((GATHER_SEMS,)), dma((GATHER_SEMS,)), dma((1,)), dma((1,))]

    def kern(*refs):
        forward_kernel(dm, n_dp, *refs)

    return pl.pallas_call(
        kern,
        out_shape=outs,
        in_specs=[SM] + [V] * (len(small) - 1) + [ANY] * len(big),
        out_specs=[ANY] * len(outs),
        scratch_shapes=scratch,
        compiler_params=pltpu.CompilerParams(vmem_limit_bytes=VMEM_LIMIT, collective_id=1, has_side_effects=True),
        name="forward",
    )(*small, *big)


class Reduce:
    KINDS = 9

    def __init__(self, ln, own, sib, rz, rx, fin, vin, vout, lsem, ssem, rsem, n_sub, n_arrays):
        self.ln, self.own, self.sibling, self.rz, self.rx, self.fin = ln, own, sib, rz, rx, fin
        self.vin, self.vout, self.lsem, self.ssem, self.rsem = vin, vout, lsem, ssem, rsem
        self.n_sub, self.total = n_sub, n_sub * n_arrays
        self.block = own.shape[1] // 4
        self.pr = self.block // n_sub
        L, z = ln.length, ln.z
        self.L = L
        self.far = (L - 1 - z, z)
        self.waves = self.total + 2 * L

    def view(self, ref, q, b):
        return ref.at[q // self.n_sub, pl.ds(pl.multiple_of(b * self.block + lax.rem(q, self.n_sub) * self.pr, 8), self.pr)]

    def parent(self, d):
        return (2 * (self.ln.z + (-1 if d == 0 else 1)) + self.ln.x, self.ln.t)

    def child(self, d):
        return (2 * (self.ln.z + (1 if d == 0 else -1)) + self.ln.x, self.ln.t)

    def partner(self):
        return (2 * self.ln.z + 1 - self.ln.x, self.ln.t)

    def local(self, src, i, j):
        return pltpu.make_async_copy(src, self.vin.at[i, j], self.lsem.at[i, j])

    def landed(self, view, q, kind):
        rcopy(view, view, self.ssem.at[0, 0], self.rsem.at[q, kind], self.ln.sib).wait_recv()

    def ok(self, q):
        return (q >= 0) & (q < self.total)

    def send(self, src, dst, slot, k, q, kind, dev):
        return rcopy(src, dst, self.ssem.at[slot, k], self.rsem.at[q, kind], dev)

    def wave(self, tau, start=True):
        ln, L = self.ln, self.L
        slot = lax.rem(tau, 2)
        col = ln.x
        leaf = 1 - ln.x

        def each(fn):
            return fn

        q = tau
        b = leaf

        @pl.when(self.ok(q))
        def _():
            v, o = self.vin, self.vout.at[slot, 0]
            if start:
                a, s = self.local(self.view(self.own, q, b), 0, 0), self.local(self.view(self.sibling, q, b), 0, 1)
                a.start()
                s.start()
                a.wait()
                s.wait()
                o[...] = v[0, 0] + v[0, 1]
            cp = self.send(o, self.view(self.rx, q, b), slot, 0, q, 0, self.partner())
            cp.start() if start else cp.wait_send()

        k = jnp.where(col == 0, self.far[0], self.far[1])
        z = ln.z
        up = (2 * (z + (2 * col - 1)) + ln.x, ln.t)
        down = (2 * (z + (1 - 2 * col)) + ln.x, ln.t)
        q1 = tau - 1 - k

        @pl.when(self.ok(q1))
        def _():
            v, o = self.vin, self.vout.at[slot, 1]
            if start:
                a, s = self.local(self.view(self.own, q1, col), 1, 0), self.local(self.view(self.sibling, q1, col), 1, 1)
                a.start()
                s.start()
                xv = self.view(self.rx, q1, col)
                self.landed(xv, q1, 0)
                x = self.local(xv, 1, 2)
                x.start()

                @pl.when(k > 0)
                def _():
                    zv = self.view(self.rz, q1, col)
                    self.landed(zv, q1, 1)
                    g = self.local(zv, 1, 3)
                    g.start()
                    g.wait()

                a.wait()
                s.wait()
                x.wait()
                o[...] = (v[1, 0] + v[1, 1]) + v[1, 2]

                @pl.when(k > 0)
                def _():
                    o[...] += v[1, 3]

            @pl.when(k < L - 1)
            def _():
                cp = self.send(o, self.view(self.rz, q1, col), slot, 1, q1, 1, up)
                cp.start() if start else cp.wait_send()

            @pl.when(k == L - 1)
            def _():
                fv = self.view(self.fin, q1, col)
                cps = [pltpu.make_async_copy(o, fv, self.lsem.at[4, slot]), self.send(o, fv, slot, 2, q1, 5, down), self.send(o, fv, slot, 3, q1, 6, self.partner())]
                for cp in cps:
                    cp.start() if start else (cp.wait() if cp is cps[0] else cp.wait_send())

        for d in range(2):
            kd = self.far[d]
            q2 = tau - 1 - kd
            bz = 2 + d

            @pl.when(self.ok(q2))
            def _():
                v, o = self.vin, self.vout.at[slot, 2 + d]
                if start:
                    a, s = self.local(self.view(self.own, q2, bz), 2, 2 * d), self.local(self.view(self.sibling, q2, bz), 2, 2 * d + 1)
                    a.start()
                    s.start()

                    @pl.when(kd > 0)
                    def _():
                        zv = self.view(self.rz, q2, bz)
                        self.landed(zv, q2, 2 + d)
                        g = self.local(zv, 3, d)
                        g.start()
                        g.wait()

                    a.wait()
                    s.wait()
                    o[...] = v[2, 2 * d] + v[2, 2 * d + 1]

                    @pl.when(kd > 0)
                    def _():
                        o[...] += v[3, d]

                @pl.when(kd < L - 1)
                def _():
                    cp = self.send(o, self.view(self.rz, q2, bz), slot, 4 + 3 * d, q2, 2 + d, self.parent(d))
                    cp.start() if start else cp.wait_send()

                @pl.when(kd == L - 1)
                def _():
                    xv, fv, tot = self.view(self.rx, q2, bz), self.view(self.fin, q2, bz), self.vout.at[slot, 4]
                    cp = self.send(o, xv, slot, 5 + 3 * d, q2, 4, self.partner())
                    if start:
                        cp.start()
                        self.landed(xv, q2, 4)
                        x = self.local(xv, 3, 2)
                        x.start()
                        x.wait()
                        tot[...] = o[...] + v[3, 2]
                    else:
                        cp.wait_send()
                    cps = [pltpu.make_async_copy(tot, fv, self.lsem.at[4, 2 + slot]), self.send(tot, fv, slot, 6 + 3 * d, q2, 7 + d, self.child(d))]
                    for cp in cps:
                        cp.start() if start else (cp.wait() if cp is cps[0] else cp.wait_send())

        r = L - 1 - k
        q3 = tau - L - r

        @pl.when(self.ok(q3) & (r > 0))
        def _():
            fv = self.view(self.fin, q3, col)
            if start:
                self.landed(fv, q3, 5)

            @pl.when(k > 0)
            def _():
                cp = self.send(fv, fv, slot, 10, q3, 5, down)
                cp.start() if start else cp.wait_send()

            cp = self.send(fv, fv, slot, 11, q3, 6, self.partner())
            cp.start() if start else cp.wait_send()

        for d in range(2):
            kd = self.far[d]
            r = L - 1 - kd
            q4 = tau - L - r

            @pl.when(self.ok(q4) & (r > 0))
            def _():
                fv = self.view(self.fin, q4, 2 + d)
                if start:
                    self.landed(fv, q4, 7 + d)

                @pl.when(kd > 0)
                def _():
                    cp = self.send(fv, fv, slot, 12 + d, q4, 7 + d, self.child(d))
                    cp.start() if start else cp.wait_send()

    def step(self, tau):
        self.wave(tau - 2, start=False)
        self.wave(tau)

    def steps(self, t0, t1):
        def body(tau, carry):
            self.step(tau)
            return carry

        lax.fori_loop(t0, t1, body, 0)

    def finish(self):
        self.wave(self.waves - 2, start=False)
        self.wave(self.waves - 1, start=False)

        def body(q, carry):
            self.landed(self.view(self.fin, q, 1 - self.ln.x), q, 6)
            return carry

        lax.fori_loop(0, self.total, body, 0)


N_SUB = 4


def backward_kernel(dm, n_dp, *refs):
    (meta, wdn_s, g1_r, g2_r, bd_r, n32, gu, p_hbm, i_wqkv, i_wo, i_bias, i_tok, i_cot, i_normed, i_q8, i_kk, i_vv, i_mixt, i_n2, i_act, i_gp, i_mid, d_own, d_sib, wup_s) = refs[:25]
    (fin, sm_out, lo32, gt32, gn_h, own, sibl, rz, rx) = refs[25:34]
    (wqkv, wo, wup, wdn, tok, cot, normed, q8, kk, vv, mixt, n2, gp, act, mid, gn, dwa, acc, pbuf, tmp, bbuf, vin, vout, small, sland) = refs[34:59]
    psem, tsem, lsem, osem, nss, nrs, xss, xrs, rls, rss, rrs, sss, srs = refs[59:]
    R, D, NS, hw, f = dm.r, dm.d, dm.ns, dm.hw, dm.f
    ln = Links(n_dp)
    y, c, t = ln.y, ln.c, ln.t
    base = c * NS
    nt, ft = D // 256, f // 256

    srcs = (i_gp, i_act, i_n2, i_cot, i_bias, i_mid, i_wqkv, i_wo, i_mixt, i_q8, i_kk, i_vv, i_normed, i_tok, wup_s)
    dsts = (gp.at[:, pl.ds(0, 2 * f)], act, n2, cot, bbuf, mid, wqkv, wo, mixt, q8, kk, vv, normed, tok, wup.at[t])
    ins = [pltpu.make_async_copy(a, b, lsem.at[i]) for i, (a, b) in enumerate(zip(srcs, dsts))]
    for cp in ins:
        cp.start()
    moved = [pltpu.make_async_copy(d_own, own.at[0], osem.at[0]), pltpu.make_async_copy(d_sib, sibl.at[0], osem.at[1])]
    for cp in moved:
        cp.start()
    bar = pltpu.get_barrier_semaphore()
    group = ln.dp - lax.rem(ln.dp, n_dp)
    for dev in (ln.ypart, ln.sib):
        pl.semaphore_signal(bar, inc=1, device_id=dev, device_id_type=MESH)

    def greet(i, carry):
        pl.semaphore_signal(bar, inc=1, device_id=(lax.rem(ln.dp + i, n_dp), t), device_id_type=MESH)
        return carry

    lax.fori_loop(1, n_dp, greet, 0)
    pl.semaphore_wait(bar, 2 + n_dp - 1)
    red = Reduce(ln, own, sibl, rz, rx, fin, vin, vout, rls, rss, rrs, N_SUB, 3)
    pending = []

    third = f // 3
    for i in range(3):
        v = pl.ds(i * third, third)
        cp = rcopy(n32.at[v], gn_h.at[t, v], nss.at[i], nrs.at[i], ln.ypart)
        cp.start()
        pending.append(cp)
    cp = rcopy(n32, gn_h.at[t], nss.at[3], nrs.at[3], ln.sib)
    cp.start()
    pending.append(cp)

    def landed(view, sem):
        rcopy(view, view, nss.at[0], sem, ln.sib).wait_recv()

    def pass_on(i):
        v = gn_h.at[ln.t_y, pl.ds(i * third, third)]
        landed(v, nrs.at[i])
        cp = rcopy(v, v, nss.at[4 + i], nrs.at[4 + i], ln.sib)
        cp.start()
        pending.append(cp)

    def narrow(src, put):
        n = src.shape[0] // 4
        cps = []
        for i in range(4):
            cps.append(pltpu.make_async_copy(src.at[pl.ds(i * n, n)], tmp.at[i % 2], tsem.at[i % 2]))
            if i == 0:
                cps[0].start()
        for i in range(4):
            if i < 3:
                cps[i + 1].start()
            cps[i].wait()
            put(i * n, n, tmp[i % 2].astype(bf16))

    def put_dn(ts):
        def put(r, n, v):
            wdn[pl.ds(pl.multiple_of(ts * f + r, 16), n), :] = v

        return put

    def put_up(ts):
        def put(r, n, v):
            wup[ts, r : r + n, :] = v

        return put

    wdn[al(t, f), :] = wdn_s[...]
    narrow(gu.at[ln.t_sib], put_up(ln.t_sib))
    landed(gn_h.at[ln.t_sib], nrs.at[3])
    narrow(gn_h.at[ln.t_sib], put_dn(ln.t_sib))
    for i in range(4):
        ins[i].wait()
    acc[...] = jnp.zeros_like(acc)

    def unit(j):
        half = j // (2 * ft)
        hf = jnp.where(half == 0, y, 1 - y)
        return 2 * hf + lax.rem(j, 2 * ft) // ft, lax.rem(j, ft)

    def grad_hidden(half):
        def one(i):
            s, j = i // (2 * ft), half * 2 * ft + lax.rem(i, 2 * ft)
            sh, k = unit(j)
            rs, cs = al(s, R), al(j, 256)
            ga = mmt(cot[rs, :], wdn[pl.ds(pl.multiple_of(sh * f + k * 256, 256), 256), :])
            gp[rs, cs] = (ga * gp[rs, cs].astype(f32)).astype(bf16)

        loop(NS * 2 * ft, one)

    grad_hidden(0)

    def dwup(i):
        sh, j = i // nt, lax.rem(i, nt)
        for n in range(ft):
            dwa[pl.ds(pl.multiple_of(i * 256, 256), 256), n * 256 : n * 256 + 256] = tmm(n2[:, al(j, 256)], gp[:, al(sh * ft + n, 256)])

    loop(2 * nt, dwup)
    up_own = pltpu.make_async_copy(dwa.at[al(c, D)], own.at[1], osem.at[2])
    up_own.start()
    up_sib = rcopy(dwa.at[al(1 - c, D)], sibl.at[1], xss.at[0], xrs.at[0], ln.sib)
    up_sib.start()
    for cp in moved:
        cp.wait()
    red.steps(0, 1)
    ones = jnp.ones((8, dm.rows), bf16)
    for sh in range(2):
        acc[6 + sh, :, :f] = mm(ones, gp[:, sh * f : (sh + 1) * f]) * 0.125

    bd = bd_r[...].reshape(1, D)
    ins[4].wait()
    ins[5].wait()

    def lo_own(s):
        rs = al(s, R)
        gn[rs, :] = mid[rs, :] + bd + mm(act[rs, :], wdn[al(y, 2 * f), :])

    loop(NS, lo_own)
    ins[14].wait()
    narrow(gu.at[ln.t_y], put_up(ln.t_y))
    narrow(gu.at[ln.t_ysib], put_up(ln.t_ysib))
    red.steps(1, 2)

    def mlp(i):
        s, j = i // (2 * ft), lax.rem(i, 2 * ft)
        sh, k = unit(2 * ft + j)
        rs, cs = al(s, R), al(k, 256)
        h = mm(n2[rs, :], wup[sh, :, cs]) + bbuf[sh, 0:1, cs]
        a, g = gelu_pair(h)
        act[rs, al(j, 256)] = a.astype(bf16)
        gp[rs, al(2 * ft + j, 256)] = g.astype(bf16)

    loop(NS * 2 * ft, mlp)
    red.steps(2, 3)
    up_own.wait()
    up_sib.wait()
    pass_on(0)
    red.steps(3, 4)
    pass_on(1)
    red.steps(4, 5)
    pass_on(2)
    narrow(gn_h.at[ln.t_y], put_dn(ln.t_y))
    for i in range(3):
        v = gn_h.at[ln.t_ysib, pl.ds(i * third, third)]
        landed(v, nrs.at[4 + i])
    narrow(gn_h.at[ln.t_ysib], put_dn(ln.t_ysib))
    grad_hidden(1)
    red.steps(5, 6)
    for cp in ins[6:]:
        if cp is not ins[14]:
            cp.wait()

    def gnorm2(s):
        rs = al(s, R)
        tot = None
        for half in range(2):
            for i in range(2):
                sh = 2 * (y if half == 0 else 1 - y) + i
                k = half * 2 + i
                p = mmt(gp[rs, k * f : (k + 1) * f], wup[sh])
                tot = p if tot is None else tot + p
        lo = gn[rs, :] + mm(act[rs, :], wdn[al(1 - y, 2 * f), :])
        dwa[rs, :] = lo
        gn[rs, :] = tot

    loop(NS, gnorm2)
    lo_copies = []
    for s in range(NS):
        v = dwa.at[pl.ds(s * R, R)]
        lo_copies.append((pltpu.make_async_copy(v, lo32.at[base + s], osem.at[3 + s]), rcopy(v, lo32.at[base + s], xss.at[1 + s], xrs.at[1 + s], ln.sib)))
        for cp in lo_copies[-1]:
            cp.start()
    red.steps(6, 7)
    g2 = g2_r[...].reshape(1, D)
    g1 = g1_r[...].reshape(1, D)

    def ln2b(i):
        rs = pl.ds(pl.multiple_of(i * CH, CH), CH)
        xh, r = centred(mid[rs, :])
        go = gn[rs, :]
        co = cot[rs, :].astype(f32)
        g = go * g2
        gx = g * xh
        gm = co + r * (g - jnp.sum(g, -1, keepdims=True) * (1.0 / D) - xh * (jnp.sum(gx, -1, keepdims=True) * (1.0 / D)))
        mid[rs, :] = gm
        gl = gm.astype(bf16)
        act[rs, 0:D] = gl
        acc[0] += fold8(co)
        acc[1] += fold8(gl.astype(f32))
        acc[4] += fold8(go * xh)
        acc[5] += fold8(go)

    loop(dm.rows // CH, ln2b)

    def gmixf(s):
        rs = al(s, R)
        act[rs, D : 2 * D] = mmt(act[rs, 0:D], wo[...]).astype(bf16)

    loop(NS, gmixf)
    own_h = al(y, 2 * hw)

    def over_samples(fn):
        tot = None
        for s in range(NS):
            p = fn(s)
            tot = p if tot is None else tot + p
        return tot

    for a, b in lo_copies:
        a.wait()
        b.wait()

    for n in range(nt):
        cc = slice(n * 256, n * 256 + 256)
        p = over_samples(lambda s: mm(mixt[s, own_h, :], act[s * R : s * R + R, cc]))
        for sh in range(2):
            dwa[sh * D + 3 * hw : sh * D + 4 * hw, cc] = p[sh * hw : (sh + 1) * hw]
    red.steps(7, 8)
    lane = lax.broadcasted_iota(jnp.int32, (1, 128), 1)
    masks = (lane < HEAD_DIM, lane >= HEAD_DIM)
    total = NS * dm.pairs

    def p_copy(i):
        slot = lax.rem(i, 2)
        return pltpu.make_async_copy(p_hbm.at[i], pbuf.at[slot], psem.at[slot])

    p_copy(0).start()

    def attn(i):
        s, p = i // dm.pairs, lax.rem(i, dm.pairs)
        slot = lax.rem(i, 2)
        rs, cs = al(s, R), al(p, 128)

        @pl.when(i + 1 < total)
        def _():
            p_copy(i + 1).start()

        p_copy(i).wait()
        q, k, v, do = q8[rs, cs], kk[rs, cs], vv[rs, cs], act[rs, pl.ds(pl.multiple_of(D + p * 128, 128), 128)]
        dv, dk = [], []
        for h in range(2):
            pt = pbuf[slot, h]
            pf = pt.astype(f32)
            dp = mmt(jnp.where(masks[h], v, jnp.bfloat16(0)), do)
            dsum = jnp.sum(pf * dp, 0, keepdims=True)
            ds = (pf * (dp - dsum)).astype(bf16)
            dv.append(mm(pt, do))
            dk.append(mm(ds, q))
            o = tmm(k, ds)
            hr = pl.ds(pl.multiple_of(p * 128 + h * HEAD_DIM, HEAD_DIM), HEAD_DIM)
            mixt[s, hr, :] = (o[h * HEAD_DIM : (h + 1) * HEAD_DIM] * 0.125).astype(bf16)
        kk[rs, cs] = jnp.where(masks[0], dk[0], dk[1]).astype(bf16)
        vv[rs, cs] = jnp.where(masks[0], dv[0], dv[1]).astype(bf16)

    loop(total, attn)
    for n in range(nt):
        cc = slice(n * 256, n * 256 + 256)
        p = over_samples(lambda s: mm(mixt[s, own_h, :], normed[s * R : s * R + R, cc]))
        tk = tmm(kk[:, own_h], normed[:, cc])
        tv = tmm(vv[:, own_h], normed[:, cc])
        for sh in range(2):
            h = slice(sh * hw, (sh + 1) * hw)
            dwa[sh * D : sh * D + hw, cc] = p[h]
            dwa[sh * D + hw : sh * D + 2 * hw, cc] = tk[h]
            dwa[sh * D + 2 * hw : sh * D + 3 * hw, cc] = tv[h]
    a_own = pltpu.make_async_copy(dwa.at[al(c, D)], own.at[2], osem.at[2])
    a_own.start()
    a_sib = rcopy(dwa.at[al(1 - c, D)], sibl.at[2], xss.at[5], xrs.at[5], ln.sib)
    a_sib.start()
    onesr = jnp.ones((8, R), bf16)
    acc[8, :, 0 : 2 * hw] = over_samples(lambda s: mmt(onesr, mixt[s, own_h, :])) * 0.125
    acc[9, :, 0 : 2 * hw] = mm(ones, vv[:, own_h]) * 0.125
    a_own.wait()
    a_sib.wait()
    red.steps(8, 9)

    def gnorm1(s):
        rs = al(s, R)
        gn[rs, :] = tmm(mixt[s], wqkv[0:D, :]) + mm(kk[rs, :], wqkv[D : 2 * D, :]) + mm(vv[rs, :], wqkv[2 * D : 3 * D, :])

    loop(NS, gnorm1)

    def ln1b(s):
        for r0, n in row_chunks(dm):
            rs = pl.ds(pl.multiple_of(s * R + r0, 16), n)
            x = tok[rs, :].astype(f32)
            keep = keep_of(meta, base, s, r0, n) if r0 == 0 else None
            xh, r = centred(x if keep is None else x * keep)
            go = gn[rs, :]
            g = go * g1
            gx = g * xh
            gi = r * (g - jnp.sum(g, -1, keepdims=True) * (1.0 / D) - xh * (jnp.sum(gx, -1, keepdims=True) * (1.0 / D)))
            o = mid[rs, :] + gi
            mid[rs, :] = o if keep is None else o * keep
            acc[2] += fold8(go * xh)
            acc[3] += fold8(go)

    loop(NS, ln1b)
    gt_copies = []
    for s in range(NS):
        v = mid.at[pl.ds(s * R, R)]
        gt_copies.append((pltpu.make_async_copy(v, gt32.at[base + s], osem.at[3 + s]), rcopy(v, gt32.at[base + s], xss.at[6 + s], xrs.at[6 + s], ln.sib)))
        for cp in gt_copies[-1]:
            cp.start()

    tot = jnp.sum(acc[...], 1)
    for sh in range(2):
        small[sh, 0:6, :] = tot[0:6]
        small[sh, 6:7, :] = tot[6 + sh : 7 + sh]
        small[sh, 7:8, 0:hw] = tot[8:9, sh * hw : (sh + 1) * hw]
        small[sh, 7:8, hw : 2 * hw] = tot[9:10, sh * hw : (sh + 1) * hw]
        small[sh, 7:8, 2 * hw :] = jnp.zeros((1, D - 2 * hw), f32)
    cp = rcopy(small.at[1 - c], small.at[2], xss.at[10], xrs.at[10], ln.sib)
    cp.start()
    cp.wait()
    sland[ln.dp] = small[c] + small[2]

    def peer(i):
        d = lax.rem(ln.dp + i, n_dp)
        return rcopy(sland.at[ln.dp], sland.at[ln.dp], sss.at[d], srs.at[ln.dp], (d, t))

    def spread(i, carry):
        peer(i).start()
        return carry

    lax.fori_loop(1, n_dp, spread, 0)
    red.steps(9, red.waves)
    red.finish()

    def gathered(i, carry):
        peer(i).wait_send()
        d = lax.rem(ln.dp + i, n_dp)
        rcopy(sland.at[d], sland.at[d], sss.at[d], srs.at[d], (d, t)).wait_recv()
        return carry

    lax.fori_loop(1, n_dp, gathered, 0)
    sm_out[...] = lax.fori_loop(1, n_dp, lambda i, v: v + sland[i], sland[0])
    for a, b in gt_copies:
        a.wait()
        b.wait()
    for cp in pending:
        cp.wait_send()


def backward_call(dm, n_dp, small, big):
    M, D, f = dm.rows, dm.d, dm.f
    sds, vm, dma = jax.ShapeDtypeStruct, pltpu.VMEM, pltpu.SemaphoreType.DMA
    st = sds((3, D, D), f32)
    outs = [st, sds((8, D), f32), sds((dm.samples, dm.r, D), f32), sds((dm.samples, dm.r, D), f32), sds((dm.n_t, f, D), f32), st, st, st, st]
    row, wide = vm((M, D), bf16), vm((M, 2 * f), bf16)
    pr = D // 4 // N_SUB
    scratch = [vm((3 * D, D), bf16), vm((D, D), bf16), vm((dm.n_t, D, f), bf16), vm((dm.ff, D), bf16)] + [row] * 6
    scratch += [vm((dm.ns, D, dm.r), bf16), row, vm((M, dm.ff), bf16), wide, vm((M, D), f32), vm((M, D), f32), vm((2 * D, D), f32), vm((10, 8, D), f32)]
    scratch += [vm((2, 2, dm.r, dm.r), bf16), vm((2, f // 4, D), f32), vm((dm.n_t, 16, D), f32), vm((4, 4, pr, D), f32), vm((2, 5, pr, D), f32), vm((3, 8, D), f32), vm((n_dp, 8, D), f32)]
    nq = 3 * N_SUB
    scratch += [dma((2,)), dma((2,)), dma((15,)), dma((7,)), dma((7,)), dma((7,)), dma((11,)), dma((11,)), dma((5, 4)), dma((2, 14)), dma((nq, Reduce.KINDS)), dma((n_dp,)), dma((n_dp,))]

    def kern(*refs):
        backward_kernel(dm, n_dp, *refs)

    return pl.pallas_call(
        kern,
        out_shape=outs,
        in_specs=[SM] + [V] * (len(small) - 1) + [ANY] * len(big),
        out_specs=[ANY, V] + [ANY] * 7,
        scratch_shapes=scratch,
        compiler_params=pltpu.CompilerParams(vmem_limit_bytes=VMEM_LIMIT, collective_id=2, has_side_effects=True),
        name="backward",
    )(*small, *big)


def shards(tokens, metadata, cotangent, w_query, w_key, w_value, w_out, b_query, b_value, b_out, w_up, b_up, w_down, b_down, gain_one, shift_one, gain_two, shift_two, n_dp, n_t):
    dm = Dims(tokens, w_up, n_t)
    D, hw, f = dm.d, dm.hw, dm.f
    bias = jnp.concatenate([b_up, b_query, b_value, jnp.zeros((16 * D - f - 2 * hw,), f32)]).reshape(16, D)
    small = (metadata, w_query, w_key, w_value, w_out, w_up, w_down, bias, gain_one, shift_one, gain_two, shift_two, b_out)
    (_, gu, n32, p, wqkv, wo, bb, tok, cot, normed, q8, kk, vv, mixt, n2, act, gp, mid, d_own, d_sib) = forward_call(dm, n_dp, small, (tokens, cotangent))
    small = (metadata, w_down, gain_one, gain_two, b_down)
    fin, sm, lo, gt, *_ = backward_call(dm, n_dp, small, (n32, gu, p, wqkv, wo, bb, tok, cot, normed, q8, kk, vv, mixt, n2, act, gp, mid, d_own, d_sib, w_up))
    a_ = fin[2]
    return (
        lo[:, : dm.length].astype(bf16),
        gt[:, : dm.length],
        a_[0:hw].T,
        a_[hw : 2 * hw].T,
        a_[2 * hw : 3 * hw].T,
        a_[3 * hw : 4 * hw],
        sm[7, :hw],
        sm[7, hw : 2 * hw],
        sm[1],
        fin[1],
        sm[6],
        fin[0],
        sm[0],
        sm[2],
        sm[3],
        sm[4],
        sm[5],
    )


def solution(mesh):
    n_dp, n_t = mesh.shape["dp"], mesh.shape["tensor"]
    rows, cols, vec, rep = P("dp", None, None), P(None, "tensor"), P("tensor"), P()
    srow = P("tensor", None)

    def run(*args):
        return shards(*args, n_dp=n_dp, n_t=n_t)

    return jax.shard_map(
        run,
        mesh=mesh,
        in_specs=(rows, P("dp"), rows, cols, cols, cols, srow, vec, vec, rep, cols, vec, srow, rep, rep, rep, rep, rep),
        out_specs=(rows, rows, cols, cols, cols, srow, vec, vec, rep, cols, vec, srow, rep, rep, rep, rep, rep),
        check_vma=False,
    )
```

```python
import math

import jax
import jax.numpy as jnp
from jax import lax
from jax.experimental import pallas as pl
from jax.experimental.pallas import tpu as pltpu
from jax.sharding import PartitionSpec as P

HEAD_DIM = 64
EPS = 1e-05
MESH = pl.DeviceIdType.MESH
f32 = jnp.float32
bf16 = jnp.bfloat16
VMEM_LIMIT = 63 << 20
RING = 8
CH = 64
TAIL_P = 0.24
TAIL = (
    0.08952743306829739,
    0.15551359433427508,
    -0.15404885518029288,
    0.6255903019940591,
    -0.6460706945688248,
    0.5545739487327468,
    -0.12508572868970558,
)
INV_SQRT_2PI = 1.0 / math.sqrt(2.0 * math.pi)
HALF_LOG2E = -0.5 / math.log(2.0)


def mm(a, b):
    return lax.dot_general(a, b, (((1,), (0,)), ((), ())), preferred_element_type=f32)


def mmt(a, b):
    return lax.dot_general(a, b, (((1,), (1,)), ((), ())), preferred_element_type=f32)


def tmm(a, b):
    return lax.dot_general(a, b, (((0,), (0,)), ((), ())), preferred_element_type=f32)


def loop(n, fn):
    def body(i, carry):
        fn(i)
        return carry

    lax.fori_loop(0, n, body, 0)


def al(i, step):
    return pl.ds(pl.multiple_of(i * step, step), step)


def centred(x):
    d = x.shape[-1]
    mu = jnp.sum(x, -1, keepdims=True) * (1.0 / d)
    xm = x - mu
    var = jnp.sum(xm * xm, -1, keepdims=True) * (1.0 / d)
    r = lax.rsqrt(var + EPS)
    return xm * r, r


def gelu_pair(v):
    d = 1.0 + TAIL_P * jnp.abs(v)
    t = pltpu.reciprocal(d, approx=True)
    t = t * (2.0 - d * t)
    e = jnp.exp2(HALF_LOG2E * (v * v))
    acc = TAIL[6] * t + TAIL[5]
    for k in range(4, -1, -1):
        acc = acc * t + TAIL[k]
    q = (acc * t) * e
    cdf = jnp.where(v < 0, q, 1.0 - q)
    return v * cdf, cdf + (v * e) * INV_SQRT_2PI


def fold8(x):
    return jnp.sum(x.reshape(x.shape[0] // 8, 8, x.shape[1]), 0)


class Dims:
    def __init__(self, tokens, w_up, n_t):
        self.samples, self.length, self.d = tokens.shape
        self.ns = self.samples // 2
        self.r = -(-self.length // 16) * 16
        self.rows = self.ns * self.r
        self.f = w_up.shape[1]
        self.ff = self.f * n_t
        self.n_t = n_t
        self.heads = self.d // HEAD_DIM
        self.pairs = self.heads // 2
        self.hw = self.d // n_t


class Links:
    def __init__(self, n_dp):
        self.n_dp = n_dp
        self.dp = lax.axis_index("dp")
        self.t = lax.axis_index("tensor")
        self.y, self.c = self.t // 2, lax.rem(self.t, 2)
        self.z, self.x = self.dp // 2, lax.rem(self.dp, 2)
        self.length = n_dp // 2
        self.sib = (self.dp, 2 * self.y + 1 - self.c)
        self.ypart = (self.dp, 2 * (1 - self.y) + self.c)
        self.t_sib = 2 * self.y + 1 - self.c
        self.t_y = 2 * (1 - self.y) + self.c
        self.t_ysib = 2 * (1 - self.y) + 1 - self.c
        g = lax.rem(self.dp, RING)
        half = RING // 2
        zz, xx = g // 2, lax.rem(g, 2)
        self.pos = jnp.where(xx == 0, zz, RING - 1 - zz)
        base = self.dp - g

        def at(pos):
            pos = lax.rem(pos + RING, RING)
            local = jnp.where(pos < half, 2 * pos, 2 * (RING - 1 - pos) + 1)
            return (base + local, self.t)

        self.step = 1 - 2 * self.c
        self.ahead, self.behind = at(self.pos + self.step), at(self.pos - self.step)

    def piece(self, offset):
        return lax.rem(self.pos + offset * self.step + RING, RING)


def rcopy(src, dst, ssem, rsem, dev):
    return pltpu.make_async_remote_copy(src_ref=src, dst_ref=dst, send_sem=ssem, recv_sem=rsem, device_id=dev, device_id_type=MESH)


def enter(devs):
    bar = pltpu.get_barrier_semaphore()
    for d in devs:
        pl.semaphore_signal(bar, inc=1, device_id=d, device_id_type=MESH)
    pl.semaphore_wait(bar, len(devs))


class Gather:
    def __init__(self, ln, src, out, direct, ssem, rsem):
        self.ln, self.src, self.out, self.direct = ln, src, out, direct
        self.ssem, self.rsem = ssem, rsem
        self.passed = self.passed_sib = False
        self.rows = src.shape[0]
        self.piece_rows = (self.rows - direct) // RING

    def at(self, ref, offset):
        return ref.at[pl.ds(pl.multiple_of(self.direct + self.ln.piece(offset) * self.piece_rows, 8), self.piece_rows)]

    def copy(self, src, dst, k, dev):
        return rcopy(src, dst, self.ssem.at[k], self.rsem.at[k], dev)

    def landed(self, view, k):
        rcopy(view, view, self.ssem.at[k], self.rsem.at[k], self.ln.sib).wait_recv()

    def spread_y(self):
        return self.copy(self.at(self.src, 0), self.at(self.out.at[self.ln.t], 0), 0, self.ln.ypart)

    def direct_y(self):
        d = pl.ds(0, self.direct)
        return self.copy(self.src.at[d], self.out.at[self.ln.t].at[d], 1, self.ln.ypart)

    def whole_sib(self):
        return self.copy(self.src, self.out.at[self.ln.t], 2, self.ln.sib)

    def start_y(self):
        self.spread_y().start()
        self.direct_y().start()

    def start_sib(self):
        self.whole_sib().start()

    def wait_sib(self):
        self.landed(self.out.at[self.ln.t_sib], 2)

    def to_sib(self, offset):
        v = self.at(self.out.at[self.ln.t_y], offset)
        return self.copy(v, v, 11 + 4 + offset, self.ln.sib)

    def direct_sib(self):
        v = self.out.at[self.ln.t_y].at[pl.ds(0, self.direct)]
        return self.copy(v, v, 10, self.ln.sib)

    def ring_ahead(self, s):
        v = self.at(self.out.at[self.ln.t_y], -s)
        return self.copy(v, v, 3 + s, self.ln.ahead)

    def ring_behind(self, s):
        v = self.at(self.out.at[self.ln.t_y], s)
        return self.copy(v, v, 7 + s, self.ln.behind)

    def tick(self, i):
        ln, out = self.ln, self.out.at[self.ln.t_y]
        if i == 0:
            self.landed(self.at(out, 0), 0)
            self.ring_ahead(0).start()
            self.ring_behind(0).start()
            self.to_sib(0).start()
            return
        s = i - 1
        self.landed(self.at(out, -s - 1), 3 + s)
        if s < 3:
            self.ring_ahead(s + 1).start()
            self.landed(self.at(out, s + 1), 7 + s)
            if s < 2:
                self.ring_behind(s + 1).start()
        self.to_sib(-s - 1).start()
        if s < 3:
            self.to_sib(s + 1).start()
        if i == 4:
            self.direct_landed()

    def direct_landed(self):
        if not self.passed:
            self.passed = True
            self.landed(self.out.at[self.ln.t_y].at[pl.ds(0, self.direct)], 1)
            self.direct_sib().start()

    def direct_sib_landed(self):
        if not self.passed_sib:
            self.passed_sib = True
            self.landed(self.out.at[self.ln.t_ysib].at[pl.ds(0, self.direct)], 10)

    def finish(self):
        ln, out = self.ln, self.out.at[self.ln.t_ysib]
        for offset in range(-4, 4):
            v = out.at[pl.ds(pl.multiple_of(self.direct + lax.rem(ln.pos - offset * ln.step + RING, RING) * self.piece_rows, 8), self.piece_rows)]
            self.landed(v, 11 + 4 + offset)
        self.direct_sib_landed()

    def drain(self):
        cps = [self.spread_y(), self.direct_y(), self.whole_sib(), self.direct_sib()]
        cps += [self.ring_ahead(s) for s in range(4)] + [self.ring_behind(s) for s in range(3)]
        cps += [self.to_sib(o) for o in range(-4, 4)]
        for cp in cps:
            cp.wait_send()


GATHER_SEMS = 19


def keep_of(meta, base, s, r0, n):
    rows = lax.broadcasted_iota(jnp.int32, (n, 1), 0) + r0
    return jnp.where(rows == 1, meta[base + s].astype(f32), 1.0)


def row_chunks(dm):
    out, r = [], 0
    while r < dm.r:
        n = min(CH, dm.r - r)
        out.append((r, n))
        r += n
    return out


def forward_kernel(dm, n_dp, *refs):
    (meta, wq, wk, wv, wo_s, wup_s, wdn_s, bup_r, bq_r, bv_r, g1_r, s1_r, g2_r, s2_r, bo_r, tokens, cotan) = refs[:17]
    (gu, gn_h, n32, p_hbm, o_wqkv, o_wo, o_bias, o_tok, o_cot, o_normed, o_q8, o_kk, o_vv, o_mixt, o_n2, o_act, o_gp, o_mid, d_own, d_sib) = refs[17:37]
    (tok3, cot3, tok, cot, wqkv, wo, wup, normed, q8, kk, vv, mixt, n2, act, gp, mid, dwd, pbuf, tmp, bbuf, bqv, ga, ustage) = refs[37:60]
    psem, tsem, lsem, osem, ssa, rsa, ssu, rsu, ssn, rsn, ssd, rsd = refs[60:]
    R, D, NS, hw, f = dm.r, dm.d, dm.ns, dm.hw, dm.f
    ln = Links(n_dp)
    y, c, t = ln.y, ln.c, ln.t
    base = c * NS

    def row(ref):
        return ref[...].reshape(1, D)

    loads = [pltpu.make_async_copy(tokens, tok3, lsem.at[0]), pltpu.make_async_copy(cotan, cot3, lsem.at[1])]
    for cp in loads:
        cp.start()
    outs = []

    def put(src, dst):
        cp = pltpu.make_async_copy(src, dst, osem.at[len(outs)])
        cp.start()
        outs.append(cp)

    own_a = mid.at[pl.ds(0, 16 + 3 * hw)]
    mid[0:16, :] = jnp.zeros((16, D), f32)
    mid[0:1, 0:f] = bup_r[...].reshape(1, f)
    mid[1:2, 0:hw] = bq_r[...].reshape(1, hw)
    mid[1:2, hw : 2 * hw] = bv_r[...].reshape(1, hw)
    bbuf[t] = mid[0:16, :]
    for i, w in enumerate((wq, wk, wv)):
        mid[16 + i * hw : 16 + (i + 1) * hw, :] = w[...].astype(f32)
        wqkv[pl.ds(pl.multiple_of(i * D + t * hw, 16), hw), :] = w[...]
    wo[al(t, hw), :] = wo_s[...]
    g_a = Gather(ln, own_a, ga, 16 + hw, ssa, rsa)
    g_u = Gather(ln, ustage, gu, hw + D // 3, ssu, rsu)
    g_n = Gather(ln, n32, gn_h, D // 3, ssn, rsn)
    enter((ln.ypart, ln.sib, ln.ahead, ln.behind))
    g_a.start_y()
    g_a.start_sib()
    ustage[0:hw, :] = wo_s[...].astype(f32)

    def widen(i):
        rs = al(i, 64)
        ustage[pl.ds(pl.multiple_of(hw + i * 64, 64), 64), :] = wup_s[rs, :].astype(f32)
        dwd[1, rs, :] = wdn_s[rs, :].astype(f32)
        wup[c, rs, :] = wup_s[rs, :]

    loop(D // 64, widen)
    put(dwd.at[1], n32)
    g_u.spread_y().start()
    outs[0].wait()
    g_n.spread_y().start()
    g_u.direct_y().start()
    g_n.direct_y().start()
    g_u.start_sib()
    g_n.start_sib()

    for cp in loads:
        cp.wait()
    g1, s1, g2, s2, bo = (row(r) for r in (g1_r, s1_r, g2_r, s2_r, bo_r))
    grp = dm.length // 32
    rest, pad = dm.length - grp * 32, R - grp * 32

    def selection(n_out, n_in):
        r = lax.broadcasted_iota(jnp.int32, (NS * n_out, n_in * 2 * NS), 0)
        col = lax.broadcasted_iota(jnp.int32, (NS * n_out, n_in * 2 * NS), 1)
        hit = (col == lax.rem(r, n_out) * (2 * NS) + base + r // n_out) & (lax.rem(r, n_out) < n_in)
        return jnp.where(hit, 1.0, 0.0).astype(bf16)

    sel = selection(32, 32)

    def regroup(g):
        for src, dst in ((tok3, tok), (cot3, cot)):
            v = src[al(g, 32)].astype(f32).reshape(32 * 2 * NS, D).astype(bf16)
            o = mm(sel, v).astype(bf16)
            for s in range(NS):
                dst[pl.ds(pl.multiple_of(s * R + g * 32, 16), 32), :] = o[s * 32 : (s + 1) * 32]

    loop(grp, regroup)
    if pad:
        sel_end = selection(pad, rest)
        for src, dst in ((tok3, tok), (cot3, cot)):
            v = src[grp * 32 : grp * 32 + rest].astype(f32).reshape(rest * 2 * NS, D).astype(bf16)
            o = mm(sel_end, v).astype(bf16)
            for s in range(NS):
                dst[s * R + grp * 32 : (s + 1) * R, :] = o[s * pad : (s + 1) * pad]
    put(tok, o_tok)
    put(cot, o_cot)

    def ln1(s):
        for r, n in row_chunks(dm):
            rs = pl.ds(pl.multiple_of(s * R + r, 16), n)
            x = tok[rs, :].astype(f32)
            if r == 0:
                x = x * keep_of(meta, base, s, r, n)
            xh, _ = centred(x)
            normed[rs, :] = (xh * g1 + s1).astype(bf16)

    loop(NS, ln1)
    put(normed, o_normed)

    def fetch(src, k):
        cp = pltpu.make_async_copy(src, tmp.at[k], tsem.at[k])
        cp.start()
        return cp

    def take_a(tp):
        bbuf[tp] = ga[tp, 0:16, :]
        for i in range(3):
            wqkv[pl.ds(pl.multiple_of(i * D + tp * hw, 16), hw), :] = ga[tp, 16 + i * hw : 16 + (i + 1) * hw, :].astype(bf16)

    lane = lax.broadcasted_iota(jnp.int32, (1, 128), 1)
    masks = (lane < HEAD_DIM, lane >= HEAD_DIM)
    hp = dm.pairs // 2
    tail = R - 16
    live = lax.broadcasted_iota(jnp.int32, (16, 1), 0) < dm.length - tail

    def project(hf):
        for i in range(2):
            b = bbuf[2 * hf + i]
            bqv[0:1, i * hw : (i + 1) * hw] = b[1:2, 0:hw]
            bqv[1:2, i * hw : (i + 1) * hw] = b[1:2, hw : 2 * hw]
        cs = al(hf, 2 * hw)

        def one(s):
            rs = al(s, R)
            n = normed[rs, :]
            w = [wqkv[pl.ds(pl.multiple_of(i * D + hf * 2 * hw, 128), 2 * hw), :] for i in range(3)]
            q8[rs, cs] = (mmt(n, w[0]) + bqv[0:1, : 2 * hw]).astype(bf16) * jnp.bfloat16(0.125)
            kk[rs, cs] = mmt(n, w[1]).astype(bf16)
            vv[rs, cs] = (mmt(n, w[2]) + bqv[1:2, : 2 * hw]).astype(bf16)

        loop(NS, one)

    def p_copy(hf, i):
        slot = lax.rem(i, 2)
        return pltpu.make_async_copy(pbuf.at[slot], p_hbm.at[(i // hp) * dm.pairs + hf * hp + lax.rem(i, hp)], psem.at[slot])

    def attend(hf, ticks):
        total = NS * hp

        def one(i):
            s, p = i // hp, hf * hp + lax.rem(i, hp)
            slot = lax.rem(i, 2)
            rs, cs = al(s, R), al(p, 128)
            for k, fn in ticks:
                pl.when(i == k)(fn)

            @pl.when(i >= 2)
            def _():
                p_copy(hf, i - 2).wait()

            q, k, v = q8[rs, cs], kk[rs, cs], vv[rs, cs]
            for h in range(2):
                st = mmt(jnp.where(masks[h], k, jnp.bfloat16(0)), q)
                sa = st[:tail]
                sb = jnp.where(live, st[tail:], -1e30)
                m = jnp.maximum(jnp.max(sa, 0, keepdims=True), jnp.max(sb, 0, keepdims=True))
                ea, eb = jnp.exp(sa - m), jnp.exp(sb - m)
                inv = 1.0 / (jnp.sum(ea, 0, keepdims=True) + jnp.sum(eb, 0, keepdims=True))
                pbuf[slot, h, :tail, :] = (ea * inv).astype(bf16)
                pbuf[slot, h, tail:, :] = (eb * inv).astype(bf16)
                o = tmm(v, pbuf[slot, h])
                hr = pl.ds(pl.multiple_of(p * 128 + h * HEAD_DIM, HEAD_DIM), HEAD_DIM)
                mixt[s, hr, :] = o[h * HEAD_DIM : (h + 1) * HEAD_DIM].astype(bf16)
            p_copy(hf, i).start()

        loop(total, one)
        p_copy(hf, total - 2).wait()
        p_copy(hf, total - 1).wait()

    g_a.wait_sib()
    take_a(ln.t_sib)
    g_a.tick(0)
    project(y)
    g_a.tick(1)
    attend(y, [(3, lambda: g_a.tick(2)), (9, lambda: g_a.tick(3))])
    g_a.tick(4)
    g_a.finish()
    take_a(ln.t_y)
    take_a(ln.t_ysib)
    put(wqkv, o_wqkv)
    put(bbuf, o_bias)
    g_u.tick(0)
    project(1 - y)
    put(q8, o_q8)
    put(kk, o_kk)
    put(vv, o_vv)
    attend(1 - y, [(2, lambda: g_u.tick(1)), (9, lambda: g_u.tick(2))])
    g_u.tick(3)
    put(mixt, o_mixt)
    g_a.drain()
    g_u.direct_landed()
    wo_rows = [fetch(gu.at[tp, pl.ds(0, hw)], i) for i, tp in enumerate((ln.t_y,))]
    g_u.wait_sib()
    wo_rows.append(fetch(gu.at[ln.t_sib, pl.ds(0, hw)], 1))
    g_u.direct_sib_landed()
    wo_rows.append(fetch(gu.at[ln.t_ysib, pl.ds(0, hw)], 2))
    for i, tp in enumerate((ln.t_y, ln.t_sib, ln.t_ysib)):
        wo_rows[i].wait()
        wo[al(tp, hw), :] = tmp[i].astype(bf16)
    put(wo, o_wo)
    ups = [fetch(gu.at[ln.t_sib, pl.ds((i + 1) * hw, hw)], i) for i in range(4)]

    def outp(s):
        rs = al(s, R)
        mid[rs, :] = tmm(mixt[s], wo[...])

    loop(NS, outp)

    def ln2(s):
        for r, n in row_chunks(dm):
            rs = pl.ds(pl.multiple_of(s * R + r, 16), n)
            x = tok[rs, :].astype(f32)
            if r == 0:
                x = x * keep_of(meta, base, s, r, n)
            m = x + (mid[rs, :] + bo)
            mid[rs, :] = m
            xh, _ = centred(m)
            n2[rs, :] = (xh * g2 + s2).astype(bf16)

    g_u.tick(4)
    g_n.tick(0)
    loop(NS, ln2)
    put(mid, o_mid)
    put(n2, o_n2)
    for i in range(4):
        ups[i].wait()
        wup[1 - c, i * hw : (i + 1) * hw, :] = tmp[i].astype(bf16)
    ft = f // 256

    def mlp(i):
        for k, n in ((7, 1), (14, 2), (21, 3)):
            pl.when(i == k)(lambda: g_n.tick(n))
        s, j = i // (2 * ft), lax.rem(i, 2 * ft)
        rs, sh, cs = al(s, R), j // ft, al(lax.rem(j, ft), 256)
        h = mm(n2[rs, :], wup[sh, :, cs]) + bbuf[2 * y + sh, 0:1, cs]
        a, g = gelu_pair(h)
        act[rs, al(j, 256)] = a.astype(bf16)
        gp[rs, al(j, 256)] = g.astype(bf16)

    loop(NS * 2 * ft, mlp)
    put(act, o_act)
    put(gp, o_gp)

    def dwdn(sh):
        def one(j):
            dwd[sh, al(j, 256), :] = tmm(act[:, al(sh * ft + j, 256)], cot[...])

        loop(ft, one)

    dwdn(1 - c)
    ex = rcopy(dwd.at[1 - c], d_sib, ssd.at[0], rsd.at[0], ln.sib)
    ex.start()
    g_n.tick(4)
    dwdn(c)
    put(dwd.at[c], d_own)
    g_u.finish()
    g_n.wait_sib()
    g_n.finish()
    g_u.drain()
    g_n.drain()
    ex.wait()
    for cp in outs[1:]:
        cp.wait()


V = pl.BlockSpec(memory_space=pltpu.VMEM)
ANY = pl.BlockSpec(memory_space=pl.ANY)
SM = pl.BlockSpec(memory_space=pltpu.SMEM)


def forward_call(dm, n_dp, small, big):
    M, D, f = dm.rows, dm.d, dm.f
    sds, vm, dma = jax.ShapeDtypeStruct, pltpu.VMEM, pltpu.SemaphoreType.DMA
    row = sds((M, D), bf16)
    wide = sds((M, 2 * f), bf16)
    sq = sds((D, f), f32)
    outs = [sds((dm.n_t, D + dm.hw, f), f32), sds((dm.n_t, f, D), f32), sds((f, D), f32), sds((dm.ns * dm.pairs, 2, dm.r, dm.r), bf16), sds((3 * D, D), bf16), sds((D, D), bf16), sds((dm.n_t, 16, D), f32)]
    outs += [row] * 6 + [sds((dm.ns, D, dm.r), bf16), row, wide, wide, sds((M, D), f32), sds((f, D), f32), sds((f, D), f32)]
    scratch = [vm((dm.length, 2 * dm.ns, D), bf16)] * 2 + [vm((M, D), bf16)] * 2 + [vm((3 * D, D), bf16), vm((D, D), bf16), vm((2, D, f), bf16)]
    scratch += [vm((M, D), bf16)] * 4 + [vm((dm.ns, D, dm.r), bf16), vm((M, D), bf16), vm((M, 2 * f), bf16), vm((M, 2 * f), bf16), vm((M, D), f32), vm((2, f, D), f32)]
    scratch += [vm((2, 2, dm.r, dm.r), bf16), vm((4, dm.hw, D), f32), vm((dm.n_t, 16, D), f32), vm((8, D), f32), vm((dm.n_t, 16 + 3 * dm.hw, D), f32), vm((dm.hw + D, D), f32)]
    scratch += [dma((2,)), dma((4,)), dma((2,)), dma((20,)), *([dma((GATHER_SEMS,))] * 6), dma((1,)), dma((1,))]

    def kern(*refs):
        forward_kernel(dm, n_dp, *refs)

    return pl.pallas_call(
        kern,
        out_shape=outs,
        in_specs=[SM] + [V] * (len(small) - 1) + [ANY] * len(big),
        out_specs=[ANY] * len(outs),
        scratch_shapes=scratch,
        compiler_params=pltpu.CompilerParams(vmem_limit_bytes=VMEM_LIMIT, collective_id=1, has_side_effects=True),
        name="forward",
    )(*small, *big)


class Reduce:
    KINDS = 7

    @staticmethod
    def scratch(n_arrays, n_sub, rows, width):
        pr, nq = rows // 4 // n_sub, n_arrays * n_sub
        vm, dma = pltpu.VMEM, pltpu.SemaphoreType.DMA
        return [vm((2, 2, 4 * pr, width), f32), vm((2, 7 * pr, width), f32), vm((nq, 5 * pr, width), f32), dma((2, 3, 2)), dma((2, 2)), dma((2, 11)), dma((nq, Reduce.KINDS))]

    def __init__(self, ln, head, own, sib, fin, first, n_arrays, n_sub, vin, vout, land, lsem, fsem, ssem, rsem):
        self.ln, self.head, self.own, self.sibling, self.fin, self.first = ln, head, own, sib, fin, first
        self.vin, self.vout, self.land, self.lsem, self.fsem, self.ssem, self.rsem = vin, vout, land, lsem, fsem, ssem, rsem
        self.n_sub, self.total = n_sub, n_sub * n_arrays
        self.pr = own.shape[1] // 4 // n_sub
        L, z, x = ln.length, ln.z, ln.x
        self.L = L
        self.waves = self.total + 2 * L - 1
        up = 2 * x - 1
        self.k = ((1 - x) * (L - 1 - z) + x * z, x * (L - 1 - z) + (1 - x) * z)
        self.up = ((2 * (z + up) + x, ln.t), (2 * (z - up) + x, ln.t))
        self.down = (self.up[1], self.up[0])
        self.partner = (2 * z + 1 - x, ln.t)
        self.parts = ((2 * x, 2), (2 * (1 - x) + 1, 1), (2 * (1 - x), 1))

    def rows(self, q, job, part=0, n=None):
        first, count = self.parts[job]
        r0 = lax.rem(q, self.n_sub) * 4 + first + part
        return pl.ds(pl.multiple_of(r0 * self.pr, 8), (n or count) * self.pr)

    def view(self, ref, q, job, part=0, n=None):
        return ref.at[self.first + q // self.n_sub, self.rows(q, job, part, n)]

    def box(self, q, part, n=1):
        return self.land.at[q, pl.ds(part * self.pr, n * self.pr)]

    def landed(self, view, q, kind):
        rcopy(view, view, self.ssem.at[0, 0], self.rsem.at[q, kind], self.ln.sib).wait_recv()

    def ok(self, q):
        return (q >= 0) & (q < self.total)

    def slabs(self, tau):
        return (tau - 1 - self.k[0], tau - 1 - self.k[1], tau)

    def loads(self, tau, job, views):
        par = lax.rem(tau, 2)
        n = self.parts[job][1] * self.pr
        at = pl.ds((0, 2, 3)[job] * self.pr, n)
        return [pltpu.make_async_copy(v, self.vin.at[par, i, at], self.lsem.at[par, job, i]) for i, v in enumerate(views)]

    def prefetch(self, tau):
        for job, q in enumerate(self.slabs(tau)):

            def start(refs):
                for cp in self.loads(tau, job, refs):
                    cp.start()

            @pl.when(self.ok(q))
            def _():
                pair = [self.view(r, q, job) for r in (self.own, self.sibling)]
                if self.head is None:
                    start(pair)
                    return
                pl.when(q < self.n_sub)(lambda: start([r.at[self.rows(q, job)] for r in self.head]))
                pl.when(q >= self.n_sub)(lambda: start(pair))

    def send(self, src, dst, slot, k, q, kind, dev):
        return rcopy(src, dst, self.ssem.at[slot, k], self.rsem.at[q, kind], dev)

    def wave(self, tau, start=True):
        L, pr = self.L, self.pr
        slot = lax.rem(tau, 2)
        q_both, q_one, q_leaf = self.slabs(tau)

        def run(*cps):
            for cp in cps:
                cp.start() if start else cp.wait_send()

        def out(part, n=1):
            return self.vout.at[slot, pl.ds(part * pr, n * pr)]

        def summed(job, q):
            for cp in self.loads(tau, job, [self.view(r, q, job) for r in (self.own, self.sibling)]):
                cp.wait()
            a = (0, 2, 3)[job] * pr
            n = self.parts[job][1] * pr
            return self.vin[slot, 0, a : a + n] + self.vin[slot, 1, a : a + n]

        @pl.when(self.ok(q_leaf))
        def _():
            o = out(3)
            if start:
                o[...] = summed(2, q_leaf)
            run(self.send(o, self.box(q_leaf, 3), slot, 0, q_leaf, 0, self.partner))

        for i in range(2):
            k = self.k[i]
            r = L - 1 - k
            q = tau - L - r

            @pl.when(self.ok(q) & (r > 0))
            def _():
                fv = self.view(self.fin, q, i)
                if start:
                    self.landed(fv, q, 4 if i == 0 else 6)

                @pl.when(k > 0)
                def _():
                    run(self.send(fv, fv, slot, 8 if i == 0 else 10, q, 4 if i == 0 else 6, self.down[i]))

                if i == 0:
                    fx = self.view(self.fin, q, 0, 0, 1)
                    run(self.send(fx, fx, slot, 9, q, 5, self.partner))

        for i, q in ((0, q_both), (1, q_one)):
            k = self.k[i]
            n, part = (2, 0) if i == 0 else (1, 2)

            @pl.when(self.ok(q))
            def _():
                o = out(part, n)
                if start:
                    v = summed(i, q)
                    if i == 0:
                        self.landed(self.box(q, 3), q, 0)
                        o[0:pr] = v[0:pr] + self.land[q, 3 * pr : 4 * pr]
                        o[pr : 2 * pr] = v[pr : 2 * pr]
                    else:
                        o[...] = v

                    @pl.when(k > 0)
                    def _():
                        self.landed(self.box(q, part, n), q, 1 + i)
                        o[...] += self.land[q, part * pr : (part + n) * pr]

                @pl.when(k < L - 1)
                def _():
                    run(self.send(o, self.box(q, part, n), slot, 1 if i == 0 else 5, q, 1 + i, self.up[i]))

                @pl.when(k == L - 1)
                def _():
                    z = out(part + n - 1)
                    tot = out(4 + 2 * i, n)
                    run(self.send(z, self.box(q, 4), slot, 4 if i == 0 else 6, q, 3, self.partner))
                    if start:
                        if i == 0:
                            tot[0:pr] = o[0:pr]
                        self.landed(self.box(q, 4), q, 3)
                        tot[(n - 1) * pr : n * pr] = z[...] + self.land[q, 4 * pr : 5 * pr]
                    fv = self.view(self.fin, q, i)
                    run(self.send(tot, fv, slot, 2 if i == 0 else 7, q, 4 if i == 0 else 6, self.down[i]))
                    if i == 0:
                        run(self.send(out(4), self.view(self.fin, q, 0, 0, 1), slot, 3, q, 5, self.partner))
                    cp = pltpu.make_async_copy(tot, fv, self.fsem.at[i, slot])
                    cp.start() if start else cp.wait()

    def step(self, tau):
        self.wave(tau - 2, start=False)
        self.wave(tau)

    def steps(self, t0, t1):
        def body(tau, carry):
            self.prefetch(tau + 1)
            self.step(tau)
            return carry

        lax.fori_loop(t0, t1, body, 0)

    def finish(self):
        self.wave(self.waves - 2, start=False)
        self.wave(self.waves - 1, start=False)

        def body(q, carry):
            self.landed(self.view(self.fin, q, 2), q, 5)
            return carry

        lax.fori_loop(0, self.total, body, 0)


N_SUB = (4, 4)


def backward_kernel(dm, n_dp, *refs):
    (meta, g1_r, g2_r, bd_r, wdn_s, gn_h, gu, p_hbm, i_wqkv, i_wo, i_bias, i_tok, i_cot, i_normed, i_q8, i_kk, i_vv, i_mixt, i_n2, i_act, i_gp, i_mid, d_own, d_sib, wup_s) = refs[:25]
    (fin, sm_out, lo32, gt32, own, sibl, sland) = refs[25:32]
    (wqkv, wo, wup, wdn, cot, mixt, n2, gp, act, mid, gn, dwa, acc, pbuf, tmp, bbuf, small) = refs[32:49]
    psem, tsem, lsem, osem, xss, xrs, sss, srs = refs[49:57]
    red_a, red_b = refs[57:64], refs[64:71]
    R, D, NS, hw, f = dm.r, dm.d, dm.ns, dm.hw, dm.f
    ln = Links(n_dp)
    y, c, t = ln.y, ln.c, ln.t
    base = c * NS
    nt, ft = D // 256, f // 256

    srcs = (i_gp, i_n2, i_cot, wdn_s, i_act, i_bias, i_mid, wup_s, i_wqkv, i_wo, i_mixt)
    dsts = (gp.at[:, pl.ds(0, 2 * f)], n2, cot, wdn.at[al(t, f)], act, bbuf, mid, wup.at[t], wqkv, wo, mixt)
    ins = [pltpu.make_async_copy(a, b, lsem.at[i]) for i, (a, b) in enumerate(zip(srcs, dsts))]
    late = [pltpu.make_async_copy(a, gp.at[:, pl.ds(i * D, D)], lsem.at[11 + i]) for i, a in enumerate((i_q8, i_kk, i_vv, i_normed))]
    late.append(pltpu.make_async_copy(i_tok, n2, lsem.at[15]))
    for cp in ins:
        cp.start()
    bar = pltpu.get_barrier_semaphore()
    group = ln.dp - lax.rem(ln.dp, n_dp)
    for dev in (ln.ypart, ln.sib):
        pl.semaphore_signal(bar, inc=1, device_id=dev, device_id_type=MESH)

    def greet(i, carry):
        pl.semaphore_signal(bar, inc=1, device_id=(lax.rem(ln.dp + i, n_dp), t), device_id_type=MESH)
        return carry

    lax.fori_loop(1, n_dp, greet, 0)
    pl.semaphore_wait(bar, 2 + n_dp - 1)
    red = Reduce(ln, (d_own, d_sib), own, sibl, fin, 0, 2, N_SUB[0], *red_a)
    last = Reduce(ln, None, own, sibl, fin, 2, 1, N_SUB[1], *red_b)
    def narrow(src, put):
        n = src.shape[0] // 256
        cps = [pltpu.make_async_copy(src.at[pl.ds(i * 256, 256)], tmp.at[i % 2], tsem.at[i % 2]) for i in range(n)]
        for cp in cps[:2]:
            cp.start()
        for i, cp in enumerate(cps):
            cp.wait()
            put(i * 256, 256, tmp[i % 2].astype(bf16))
            if i + 2 < n:
                cps[i + 2].start()

    def put_dn(ts, r0=0):
        def put(r, n, v):
            wdn[pl.ds(pl.multiple_of(ts * f + r0 + r, 16), n), :] = v

        return put

    def put_up(ts):
        def put(r, n, v):
            wup[ts, r : r + n, :] = v

        return put

    red.prefetch(0)
    red.step(0)
    red.prefetch(1)
    narrow(gn_h.at[ln.t_sib], put_dn(ln.t_sib))
    for cp in ins[:4]:
        cp.wait()
    acc[...] = jnp.zeros_like(acc)

    def unit(j):
        half = j // (2 * ft)
        hf = jnp.where(half == 0, y, 1 - y)
        return 2 * hf + lax.rem(j, 2 * ft) // ft, lax.rem(j, ft)

    def grad_hidden(n, block):
        def one(i):
            s, j = i // n, block(lax.rem(i, n))
            sh, k = unit(j)
            rs, cs = al(s, R), al(j, 256)
            ga = mmt(cot[rs, :], wdn[pl.ds(pl.multiple_of(sh * f + k * 256, 256), 256), :])
            gp[rs, cs] = (ga * gp[rs, cs].astype(f32)).astype(bf16)

        loop(NS * n, one)

    grad_hidden(2 * ft, lambda j: j)
    red.step(1)
    red.prefetch(2)

    def dwup(i):
        sh, j = i // nt, lax.rem(i, nt)
        for n in range(ft):
            dwa[pl.ds(pl.multiple_of(i * 256, 256), 256), n * 256 : n * 256 + 256] = tmm(n2[:, al(j, 256)], gp[:, al(sh * ft + n, 256)])

    loop(2 * nt, dwup)
    up_own = pltpu.make_async_copy(dwa.at[al(c, D)], own.at[1], osem.at[2])
    up_own.start()
    up_sib = rcopy(dwa.at[al(1 - c, D)], sibl.at[1], xss.at[0], xrs.at[0], ln.sib)
    up_sib.start()
    red.step(2)
    red.prefetch(3)
    ones = jnp.ones((8, dm.rows), bf16)
    for sh in range(2):
        acc[6 + sh, :, :f] = mm(ones, gp[:, sh * f : (sh + 1) * f]) * 0.125

    bd = bd_r[...].reshape(1, D)
    for cp in ins[4:]:
        cp.wait()

    def lo_own(s):
        rs = al(s, R)
        gn[rs, :] = mid[rs, :] + bd + mm(act[rs, :], wdn[al(y, 2 * f), :])

    loop(NS, lo_own)
    narrow(gu.at[ln.t_y, pl.ds(hw, D)], put_up(ln.t_y))
    narrow(gu.at[ln.t_ysib, pl.ds(hw, D)], put_up(ln.t_ysib))
    red.step(3)
    up_own.wait()
    up_sib.wait()
    red.prefetch(4)

    def mlp(i):
        pl.when(i == NS * ft)(lambda: red.steps(4, 5))
        s, j = i // (2 * ft), lax.rem(i, 2 * ft)
        sh, k = unit(2 * ft + j)
        rs, cs = al(s, R), al(k, 256)
        h = mm(n2[rs, :], wup[sh, :, cs]) + bbuf[sh, 0:1, cs]
        a, g = gelu_pair(h)
        act[rs, al(j, 256)] = a.astype(bf16)
        gp[rs, al(2 * ft + j, 256)] = g.astype(bf16)

    loop(NS * 2 * ft, mlp)
    narrow(gn_h.at[ln.t_y], put_dn(ln.t_y))
    red.steps(5, 6)
    narrow(gn_h.at[ln.t_ysib], put_dn(ln.t_ysib))
    narrow(gu.at[ln.t_sib, pl.ds(hw, D)], put_up(ln.t_sib))
    grad_hidden(2 * ft, lambda j: 2 * ft + j)
    red.steps(6, 7)

    def gnorm2(s):
        rs = al(s, R)
        tot = None
        for half in range(2):
            for i in range(2):
                sh = 2 * (y if half == 0 else 1 - y) + i
                k = half * 2 + i
                p = mmt(gp[rs, k * f : (k + 1) * f], wup[sh])
                tot = p if tot is None else tot + p
        lo = gn[rs, :] + mm(act[rs, :], wdn[al(1 - y, 2 * f), :])
        dwa[rs, :] = lo
        gn[rs, :] = tot

    loop(NS, gnorm2)
    lo_copies = []
    for s in range(NS):
        v = dwa.at[pl.ds(s * R, R)]
        lo_copies.append((pltpu.make_async_copy(v, lo32.at[base + s], osem.at[3 + s]), rcopy(v, lo32.at[base + s], xss.at[1 + s], xrs.at[1 + s], ln.sib)))
        for cp in lo_copies[-1]:
            cp.start()
    for cp in late:
        cp.start()
    q8, kk, vv, normed = (gp.at[:, pl.ds(i * D, D)] for i in range(4))
    tok = n2
    red.steps(7, 8)
    g2 = g2_r[...].reshape(1, D)
    g1 = g1_r[...].reshape(1, D)

    def ln2b(i):
        rs = pl.ds(pl.multiple_of(i * CH, CH), CH)
        xh, r = centred(mid[rs, :])
        go = gn[rs, :]
        co = cot[rs, :].astype(f32)
        g = go * g2
        gx = g * xh
        gm = co + r * (g - jnp.sum(g, -1, keepdims=True) * (1.0 / D) - xh * (jnp.sum(gx, -1, keepdims=True) * (1.0 / D)))
        mid[rs, :] = gm
        gl = gm.astype(bf16)
        act[rs, 0:D] = gl
        acc[0] += fold8(co)
        acc[1] += fold8(gl.astype(f32))
        acc[4] += fold8(go * xh)
        acc[5] += fold8(go)

    loop(dm.rows // CH, ln2b)

    def gmixf(s):
        rs = al(s, R)
        act[rs, D : 2 * D] = mmt(act[rs, 0:D], wo[...]).astype(bf16)

    loop(NS, gmixf)
    own_h = al(y, 2 * hw)

    def over_samples(fn):
        tot = None
        for s in range(NS):
            p = fn(s)
            tot = p if tot is None else tot + p
        return tot

    for a, b in lo_copies:
        a.wait()
        b.wait()

    for n in range(nt):
        cc = slice(n * 256, n * 256 + 256)
        p = over_samples(lambda s: mm(mixt[s, own_h, :], act[s * R : s * R + R, cc]))
        for sh in range(2):
            dwa[sh * D + 3 * hw : sh * D + 4 * hw, cc] = p[sh * hw : (sh + 1) * hw]
    red.steps(8, 9)
    for cp in late:
        cp.wait()
    lane = lax.broadcasted_iota(jnp.int32, (1, 128), 1)
    masks = (lane < HEAD_DIM, lane >= HEAD_DIM)
    total, hp = NS * dm.pairs, dm.pairs // 2

    def place(i):
        j = lax.rem(i, NS * hp)
        half = i // (NS * hp)
        hf = y + half * (1 - 2 * y)
        return j // hp, hf * hp + lax.rem(j, hp)

    def p_copy(i):
        slot = lax.rem(i, 2)
        s, p = place(i)
        return pltpu.make_async_copy(p_hbm.at[s * dm.pairs + p], pbuf.at[slot], psem.at[slot])

    p_copy(0).start()

    def attn(i):
        s, p = place(i)
        slot = lax.rem(i, 2)
        rs, cs = al(s, R), al(p, 128)

        @pl.when(i + 1 < total)
        def _():
            p_copy(i + 1).start()

        p_copy(i).wait()
        q, k, v, do = q8[rs, cs], kk[rs, cs], vv[rs, cs], act[rs, pl.ds(pl.multiple_of(D + p * 128, 128), 128)]
        dv, dk = [], []
        for h in range(2):
            pt = pbuf[slot, h]
            pf = pt.astype(f32)
            dp = mmt(jnp.where(masks[h], v, jnp.bfloat16(0)), do)
            dsum = jnp.sum(pf * dp, 0, keepdims=True)
            ds = (pf * (dp - dsum)).astype(bf16)
            dv.append(mm(pt, do))
            dk.append(mm(ds, q))
            o = tmm(k, ds)
            hr = pl.ds(pl.multiple_of(p * 128 + h * HEAD_DIM, HEAD_DIM), HEAD_DIM)
            mixt[s, hr, :] = (o[h * HEAD_DIM : (h + 1) * HEAD_DIM] * 0.125).astype(bf16)
        kk[rs, cs] = jnp.where(masks[0], dk[0], dk[1]).astype(bf16)
        vv[rs, cs] = jnp.where(masks[0], dv[0], dv[1]).astype(bf16)

    def attend(i0, i1, between):
        def one(i, carry):
            attn(i)
            for k, fn in between:
                pl.when(i == k)(fn)
            return carry

        lax.fori_loop(i0, i1, one, 0)

    half = NS * hp
    attend(0, half, [(half // 3, lambda: red.steps(9, 10)), (half * 2 // 3, lambda: red.steps(10, 11))])
    for n in range(nt):
        cc = slice(n * 256, n * 256 + 256)
        p = over_samples(lambda s: mm(mixt[s, own_h, :], normed[s * R : s * R + R, cc]))
        tk = tmm(kk[:, own_h], normed[:, cc])
        tv = tmm(vv[:, own_h], normed[:, cc])
        for sh in range(2):
            h = slice(sh * hw, (sh + 1) * hw)
            dwa[sh * D : sh * D + hw, cc] = p[h]
            dwa[sh * D + hw : sh * D + 2 * hw, cc] = tk[h]
            dwa[sh * D + 2 * hw : sh * D + 3 * hw, cc] = tv[h]
    a_own = pltpu.make_async_copy(dwa.at[al(c, D)], own.at[2], osem.at[2])
    a_own.start()
    a_sib = rcopy(dwa.at[al(1 - c, D)], sibl.at[2], xss.at[5], xrs.at[5], ln.sib)
    a_sib.start()
    onesr = jnp.ones((8, R), bf16)
    acc[8, :, 0 : 2 * hw] = over_samples(lambda s: mmt(onesr, mixt[s, own_h, :])) * 0.125
    acc[9, :, 0 : 2 * hw] = mm(ones, vv[:, own_h]) * 0.125
    red.steps(11, 12)
    a_own.wait()
    a_sib.wait()
    last.prefetch(0)
    attend(
        half,
        total,
        [
            (half + 1, lambda: last.steps(0, 1)),
            (half * 4 // 3, lambda: red.steps(12, red.waves - 1)),
            (half * 5 // 3, lambda: last.steps(1, 2)),
        ],
    )
    red.steps(red.waves - 1, red.waves)
    red.finish()
    last.steps(2, 3)

    def gnorm1(s):
        rs = al(s, R)
        gn[rs, :] = tmm(mixt[s], wqkv[0:D, :]) + mm(kk[rs, :], wqkv[D : 2 * D, :]) + mm(vv[rs, :], wqkv[2 * D : 3 * D, :])

    loop(NS, gnorm1)
    last.steps(3, 4)

    def ln1b(s):
        for r0, n in row_chunks(dm):
            rs = pl.ds(pl.multiple_of(s * R + r0, 16), n)
            x = tok[rs, :].astype(f32)
            keep = keep_of(meta, base, s, r0, n) if r0 == 0 else None
            xh, r = centred(x if keep is None else x * keep)
            go = gn[rs, :]
            g = go * g1
            gx = g * xh
            gi = r * (g - jnp.sum(g, -1, keepdims=True) * (1.0 / D) - xh * (jnp.sum(gx, -1, keepdims=True) * (1.0 / D)))
            o = mid[rs, :] + gi
            mid[rs, :] = o if keep is None else o * keep
            acc[2] += fold8(go * xh)
            acc[3] += fold8(go)

    loop(NS, ln1b)
    gt_copies = []
    for s in range(NS):
        v = mid.at[pl.ds(s * R, R)]
        gt_copies.append((pltpu.make_async_copy(v, gt32.at[base + s], osem.at[3 + s]), rcopy(v, gt32.at[base + s], xss.at[6 + s], xrs.at[6 + s], ln.sib)))
        for cp in gt_copies[-1]:
            cp.start()

    tot = jnp.sum(acc[...], 1)
    for sh in range(2):
        small[sh, 0:6, :] = tot[0:6]
        small[sh, 6:7, :] = tot[6 + sh : 7 + sh]
        small[sh, 7:8, 0:hw] = tot[8:9, sh * hw : (sh + 1) * hw]
        small[sh, 7:8, hw : 2 * hw] = tot[9:10, sh * hw : (sh + 1) * hw]
        small[sh, 7:8, 2 * hw :] = jnp.zeros((1, D - 2 * hw), f32)
    cp = rcopy(small.at[1 - c], small.at[2], xss.at[10], xrs.at[10], ln.sib)
    cp.start()
    cp.wait()
    small[2] = small[c] + small[2]
    mine = sland.at[al(ln.dp, 8)]
    kept = pltpu.make_async_copy(small.at[2], mine, osem.at[0])
    kept.start()

    def peer(i):
        d = lax.rem(ln.dp + i, n_dp)
        return rcopy(small.at[2], mine, sss.at[d], srs.at[ln.dp], (d, t))

    def spread(i, carry):
        peer(i).start()
        return carry

    lax.fori_loop(1, n_dp, spread, 0)
    last.steps(4, last.waves)
    last.finish()

    def gathered(i, carry):
        peer(i).wait_send()
        d = lax.rem(ln.dp + i, n_dp)
        theirs = sland.at[al(d, 8)]
        rcopy(theirs, theirs, sss.at[d], srs.at[d], (d, t)).wait_recv()
        return carry

    lax.fori_loop(1, n_dp, gathered, 0)
    kept.wait()
    back = pltpu.make_async_copy(sland, dwa.at[pl.ds(0, 8 * n_dp)], osem.at[0])
    back.start()
    back.wait()
    sm_out[...] = lax.fori_loop(1, n_dp, lambda i, v: v + dwa[al(i, 8), :], dwa[0:8, :])
    for a, b in gt_copies:
        a.wait()
        b.wait()


def backward_call(dm, n_dp, small, big):
    M, D, f = dm.rows, dm.d, dm.f
    sds, vm, dma = jax.ShapeDtypeStruct, pltpu.VMEM, pltpu.SemaphoreType.DMA
    st = sds((3, D, D), f32)
    outs = [st, sds((8, D), f32), sds((dm.samples, dm.r, D), f32), sds((dm.samples, dm.r, D), f32), st, st, sds((8 * n_dp, D), f32)]
    row, wide = vm((M, D), bf16), vm((M, 2 * f), bf16)
    scratch = [vm((3 * D, D), bf16), vm((D, D), bf16), vm((dm.n_t, D, f), bf16), vm((dm.ff, D), bf16), row]
    scratch += [vm((dm.ns, D, dm.r), bf16), row, vm((M, dm.ff), bf16), wide, vm((M, D), f32), vm((M, D), f32), vm((2 * D, D), f32), vm((10, 8, D), f32)]
    scratch += [vm((2, 2, dm.r, dm.r), bf16), vm((2, 256, D), f32), vm((dm.n_t, 16, D), f32), vm((3, 8, D), f32)]
    scratch += [dma((2,)), dma((2,)), dma((16,)), dma((7,)), dma((11,)), dma((11,)), dma((n_dp,)), dma((n_dp,))]
    scratch += Reduce.scratch(2, N_SUB[0], D, D) + Reduce.scratch(1, N_SUB[1], D, D)

    def kern(*refs):
        backward_kernel(dm, n_dp, *refs)

    return pl.pallas_call(
        kern,
        out_shape=outs,
        in_specs=[SM] + [V] * (len(small) - 1) + [ANY] * len(big),
        out_specs=[ANY, V] + [ANY] * 5,
        scratch_shapes=scratch,
        compiler_params=pltpu.CompilerParams(vmem_limit_bytes=VMEM_LIMIT, collective_id=2, has_side_effects=True),
        name="backward",
    )(*small, *big)


def shards(tokens, metadata, cotangent, w_query, w_key, w_value, w_out, b_query, b_value, b_out, w_up, b_up, w_down, b_down, gain_one, shift_one, gain_two, shift_two, n_dp, n_t):
    dm = Dims(tokens, w_up, n_t)
    D, hw, f = dm.d, dm.hw, dm.f
    small = (metadata, w_query.T, w_key.T, w_value.T, w_out, w_up, w_down, b_up, b_query, b_value, gain_one, shift_one, gain_two, shift_two, b_out)
    (gu, gnw, _, p, wqkv, wo, bb, tok, cot, normed, q8, kk, vv, mixt, n2, act, gp, mid, d_own, d_sib) = forward_call(dm, n_dp, small, (tokens.transpose(1, 0, 2), cotangent.transpose(1, 0, 2)))
    small = (metadata, gain_one, gain_two, b_down)
    fin, sm, lo, gt, *_ = backward_call(dm, n_dp, small, (w_down, gnw, gu, p, wqkv, wo, bb, tok, cot, normed, q8, kk, vv, mixt, n2, act, gp, mid, d_own, d_sib, w_up))
    a_ = fin[2]
    return (
        lo[:, : dm.length].astype(bf16),
        gt[:, : dm.length],
        a_[0:hw].T,
        a_[hw : 2 * hw].T,
        a_[2 * hw : 3 * hw].T,
        a_[3 * hw : 4 * hw],
        sm[7, :hw],
        sm[7, hw : 2 * hw],
        sm[1],
        fin[1],
        sm[6],
        fin[0],
        sm[0],
        sm[2],
        sm[3],
        sm[4],
        sm[5],
    )


def solution(mesh):
    n_dp, n_t = mesh.shape["dp"], mesh.shape["tensor"]
    rows, cols, vec, rep = P("dp", None, None), P(None, "tensor"), P("tensor"), P()
    srow = P("tensor", None)

    def run(*args):
        return shards(*args, n_dp=n_dp, n_t=n_t)

    return jax.shard_map(
        run,
        mesh=mesh,
        in_specs=(rows, P("dp"), rows, cols, cols, cols, srow, vec, vec, rep, cols, vec, srow, rep, rep, rep, rep, rep),
        out_specs=(rows, rows, cols, cols, cols, srow, vec, vec, rep, cols, vec, srow, rep, rep, rep, rep, rep),
        check_vma=False,
    )
```

```python
import math

import jax
import jax.numpy as jnp
from jax import lax
from jax.experimental import pallas as pl
from jax.experimental.pallas import tpu as pltpu
from jax.sharding import PartitionSpec as P

HEAD_DIM = 64
EPS = 1e-05
MESH = pl.DeviceIdType.MESH
f32 = jnp.float32
bf16 = jnp.bfloat16
VMEM_LIMIT = 63 << 20
RING = 8
CH = 64
TAIL_P = 0.24
TAIL = (
    0.08952743306829739,
    0.15551359433427508,
    -0.15404885518029288,
    0.6255903019940591,
    -0.6460706945688248,
    0.5545739487327468,
    -0.12508572868970558,
)
INV_SQRT_2PI = 1.0 / math.sqrt(2.0 * math.pi)
HALF_LOG2E = -0.5 / math.log(2.0)


def mm(a, b):
    return lax.dot_general(a, b, (((1,), (0,)), ((), ())), preferred_element_type=f32)


def mmt(a, b):
    return lax.dot_general(a, b, (((1,), (1,)), ((), ())), preferred_element_type=f32)


def tmm(a, b):
    return lax.dot_general(a, b, (((0,), (0,)), ((), ())), preferred_element_type=f32)


def loop(n, fn):
    def body(i, carry):
        fn(i)
        return carry

    lax.fori_loop(0, n, body, 0)


def al(i, step):
    return pl.ds(pl.multiple_of(i * step, step), step)


def centred(x):
    d = x.shape[-1]
    mu = jnp.sum(x, -1, keepdims=True) * (1.0 / d)
    xm = x - mu
    var = jnp.sum(xm * xm, -1, keepdims=True) * (1.0 / d)
    r = lax.rsqrt(var + EPS)
    return xm * r, r


def gelu_pair(v):
    d = 1.0 + TAIL_P * jnp.abs(v)
    t = pltpu.reciprocal(d, approx=True)
    t = t * (2.0 - d * t)
    e = jnp.exp2(HALF_LOG2E * (v * v))
    acc = TAIL[6] * t + TAIL[5]
    for k in range(4, -1, -1):
        acc = acc * t + TAIL[k]
    q = (acc * t) * e
    cdf = jnp.where(v < 0, q, 1.0 - q)
    return v * cdf, cdf + (v * e) * INV_SQRT_2PI


def fold8(x):
    return jnp.sum(x.reshape(x.shape[0] // 8, 8, x.shape[1]), 0)


class Dims:
    def __init__(self, tokens, w_up, n_t):
        self.samples, self.length, self.d = tokens.shape
        self.ns = self.samples // 2
        self.r = -(-self.length // 16) * 16
        self.rp = -(-self.r // 128) * 128
        self.rows = self.ns * self.r
        self.f = w_up.shape[1]
        self.ff = self.f * n_t
        self.n_t = n_t
        self.heads = self.d // HEAD_DIM
        self.pairs = self.heads // 2
        self.hw = self.d // n_t


class Links:
    def __init__(self, n_dp):
        self.n_dp = n_dp
        self.dp = lax.axis_index("dp")
        self.t = lax.axis_index("tensor")
        self.y, self.c = self.t // 2, lax.rem(self.t, 2)
        self.z, self.x = self.dp // 2, lax.rem(self.dp, 2)
        self.length = n_dp // 2
        self.sib = (self.dp, 2 * self.y + 1 - self.c)
        self.ypart = (self.dp, 2 * (1 - self.y) + self.c)
        self.t_sib = 2 * self.y + 1 - self.c
        self.t_y = 2 * (1 - self.y) + self.c
        self.t_ysib = 2 * (1 - self.y) + 1 - self.c
        g = lax.rem(self.dp, RING)
        half = RING // 2
        zz, xx = g // 2, lax.rem(g, 2)
        self.pos = jnp.where(xx == 0, zz, RING - 1 - zz)
        base = self.dp - g

        def at(pos):
            pos = lax.rem(pos + RING, RING)
            local = jnp.where(pos < half, 2 * pos, 2 * (RING - 1 - pos) + 1)
            return (base + local, self.t)

        self.step = 1 - 2 * self.c
        self.ahead, self.behind = at(self.pos + self.step), at(self.pos - self.step)

    def piece(self, offset):
        return lax.rem(self.pos + offset * self.step + RING, RING)


def rcopy(src, dst, ssem, rsem, dev):
    return pltpu.make_async_remote_copy(src_ref=src, dst_ref=dst, send_sem=ssem, recv_sem=rsem, device_id=dev, device_id_type=MESH)


def enter(devs):
    bar = pltpu.get_barrier_semaphore()
    for d in devs:
        pl.semaphore_signal(bar, inc=1, device_id=d, device_id_type=MESH)
    pl.semaphore_wait(bar, len(devs))


class Gather:
    def __init__(self, ln, src, out, direct, ssem, rsem):
        self.ln, self.src, self.out, self.direct = ln, src, out, direct
        self.ssem, self.rsem = ssem, rsem
        self.passed = self.passed_sib = False
        self.rows = src.shape[0]
        self.piece_rows = (self.rows - direct) // RING

    def at(self, ref, offset):
        return ref.at[pl.ds(pl.multiple_of(self.direct + self.ln.piece(offset) * self.piece_rows, 8), self.piece_rows)]

    def copy(self, src, dst, k, dev):
        return rcopy(src, dst, self.ssem.at[k], self.rsem.at[k], dev)

    def landed(self, view, k):
        rcopy(view, view, self.ssem.at[k], self.rsem.at[k], self.ln.sib).wait_recv()

    def spread_y(self):
        return self.copy(self.at(self.src, 0), self.at(self.out.at[self.ln.t], 0), 0, self.ln.ypart)

    def direct_y(self):
        d = pl.ds(0, self.direct)
        return self.copy(self.src.at[d], self.out.at[self.ln.t].at[d], 1, self.ln.ypart)

    def whole_sib(self):
        return self.copy(self.src, self.out.at[self.ln.t], 2, self.ln.sib)

    def start_y(self):
        self.spread_y().start()
        self.direct_y().start()

    def start_sib(self):
        self.whole_sib().start()

    def wait_sib(self):
        self.landed(self.out.at[self.ln.t_sib], 2)

    def to_sib(self, offset):
        v = self.at(self.out.at[self.ln.t_y], offset)
        return self.copy(v, v, 11 + 4 + offset, self.ln.sib)

    def direct_sib(self):
        v = self.out.at[self.ln.t_y].at[pl.ds(0, self.direct)]
        return self.copy(v, v, 10, self.ln.sib)

    def ring_ahead(self, s):
        v = self.at(self.out.at[self.ln.t_y], -s)
        return self.copy(v, v, 3 + s, self.ln.ahead)

    def ring_behind(self, s):
        v = self.at(self.out.at[self.ln.t_y], s)
        return self.copy(v, v, 7 + s, self.ln.behind)

    def tick(self, i):
        ln, out = self.ln, self.out.at[self.ln.t_y]
        if i == 0:
            self.landed(self.at(out, 0), 0)
            self.ring_ahead(0).start()
            self.ring_behind(0).start()
            self.to_sib(0).start()
            return
        s = i - 1
        self.landed(self.at(out, -s - 1), 3 + s)
        if s < 3:
            self.ring_ahead(s + 1).start()
            self.landed(self.at(out, s + 1), 7 + s)
            if s < 2:
                self.ring_behind(s + 1).start()
        self.to_sib(-s - 1).start()
        if s < 3:
            self.to_sib(s + 1).start()

    def direct_landed(self):
        if not self.passed:
            self.passed = True
            self.landed(self.out.at[self.ln.t_y].at[pl.ds(0, self.direct)], 1)
            self.direct_sib().start()

    def direct_sib_landed(self):
        if not self.passed_sib:
            self.passed_sib = True
            self.landed(self.out.at[self.ln.t_ysib].at[pl.ds(0, self.direct)], 10)

    def finish(self):
        ln, out = self.ln, self.out.at[self.ln.t_ysib]
        for offset in range(-4, 4):
            v = out.at[pl.ds(pl.multiple_of(self.direct + lax.rem(ln.pos - offset * ln.step + RING, RING) * self.piece_rows, 8), self.piece_rows)]
            self.landed(v, 11 + 4 + offset)
        self.direct_sib_landed()

    def drain(self):
        cps = [self.spread_y(), self.direct_y(), self.whole_sib(), self.direct_sib()]
        cps += [self.ring_ahead(s) for s in range(4)] + [self.ring_behind(s) for s in range(3)]
        cps += [self.to_sib(o) for o in range(-4, 4)]
        for cp in cps:
            cp.wait_send()


GATHER_SEMS = 19


def keep_of(meta, base, s, r0, n):
    rows = lax.broadcasted_iota(jnp.int32, (n, 1), 0) + r0
    return jnp.where(rows == 1, meta[base + s].astype(f32), 1.0)


def row_chunks(dm):
    out, r = [], 0
    while r < dm.r:
        n = min(CH, dm.r - r)
        out.append((r, n))
        r += n
    return out


def forward_kernel(dm, n_dp, *refs):
    (meta, wq, wk, wv, wo_s, wup_s, wdn_s, bup_r, bq_r, bv_r, g1_r, s1_r, g2_r, s2_r, bo_r, tokens, cotan) = refs[:17]
    (gu, gn_h, n32, p_hbm, o_wqkv, o_wo, o_wup, o_bias, o_tok, o_cot, o_normed, o_q8, o_kk, o_vv, o_mixt, o_n2, o_act, o_gp, o_mid, d_own, d_sib) = refs[17:38]
    (tok3, cot3, tok, cot, wqkv, wo, wup, normed, q8, kk, vv, mixt, n2, act, gp, mid, dwd, pbuf, tmp, bbuf, bqv, ga, ustage) = refs[38:61]
    psem, tsem, lsem, osem, ssa, rsa, ssu, rsu, ssn, rsn, ssd, rsd = refs[61:]
    R, D, NS, hw, f = dm.r, dm.d, dm.ns, dm.hw, dm.f
    ln = Links(n_dp)
    y, c, t = ln.y, ln.c, ln.t
    base = c * NS

    def row(ref):
        return ref[...].reshape(1, D)

    loads = [pltpu.make_async_copy(tokens, tok3, lsem.at[0]), pltpu.make_async_copy(cotan, cot3, lsem.at[1])]
    for cp in loads:
        cp.start()
    outs = []

    def put(src, dst):
        cp = pltpu.make_async_copy(src, dst, osem.at[len(outs)])
        cp.start()
        outs.append(cp)

    own_a = mid.at[pl.ds(0, 16 + 3 * hw)]
    mid[0:16, :] = jnp.zeros((16, D), f32)
    mid[0:1, 0:f] = bup_r[...].reshape(1, f)
    mid[1:2, 0:hw] = bq_r[...].reshape(1, hw)
    mid[1:2, hw : 2 * hw] = bv_r[...].reshape(1, hw)
    bbuf[t] = mid[0:16, :]
    for i, w in enumerate((wq, wk, wv)):
        mid[16 + i * hw : 16 + (i + 1) * hw, :] = w[...].astype(f32)
        wqkv[pl.ds(pl.multiple_of(i * D + t * hw, 16), hw), :] = w[...]
    wo[al(t, hw), :] = wo_s[...]
    g_a = Gather(ln, own_a, ga, 16 + hw, ssa, rsa)
    g_u = Gather(ln, ustage, gu, hw + D // 3, ssu, rsu)
    g_n = Gather(ln, n32, gn_h, D // 4, ssn, rsn)
    enter((ln.ypart, ln.sib, ln.ahead, ln.behind))
    g_a.start_y()
    g_a.start_sib()
    ustage[0:hw, :] = wo_s[...].astype(f32)

    def widen(i):
        rs = al(i, 64)
        ustage[pl.ds(pl.multiple_of(hw + i * 64, 64), 64), :] = wup_s[rs, :].astype(f32)
        dwd[1, rs, :] = wdn_s[rs, :].astype(f32)
        wup[c, rs, :] = wup_s[rs, :]

    loop(D // 64, widen)
    put(dwd.at[1], n32)
    g_u.spread_y().start()
    outs[0].wait()
    g_n.spread_y().start()
    g_u.direct_y().start()
    g_n.direct_y().start()
    g_u.start_sib()
    g_n.start_sib()

    for cp in loads:
        cp.wait()
    g1, s1, g2, s2, bo = (row(r) for r in (g1_r, s1_r, g2_r, s2_r, bo_r))
    grp = dm.length // 32
    rest, pad = dm.length - grp * 32, R - grp * 32

    def selection(n_out, n_in):
        r = lax.broadcasted_iota(jnp.int32, (NS * n_out, n_in * 2 * NS), 0)
        col = lax.broadcasted_iota(jnp.int32, (NS * n_out, n_in * 2 * NS), 1)
        hit = (col == lax.rem(r, n_out) * (2 * NS) + base + r // n_out) & (lax.rem(r, n_out) < n_in)
        return jnp.where(hit, 1.0, 0.0).astype(bf16)

    sel = selection(32, 32)

    def regroup(g):
        for src, dst in ((tok3, tok), (cot3, cot)):
            v = src[al(g, 32)].astype(f32).reshape(32 * 2 * NS, D).astype(bf16)
            o = mm(sel, v).astype(bf16)
            for s in range(NS):
                dst[pl.ds(pl.multiple_of(s * R + g * 32, 16), 32), :] = o[s * 32 : (s + 1) * 32]

    loop(grp, regroup)
    if pad:
        sel_end = selection(pad, rest)
        for src, dst in ((tok3, tok), (cot3, cot)):
            v = src[grp * 32 : grp * 32 + rest].astype(f32).reshape(rest * 2 * NS, D).astype(bf16)
            o = mm(sel_end, v).astype(bf16)
            for s in range(NS):
                dst[s * R + grp * 32 : (s + 1) * R, :] = o[s * pad : (s + 1) * pad]
    put(tok, o_tok)
    put(cot, o_cot)

    def ln1(s):
        for r, n in row_chunks(dm):
            rs = pl.ds(pl.multiple_of(s * R + r, 16), n)
            x = tok[rs, :].astype(f32)
            if r == 0:
                x = x * keep_of(meta, base, s, r, n)
            xh, _ = centred(x)
            normed[rs, :] = (xh * g1 + s1).astype(bf16)

    loop(NS, ln1)
    put(normed, o_normed)

    def fetch(src, k):
        cp = pltpu.make_async_copy(src, tmp.at[k], tsem.at[k])
        cp.start()
        return cp

    def take_a(tp):
        bbuf[tp] = ga[tp, 0:16, :]
        for i in range(3):
            wqkv[pl.ds(pl.multiple_of(i * D + tp * hw, 16), hw), :] = ga[tp, 16 + i * hw : 16 + (i + 1) * hw, :].astype(bf16)

    lane = lax.broadcasted_iota(jnp.int32, (1, 128), 1)
    masks = (lane < HEAD_DIM, lane >= HEAD_DIM)
    hp = dm.pairs // 2
    tail = R - 16
    live = lax.broadcasted_iota(jnp.int32, (16, 1), 0) < dm.length - tail

    def project(hf):
        for i in range(2):
            b = bbuf[2 * hf + i]
            bqv[0:1, i * hw : (i + 1) * hw] = b[1:2, 0:hw]
            bqv[1:2, i * hw : (i + 1) * hw] = b[1:2, hw : 2 * hw]
        cs = al(hf, 2 * hw)

        def one(s):
            rs = al(s, R)
            n = normed[rs, :]
            w = [wqkv[pl.ds(pl.multiple_of(i * D + hf * 2 * hw, 128), 2 * hw), :] for i in range(3)]
            q8[rs, cs] = (mmt(n, w[0]) + bqv[0:1, : 2 * hw]).astype(bf16) * jnp.bfloat16(0.125)
            kk[rs, cs] = mmt(n, w[1]).astype(bf16)
            vv[rs, cs] = (mmt(n, w[2]) + bqv[1:2, : 2 * hw]).astype(bf16)

        loop(NS, one)

    def p_copy(hf, i):
        slot = lax.rem(i, 2)
        return pltpu.make_async_copy(pbuf.at[slot], p_hbm.at[(i // hp) * dm.pairs + hf * hp + lax.rem(i, hp)], psem.at[slot])

    def attend(hf, ticks):
        total = NS * hp

        def one(i):
            s, p = i // hp, hf * hp + lax.rem(i, hp)
            slot = lax.rem(i, 2)
            rs, cs = al(s, R), al(p, 128)
            for k, fn in ticks:
                pl.when(i == k)(fn)

            @pl.when(i >= 2)
            def _():
                p_copy(hf, i - 2).wait()

            q, k, v = q8[rs, cs], kk[rs, cs], vv[rs, cs]
            for h in range(2):
                st = mmt(jnp.where(masks[h], k, jnp.bfloat16(0)), q)
                sa = st[:tail]
                sb = jnp.where(live, st[tail:], -1e30)
                m = jnp.maximum(jnp.max(sa, 0, keepdims=True), jnp.max(sb, 0, keepdims=True))
                ea, eb = jnp.exp(sa - m), jnp.exp(sb - m)
                inv = 1.0 / (jnp.sum(ea, 0, keepdims=True) + jnp.sum(eb, 0, keepdims=True))
                pbuf[slot, h * R : h * R + tail, 0:R] = (ea * inv).astype(bf16)
                pbuf[slot, h * R + tail : (h + 1) * R, 0:R] = (eb * inv).astype(bf16)
                o = tmm(v, pbuf[slot, h * R : (h + 1) * R, 0:R])
                hr = pl.ds(pl.multiple_of(p * 128 + h * HEAD_DIM, HEAD_DIM), HEAD_DIM)
                mixt[s, hr, :] = o[h * HEAD_DIM : (h + 1) * HEAD_DIM].astype(bf16)
            p_copy(hf, i).start()

        loop(total, one)
        p_copy(hf, total - 2).wait()
        p_copy(hf, total - 1).wait()

    g_a.wait_sib()
    take_a(ln.t_sib)
    g_a.tick(0)
    project(y)
    g_a.tick(1)
    attend(y, [(3, lambda: g_a.tick(2)), (9, lambda: g_a.tick(3))])
    g_a.tick(4)
    g_a.direct_landed()
    g_a.finish()
    take_a(ln.t_y)
    take_a(ln.t_ysib)
    put(wqkv, o_wqkv)
    put(bbuf, o_bias)
    g_u.tick(0)
    project(1 - y)
    put(q8, o_q8)
    put(kk, o_kk)
    put(vv, o_vv)
    g_n.tick(0)

    def both(i):
        g_u.tick(i)
        g_n.tick(i)

    attend(1 - y, [(2, lambda: both(1)), (10, lambda: both(2))])
    put(mixt, o_mixt)
    g_a.drain()
    g_u.direct_landed()
    wo_rows = [fetch(gu.at[tp, pl.ds(0, hw)], i) for i, tp in enumerate((ln.t_y,))]
    g_u.wait_sib()
    wo_rows.append(fetch(gu.at[ln.t_sib, pl.ds(0, hw)], 1))
    g_u.direct_sib_landed()
    wo_rows.append(fetch(gu.at[ln.t_ysib, pl.ds(0, hw)], 2))
    for i, tp in enumerate((ln.t_y, ln.t_sib, ln.t_ysib)):
        wo_rows[i].wait()
        wo[al(tp, hw), :] = tmp[i].astype(bf16)
    put(wo, o_wo)
    ups = [fetch(gu.at[ln.t_sib, pl.ds((i + 1) * hw, hw)], i) for i in range(4)]

    def outp(s):
        rs = al(s, R)
        mid[rs, :] = tmm(mixt[s], wo[...])

    loop(NS, outp)

    def ln2(s):
        for r, n in row_chunks(dm):
            rs = pl.ds(pl.multiple_of(s * R + r, 16), n)
            x = tok[rs, :].astype(f32)
            if r == 0:
                x = x * keep_of(meta, base, s, r, n)
            m = x + (mid[rs, :] + bo)
            mid[rs, :] = m
            xh, _ = centred(m)
            n2[rs, :] = (xh * g2 + s2).astype(bf16)

    both(3)
    loop(NS, ln2)
    put(mid, o_mid)
    put(n2, o_n2)
    for i in range(4):
        ups[i].wait()
        wup[1 - c, i * hw : (i + 1) * hw, :] = tmp[i].astype(bf16)
    put(wup, o_wup)
    ft = f // 256
    tw = 384 if f % 384 == 0 else 256
    mt = f // tw

    def mlp(i):
        pl.when(i == NS * 2)(lambda: both(4))
        s, j = i // (2 * mt), lax.rem(i, 2 * mt)
        rs, sh, cs = al(s, R), j // mt, al(lax.rem(j, mt), tw)
        h = mm(n2[rs, :], wup[sh, :, cs]) + bbuf[2 * y + sh, 0:1, cs]
        a, g = gelu_pair(h)
        act[rs, al(j, tw)] = a.astype(bf16)
        gp[rs, al(j, tw)] = g.astype(bf16)

    loop(NS * 2 * mt, mlp)
    put(act, o_act)
    put(gp, o_gp)

    def dwdn(sh):
        def one(j):
            dwd[sh, al(j, 256), :] = tmm(act[:, al(sh * ft + j, 256)], cot[...])

        loop(ft, one)

    dwdn(1 - c)
    ex = rcopy(dwd.at[1 - c], d_sib, ssd.at[0], rsd.at[0], ln.sib)
    ex.start()
    dwdn(c)
    put(dwd.at[c], d_own)
    g_u.finish()
    g_n.direct_landed()
    g_n.wait_sib()
    g_n.finish()
    g_u.drain()
    g_n.drain()
    ex.wait()
    for cp in outs[1:]:
        cp.wait()


V = pl.BlockSpec(memory_space=pltpu.VMEM)
ANY = pl.BlockSpec(memory_space=pl.ANY)
SM = pl.BlockSpec(memory_space=pltpu.SMEM)


def forward_call(dm, n_dp, small, big):
    M, D, f = dm.rows, dm.d, dm.f
    sds, vm, dma = jax.ShapeDtypeStruct, pltpu.VMEM, pltpu.SemaphoreType.DMA
    row = sds((M, D), bf16)
    wide = sds((M, 2 * f), bf16)
    sq = sds((D, f), f32)
    outs = [sds((dm.n_t, D + dm.hw, f), f32), sds((dm.n_t, f, D), f32), sds((f, D), f32), sds((dm.ns * dm.pairs, 2 * dm.r, dm.rp), bf16), sds((3 * D, D), bf16), sds((D, D), bf16), sds((2, D, f), bf16), sds((dm.n_t, 16, D), f32)]
    outs += [row] * 6 + [sds((dm.ns, D, dm.r), bf16), row, wide, wide, sds((M, D), f32), sds((f, D), f32), sds((f, D), f32)]
    scratch = [vm((dm.length, 2 * dm.ns, D), bf16)] * 2 + [vm((M, D), bf16)] * 2 + [vm((3 * D, D), bf16), vm((D, D), bf16), vm((2, D, f), bf16)]
    scratch += [vm((M, D), bf16)] * 4 + [vm((dm.ns, D, dm.r), bf16), vm((M, D), bf16), vm((M, 2 * f), bf16), vm((M, 2 * f), bf16), vm((M, D), f32), vm((2, f, D), f32)]
    scratch += [vm((2, 2 * dm.r, dm.rp), bf16), vm((4, dm.hw, D), f32), vm((dm.n_t, 16, D), f32), vm((8, D), f32), vm((dm.n_t, 16 + 3 * dm.hw, D), f32), vm((dm.hw + D, D), f32)]
    scratch += [dma((2,)), dma((4,)), dma((2,)), dma((20,)), *([dma((GATHER_SEMS,))] * 6), dma((1,)), dma((1,))]

    def kern(*refs):
        forward_kernel(dm, n_dp, *refs)

    return pl.pallas_call(
        kern,
        out_shape=outs,
        in_specs=[SM] + [V] * (len(small) - 1) + [ANY] * len(big),
        out_specs=[ANY] * len(outs),
        scratch_shapes=scratch,
        compiler_params=pltpu.CompilerParams(vmem_limit_bytes=VMEM_LIMIT, collective_id=1, has_side_effects=True),
        name="forward",
    )(*small, *big)


class Reduce:
    KINDS = 7

    @staticmethod
    def scratch(n_arrays, n_sub, rows, width):
        pr, nq = rows // 4 // n_sub, n_arrays * n_sub
        vm, dma = pltpu.VMEM, pltpu.SemaphoreType.DMA
        return [vm((2, 2, 4 * pr, width), f32), vm((2, 7 * pr, width), f32), vm((nq, 5 * pr, width), f32), dma((2, 3, 2)), dma((2, 2)), dma((2, 11)), dma((nq, Reduce.KINDS))]

    def __init__(self, ln, head, own, sib, fin, height, n_arrays, n_sub, vin, vout, land, lsem, fsem, ssem, rsem):
        self.ln, self.head, self.own, self.sibling, self.fin = ln, head, own, sib, fin
        self.vin, self.vout, self.land, self.lsem, self.fsem, self.ssem, self.rsem = vin, vout, land, lsem, fsem, ssem, rsem
        self.n_sub, self.total = n_sub, n_sub * n_arrays
        self.pr = height // 4 // n_sub
        L, z, x = ln.length, ln.z, ln.x
        self.L = L
        self.waves = self.total + 2 * L
        up = 2 * x - 1
        self.k = ((1 - x) * (L - 1 - z) + x * z, x * (L - 1 - z) + (1 - x) * z)
        self.up = ((2 * (z + up) + x, ln.t), (2 * (z - up) + x, ln.t))
        self.down = (self.up[1], self.up[0])
        self.partner = (2 * z + 1 - x, ln.t)
        self.parts = ((2 * x, 2), (2 * (1 - x) + 1, 1), (2 * (1 - x), 1))

    def rows(self, q, job, part=0, n=None):
        first, count = self.parts[job]
        return pl.ds(pl.multiple_of((q * 4 + first + part) * self.pr, 8), (n or count) * self.pr)

    def view(self, ref, q, job, part=0, n=None):
        return ref.at[self.rows(q, job, part, n)]

    def box(self, q, part, n=1):
        return self.land.at[q, pl.ds(part * self.pr, n * self.pr)]

    def landed(self, view, q, kind):
        rcopy(view, view, self.ssem.at[0, 0], self.rsem.at[q, kind], self.ln.sib).wait_recv()

    def ok(self, q):
        return (q >= 0) & (q < self.total)

    def slabs(self, tau):
        return (tau - 1 - self.k[0], tau - 1 - self.k[1], tau)

    def loads(self, tau, job, views):
        par = lax.rem(tau, 2)
        n = self.parts[job][1] * self.pr
        at = pl.ds((0, 2, 3)[job] * self.pr, n)
        return [pltpu.make_async_copy(v, self.vin.at[par, i, at], self.lsem.at[par, job, i]) for i, v in enumerate(views)]

    def prefetch(self, tau):
        for job, q in enumerate(self.slabs(tau)):

            def start(refs):
                for cp in self.loads(tau, job, refs):
                    cp.start()

            @pl.when(self.ok(q))
            def _():
                pair = [self.view(r, q, job) for r in (self.own, self.sibling)]
                if self.head is None:
                    start(pair)
                    return
                pl.when(q < self.n_sub)(lambda: start([r.at[self.rows(q, job)] for r in self.head]))
                pl.when(q >= self.n_sub)(lambda: start(pair))

    def send(self, src, dst, slot, k, q, kind, dev):
        return rcopy(src, dst, self.ssem.at[slot, k], self.rsem.at[q, kind], dev)

    def wave(self, tau, start=True):
        L, pr = self.L, self.pr
        slot = lax.rem(tau, 2)
        q_both, q_one, q_leaf = self.slabs(tau)

        def run(*cps):
            for cp in cps:
                cp.start() if start else cp.wait_send()

        def out(part, n=1):
            return self.vout.at[slot, pl.ds(part * pr, n * pr)]

        def summed(job, q):
            for cp in self.loads(tau, job, [self.view(r, q, job) for r in (self.own, self.sibling)]):
                cp.wait()
            a = (0, 2, 3)[job] * pr
            n = self.parts[job][1] * pr
            return self.vin[slot, 0, a : a + n] + self.vin[slot, 1, a : a + n]

        @pl.when(self.ok(q_leaf))
        def _():
            o = out(3)
            if start:
                o[...] = summed(2, q_leaf)
            run(self.send(o, self.box(q_leaf, 3), slot, 0, q_leaf, 0, self.partner))

        q_met = tau - L - 1
        for i in range(2):
            n, part = (2, 0) if i == 0 else (1, 2)

            @pl.when(self.ok(q_met) & (self.k[i] == L - 1))
            def _():
                tot = out(4 + 2 * i, n)
                if start:
                    a = (part + n - 1) * pr
                    self.landed(self.box(q_met, 4), q_met, 3)
                    if i == 0:
                        tot[0:pr] = self.vout[1 - slot, 0:pr]
                    tot[(n - 1) * pr : n * pr] = self.vout[1 - slot, a : a + pr] + self.land[q_met, 4 * pr : 5 * pr]
                fv = self.view(self.fin, q_met, i)
                run(self.send(tot, fv, slot, 2 if i == 0 else 7, q_met, 4 if i == 0 else 6, self.down[i]))
                if i == 0:
                    run(self.send(out(4), self.view(self.fin, q_met, 0, 0, 1), slot, 3, q_met, 5, self.partner))
                cp = pltpu.make_async_copy(tot, fv, self.fsem.at[i, slot])
                cp.start() if start else cp.wait()

        for i in range(2):
            k = self.k[i]
            r = L - 1 - k
            q = tau - L - 1 - r

            @pl.when(self.ok(q) & (r > 0))
            def _():
                fv = self.view(self.fin, q, i)
                if start:
                    self.landed(fv, q, 4 if i == 0 else 6)

                @pl.when(k > 0)
                def _():
                    run(self.send(fv, fv, slot, 8 if i == 0 else 10, q, 4 if i == 0 else 6, self.down[i]))

                if i == 0:
                    fx = self.view(self.fin, q, 0, 0, 1)
                    run(self.send(fx, fx, slot, 9, q, 5, self.partner))

        for i, q in ((0, q_both), (1, q_one)):
            k = self.k[i]
            n, part = (2, 0) if i == 0 else (1, 2)

            @pl.when(self.ok(q))
            def _():
                o = out(part, n)
                if start:
                    v = summed(i, q)
                    if i == 0:
                        self.landed(self.box(q, 3), q, 0)
                        o[0:pr] = v[0:pr] + self.land[q, 3 * pr : 4 * pr]
                        o[pr : 2 * pr] = v[pr : 2 * pr]
                    else:
                        o[...] = v

                    @pl.when(k > 0)
                    def _():
                        self.landed(self.box(q, part, n), q, 1 + i)
                        o[...] += self.land[q, part * pr : (part + n) * pr]

                @pl.when(k < L - 1)
                def _():
                    run(self.send(o, self.box(q, part, n), slot, 1 if i == 0 else 5, q, 1 + i, self.up[i]))

                @pl.when(k == L - 1)
                def _():
                    run(self.send(out(part + n - 1), self.box(q, 4), slot, 4 if i == 0 else 6, q, 3, self.partner))

    def step(self, tau):
        self.wave(tau - 2, start=False)
        self.wave(tau)

    def steps(self, t0, t1):
        def body(tau, carry):
            self.prefetch(tau + 1)
            self.step(tau)
            return carry

        lax.fori_loop(t0, t1, body, 0)

    def finish(self):
        self.wave(self.waves - 2, start=False)
        self.wave(self.waves - 1, start=False)

        def body(q, carry):
            self.landed(self.view(self.fin, q, 2), q, 5)
            return carry

        lax.fori_loop(0, self.total, body, 0)


N_SUB = 4
PER = N_SUB // 4
P_AHEAD = 8


def backward_kernel(dm, n_dp, *refs):
    (meta, g1_r, g2_r, bd_r, wdn_s, gn_h, gu, p_hbm, i_wqkv, i_wo, i_wup, i_bias, i_tok, i_cot, i_normed, i_q8, i_kk, i_vv, i_mixt, i_n2, i_act, i_gp, i_mid, d_own, d_sib) = refs[:25]
    (fin, sm_out, lo32, gt32, own, sibl, sland) = refs[25:32]
    (wqkv, wo, wup, wdn, cot, mixt, n2, gp, act, mid, gn, dwa, acc, bbuf, small) = refs[32:47]
    psem, tsem, lsem, osem, xss, xrs, sss, srs = refs[47:55]
    red_a = refs[55:62]
    R, D, NS, hw, f = dm.r, dm.d, dm.ns, dm.hw, dm.f
    ln = Links(n_dp)
    y, c, t = ln.y, ln.c, ln.t
    base = c * NS
    nt, ft = D // 256, f // 256

    srcs = (i_gp, i_n2, i_cot, wdn_s, i_act, i_bias, i_mid, i_wup, i_wqkv, i_wo, i_mixt)
    dsts = (gp.at[:, pl.ds(0, 2 * f)], n2, cot, wdn.at[al(t, f)], act, bbuf, mid, wup.at[pl.ds(2 * y, 2)], wqkv, wo, mixt)
    ins = [pltpu.make_async_copy(a, b, lsem.at[i]) for i, (a, b) in enumerate(zip(srcs, dsts))]
    late = [pltpu.make_async_copy(a, gp.at[:, pl.ds(i * D, D)], lsem.at[11 + i]) for i, a in enumerate((i_q8, i_kk, i_vv, i_normed))]
    late.append(pltpu.make_async_copy(i_tok, n2, lsem.at[15]))
    for cp in ins:
        cp.start()
    bar = pltpu.get_barrier_semaphore()
    group = ln.dp - lax.rem(ln.dp, n_dp)
    for dev in (ln.ypart, ln.sib):
        pl.semaphore_signal(bar, inc=1, device_id=dev, device_id_type=MESH)

    def greet(i, carry):
        pl.semaphore_signal(bar, inc=1, device_id=(lax.rem(ln.dp + i, n_dp), t), device_id_type=MESH)
        return carry

    lax.fori_loop(1, n_dp, greet, 0)
    pl.semaphore_wait(bar, 2 + n_dp - 1)
    red = Reduce(ln, (d_own, d_sib), own, sibl, fin, D, 3, N_SUB, *red_a)
    def at(i):
        red.steps(i * PER, (i + 1) * PER)

    def stage(src, ref, r0, k):
        return pltpu.make_async_copy(src, ref.at[pl.ds(r0, D)], tsem.at[k])

    staged = [stage(gn_h.at[ln.t_sib], dwa, 0, 0), stage(gu.at[ln.t_y, pl.ds(hw, D)], dwa, D, 1), stage(gu.at[ln.t_ysib, pl.ds(hw, D)], gn, 0, 2)]
    for cp in staged:
        cp.start()

    def narrow(cp, ref, r0, dst):
        cp.wait()
        for r in range(0, D, 128):
            dst[r : r + 128, :] = ref[r0 + r : r0 + r + 128, :].astype(bf16)

    red.prefetch(0)
    at(0)
    narrow(staged[0], dwa, 0, wdn.at[al(ln.t_sib, f)])
    for cp in ins[:4]:
        cp.wait()
    acc[...] = jnp.zeros_like(acc)

    def grad_hidden(half):
        def one(i):
            s, sh = i // 2, lax.rem(i, 2)
            rs, cs = al(s, R), al(half * 2 + sh, f)
            hf = y if half == 0 else 1 - y
            ga = mmt(cot[rs, :], wdn[al(2 * hf + sh, f), :])
            gp[rs, cs] = (ga * gp[rs, cs].astype(f32)).astype(bf16)

        loop(NS * 2, one)

    grad_hidden(0)
    at(1)
    narrow(staged[1], dwa, D, wup.at[ln.t_y])
    narrow(staged[2], gn, 0, wup.at[ln.t_ysib])

    def dwup(i):
        sh, j = i // nt, lax.rem(i, nt)
        for n in range(ft):
            dwa[pl.ds(pl.multiple_of(i * 256, 256), 256), n * 256 : n * 256 + 256] = tmm(n2[:, al(j, 256)], gp[:, al(sh * ft + n, 256)])

    loop(2 * nt, dwup)
    up_own = pltpu.make_async_copy(dwa.at[al(c, D)], own.at[pl.ds(D, D)], osem.at[2])
    up_own.start()
    up_sib = rcopy(dwa.at[al(1 - c, D)], sibl.at[pl.ds(D, D)], xss.at[0], xrs.at[0], ln.sib)
    up_sib.start()
    ones = jnp.ones((8, dm.rows), bf16)
    for sh in range(2):
        acc[6 + sh, :, :f] = mm(ones, gp[:, sh * f : (sh + 1) * f]) * 0.125

    bd = bd_r[...].reshape(1, D)
    for cp in ins[4:]:
        cp.wait()

    def lo_own(s):
        rs = al(s, R)
        gn[rs, :] = mid[rs, :] + bd + mm(act[rs, :], wdn[al(y, 2 * f), :])

    loop(NS, lo_own)
    at(2)
    up_own.wait()
    up_sib.wait()
    staged = [stage(gn_h.at[ln.t_y], dwa, 0, 0), stage(gn_h.at[ln.t_ysib], dwa, D, 1)]
    for cp in staged:
        cp.start()
    tw = 384 if f % 384 == 0 else 256
    mt = f // tw

    def mlp(i):
        pl.when(i == NS * mt)(lambda: at(3))
        s, j = i // (2 * mt), lax.rem(i, 2 * mt)
        sh = 2 * (1 - y) + j // mt
        rs, cs = al(s, R), al(lax.rem(j, mt), tw)
        h = mm(n2[rs, :], wup[sh, :, cs]) + bbuf[sh, 0:1, cs]
        a, g = gelu_pair(h)
        act[rs, al(j, tw)] = a.astype(bf16)
        gp[rs, al(2 * mt + j, tw)] = g.astype(bf16)

    loop(NS * 2 * mt, mlp)
    at(4)
    narrow(staged[0], dwa, 0, wdn.at[al(ln.t_y, f)])
    narrow(staged[1], dwa, D, wdn.at[al(ln.t_ysib, f)])
    grad_hidden(1)

    def gnorm2(s):
        rs = al(s, R)
        tot = None
        for half in range(2):
            for i in range(2):
                sh = 2 * (y if half == 0 else 1 - y) + i
                k = half * 2 + i
                p = mmt(gp[rs, k * f : (k + 1) * f], wup[sh])
                tot = p if tot is None else tot + p
        lo = gn[rs, :] + mm(act[rs, :], wdn[al(1 - y, 2 * f), :])
        dwa[rs, :] = lo
        gn[rs, :] = tot

    loop(NS, gnorm2)
    at(5)
    total, hp = NS * dm.pairs, dm.pairs // 2

    def place(i):
        j = lax.rem(i, NS * hp)
        half = i // (NS * hp)
        hf = y + half * (1 - 2 * y)
        return j // hp, hf * hp + lax.rem(j, hp)

    def p_slot(i):
        k = lax.rem(i, P_AHEAD)
        return k // 2, pl.ds(pl.multiple_of(lax.rem(k, 2) * dm.rp, 128), dm.rp)

    def p_copy(i):
        s, p = place(i)
        k, cs = p_slot(i)
        return pltpu.make_async_copy(p_hbm.at[s * dm.pairs + p], wup.at[k, pl.ds(0, 2 * R), cs], psem.at[lax.rem(i, P_AHEAD)])

    for i in range(P_AHEAD - 1):
        p_copy(i).start()
    lo_copies = []
    for s in range(NS):
        v = dwa.at[pl.ds(s * R, R)]
        lo_copies.append((pltpu.make_async_copy(v, lo32.at[base + s], osem.at[3 + s]), rcopy(v, lo32.at[base + s], xss.at[1 + s], xrs.at[1 + s], ln.sib)))
        for cp in lo_copies[-1]:
            cp.start()
    for cp in late:
        cp.start()
    q8, kk, vv, normed = (gp.at[:, pl.ds(i * D, D)] for i in range(4))
    tok = n2
    g2 = g2_r[...].reshape(1, D)
    g1 = g1_r[...].reshape(1, D)

    def ln2b(i):
        rs = pl.ds(pl.multiple_of(i * CH, CH), CH)
        xh, r = centred(mid[rs, :])
        go = gn[rs, :]
        co = cot[rs, :].astype(f32)
        g = go * g2
        gx = g * xh
        gm = co + r * (g - jnp.sum(g, -1, keepdims=True) * (1.0 / D) - xh * (jnp.sum(gx, -1, keepdims=True) * (1.0 / D)))
        mid[rs, :] = gm
        gl = gm.astype(bf16)
        act[rs, 0:D] = gl
        acc[0] += fold8(co)
        acc[1] += fold8(gl.astype(f32))
        acc[4] += fold8(go * xh)
        acc[5] += fold8(go)

    loop(dm.rows // CH, ln2b)

    def gmixf(s):
        rs = al(s, R)
        act[rs, D : 2 * D] = mmt(act[rs, 0:D], wo[...]).astype(bf16)

    loop(NS, gmixf)
    at(6)
    own_h = al(y, 2 * hw)

    def over_samples(fn):
        tot = None
        for s in range(NS):
            p = fn(s)
            tot = p if tot is None else tot + p
        return tot

    for a, b in lo_copies:
        a.wait()
        b.wait()

    for n in range(nt):
        cc = slice(n * 256, n * 256 + 256)
        p = over_samples(lambda s: mm(mixt[s, own_h, :], act[s * R : s * R + R, cc]))
        for sh in range(2):
            dwa[sh * D + 3 * hw : sh * D + 4 * hw, cc] = p[sh * hw : (sh + 1) * hw]
    for cp in late:
        cp.wait()
    lane = lax.broadcasted_iota(jnp.int32, (1, 128), 1)
    masks = (lane < HEAD_DIM, lane >= HEAD_DIM)
    def attn(i):
        s, p = place(i)
        rs, cs = al(s, R), al(p, 128)
        slab, pc = p_slot(i)

        @pl.when(i + P_AHEAD - 1 < total)
        def _():
            p_copy(i + P_AHEAD - 1).start()

        p_copy(i).wait()
        q, k, v, do = q8[rs, cs], kk[rs, cs], vv[rs, cs], act[rs, pl.ds(pl.multiple_of(D + p * 128, 128), 128)]
        dv, dk = [], []
        for h in range(2):
            pt = wup[slab, h * R : (h + 1) * R, pc][:, :R]
            pf = pt.astype(f32)
            dp = mmt(jnp.where(masks[h], v, jnp.bfloat16(0)), do)
            dsum = jnp.sum(pf * dp, 0, keepdims=True)
            ds = (pf * (dp - dsum)).astype(bf16)
            dv.append(mm(pt, do))
            dk.append(mm(ds, q))
            o = tmm(k, ds)
            hr = pl.ds(pl.multiple_of(p * 128 + h * HEAD_DIM, HEAD_DIM), HEAD_DIM)
            mixt[s, hr, :] = (o[h * HEAD_DIM : (h + 1) * HEAD_DIM] * 0.125).astype(bf16)
        kk[rs, cs] = jnp.where(masks[0], dk[0], dk[1]).astype(bf16)
        vv[rs, cs] = jnp.where(masks[0], dv[0], dv[1]).astype(bf16)

    def attend(i0, i1, between):
        def one(i, carry):
            attn(i)
            for k, fn in between:
                pl.when(i == k)(fn)
            return carry

        lax.fori_loop(i0, i1, one, 0)

    half = NS * hp

    def seventh():
        red.steps(7 * PER, 8 * PER - 1)
        red.step(8 * PER - 1)

    attend(0, half, [(half // 2, seventh)])
    for n in range(nt):
        cc = slice(n * 256, n * 256 + 256)
        p = over_samples(lambda s: mm(mixt[s, own_h, :], normed[s * R : s * R + R, cc]))
        tk = tmm(kk[:, own_h], normed[:, cc])
        tv = tmm(vv[:, own_h], normed[:, cc])
        for sh in range(2):
            h = slice(sh * hw, (sh + 1) * hw)
            dwa[sh * D : sh * D + hw, cc] = p[h]
            dwa[sh * D + hw : sh * D + 2 * hw, cc] = tk[h]
            dwa[sh * D + 2 * hw : sh * D + 3 * hw, cc] = tv[h]
    a_own = pltpu.make_async_copy(dwa.at[al(c, D)], own.at[pl.ds(2 * D, D)], osem.at[2])
    a_own.start()
    a_sib = rcopy(dwa.at[al(1 - c, D)], sibl.at[pl.ds(2 * D, D)], xss.at[5], xrs.at[5], ln.sib)
    a_sib.start()
    onesr = jnp.ones((8, R), bf16)
    acc[8, :, 0 : 2 * hw] = over_samples(lambda s: mmt(onesr, mixt[s, own_h, :])) * 0.125
    acc[9, :, 0 : 2 * hw] = mm(ones, vv[:, own_h]) * 0.125
    third3 = NS * hp // 3
    attend(half, half + third3, [])
    a_own.wait()
    a_sib.wait()
    red.prefetch(8 * PER)
    at(8)
    attend(half + third3, total, [(half + 2 * third3, lambda: at(9))])
    at(10)

    def gnorm1(s):
        rs = al(s, R)
        gn[rs, :] = tmm(mixt[s], wqkv[0:D, :]) + mm(kk[rs, :], wqkv[D : 2 * D, :]) + mm(vv[rs, :], wqkv[2 * D : 3 * D, :])

    loop(NS, gnorm1)
    at(11)

    def ln1b(s):
        for r0, n in row_chunks(dm):
            rs = pl.ds(pl.multiple_of(s * R + r0, 16), n)
            x = tok[rs, :].astype(f32)
            keep = keep_of(meta, base, s, r0, n) if r0 == 0 else None
            xh, r = centred(x if keep is None else x * keep)
            go = gn[rs, :]
            g = go * g1
            gx = g * xh
            gi = r * (g - jnp.sum(g, -1, keepdims=True) * (1.0 / D) - xh * (jnp.sum(gx, -1, keepdims=True) * (1.0 / D)))
            o = mid[rs, :] + gi
            mid[rs, :] = o if keep is None else o * keep
            acc[2] += fold8(go * xh)
            acc[3] += fold8(go)

    loop(NS, ln1b)
    gt_copies = []
    for s in range(NS):
        v = mid.at[pl.ds(s * R, R)]
        gt_copies.append((pltpu.make_async_copy(v, gt32.at[base + s], osem.at[3 + s]), rcopy(v, gt32.at[base + s], xss.at[6 + s], xrs.at[6 + s], ln.sib)))
        for cp in gt_copies[-1]:
            cp.start()

    tot = jnp.sum(acc[...], 1)
    for sh in range(2):
        small[sh, 0:6, :] = tot[0:6]
        small[sh, 6:7, :] = tot[6 + sh : 7 + sh]
        small[sh, 7:8, 0:hw] = tot[8:9, sh * hw : (sh + 1) * hw]
        small[sh, 7:8, hw : 2 * hw] = tot[9:10, sh * hw : (sh + 1) * hw]
        small[sh, 7:8, 2 * hw :] = jnp.zeros((1, D - 2 * hw), f32)
    cp = rcopy(small.at[1 - c], small.at[2], xss.at[10], xrs.at[10], ln.sib)
    cp.start()
    cp.wait()
    small[2] = small[c] + small[2]
    mine = sland.at[al(ln.dp, 8)]
    kept = pltpu.make_async_copy(small.at[2], mine, osem.at[0])
    kept.start()

    def peer(i):
        d = lax.rem(ln.dp + i, n_dp)
        return rcopy(small.at[2], mine, sss.at[d], srs.at[ln.dp], (d, t))

    def spread(i, carry):
        peer(i).start()
        return carry

    lax.fori_loop(1, n_dp, spread, 0)

    red.steps(12 * PER, red.waves)
    red.finish()

    def gathered(i, carry):
        peer(i).wait_send()
        d = lax.rem(ln.dp + i, n_dp)
        theirs = sland.at[al(d, 8)]
        rcopy(theirs, theirs, sss.at[d], srs.at[d], (d, t)).wait_recv()
        return carry

    lax.fori_loop(1, n_dp, gathered, 0)
    kept.wait()
    back = pltpu.make_async_copy(sland, dwa.at[pl.ds(0, 8 * n_dp)], osem.at[0])
    back.start()
    back.wait()
    sm_out[...] = lax.fori_loop(1, n_dp, lambda i, v: v + dwa[al(i, 8), :], dwa[0:8, :])
    for a, b in gt_copies:
        a.wait()
        b.wait()


def backward_call(dm, n_dp, small, big):
    M, D, f = dm.rows, dm.d, dm.f
    sds, vm, dma = jax.ShapeDtypeStruct, pltpu.VMEM, pltpu.SemaphoreType.DMA
    st = sds((3 * D, D), f32)
    outs = [st, sds((8, D), f32), sds((dm.samples, dm.r, D), f32), sds((dm.samples, dm.r, D), f32), st, st, sds((8 * n_dp, D), f32)]
    row, wide = vm((M, D), bf16), vm((M, 2 * f), bf16)
    scratch = [vm((3 * D, D), bf16), vm((D, D), bf16), vm((dm.n_t, D, f), bf16), vm((dm.ff, D), bf16), row]
    scratch += [vm((dm.ns, D, dm.r), bf16), row, vm((M, dm.ff), bf16), wide, vm((M, D), f32), vm((M, D), f32), vm((2 * D, D), f32), vm((10, 8, D), f32)]
    scratch += [vm((dm.n_t, 16, D), f32), vm((3, 8, D), f32)]
    scratch += [dma((P_AHEAD,)), dma((3,)), dma((16,)), dma((7,)), dma((11,)), dma((11,)), dma((n_dp,)), dma((n_dp,))]
    scratch += Reduce.scratch(3, N_SUB, D, D)

    def kern(*refs):
        backward_kernel(dm, n_dp, *refs)

    return pl.pallas_call(
        kern,
        out_shape=outs,
        in_specs=[SM] + [V] * (len(small) - 1) + [ANY] * len(big),
        out_specs=[ANY, V] + [ANY] * 5,
        scratch_shapes=scratch,
        compiler_params=pltpu.CompilerParams(vmem_limit_bytes=VMEM_LIMIT, collective_id=2, has_side_effects=True),
        name="backward",
    )(*small, *big)


def shards(tokens, metadata, cotangent, w_query, w_key, w_value, w_out, b_query, b_value, b_out, w_up, b_up, w_down, b_down, gain_one, shift_one, gain_two, shift_two, n_dp, n_t):
    dm = Dims(tokens, w_up, n_t)
    D, hw, f = dm.d, dm.hw, dm.f
    small = (metadata, w_query.T, w_key.T, w_value.T, w_out, w_up, w_down, b_up, b_query, b_value, gain_one, shift_one, gain_two, shift_two, b_out)
    (gu, gnw, _, p, wqkv, wo, wu, bb, tok, cot, normed, q8, kk, vv, mixt, n2, act, gp, mid, d_own, d_sib) = forward_call(dm, n_dp, small, (tokens.transpose(1, 0, 2), cotangent.transpose(1, 0, 2)))
    small = (metadata, gain_one, gain_two, b_down)
    fin, sm, lo, gt, *_ = backward_call(dm, n_dp, small, (w_down, gnw, gu, p, wqkv, wo, wu, bb, tok, cot, normed, q8, kk, vv, mixt, n2, act, gp, mid, d_own, d_sib))
    a_ = fin[2 * D :]
    return (
        lo[:, : dm.length].astype(bf16),
        gt[:, : dm.length],
        a_[0:hw].T,
        a_[hw : 2 * hw].T,
        a_[2 * hw : 3 * hw].T,
        a_[3 * hw : 4 * hw],
        sm[7, :hw],
        sm[7, hw : 2 * hw],
        sm[1],
        fin[D : 2 * D],
        sm[6],
        fin[:D],
        sm[0],
        sm[2],
        sm[3],
        sm[4],
        sm[5],
    )


def solution(mesh):
    n_dp, n_t = mesh.shape["dp"], mesh.shape["tensor"]
    rows, cols, vec, rep = P("dp", None, None), P(None, "tensor"), P("tensor"), P()
    srow = P("tensor", None)

    def run(*args):
        return shards(*args, n_dp=n_dp, n_t=n_t)

    return jax.shard_map(
        run,
        mesh=mesh,
        in_specs=(rows, P("dp"), rows, cols, cols, cols, srow, vec, vec, rep, cols, vec, srow, rep, rep, rep, rep, rep),
        out_specs=(rows, rows, cols, cols, cols, srow, vec, vec, rep, cols, vec, srow, rep, rep, rep, rep, rep),
        check_vma=False,
    )
```

```python
import math

import jax
import jax.numpy as jnp
from jax import lax
from jax.experimental import pallas as pl
from jax.experimental.pallas import tpu as pltpu
from jax.sharding import PartitionSpec as P

HEAD_DIM = 64
EPS = 1e-05
MESH = pl.DeviceIdType.MESH
f32 = jnp.float32
bf16 = jnp.bfloat16
VMEM_LIMIT = 63 << 20
RING = 8
CH = 64
TAIL_P = 0.24
TAIL = (
    0.08952743306829739,
    0.15551359433427508,
    -0.15404885518029288,
    0.6255903019940591,
    -0.6460706945688248,
    0.5545739487327468,
    -0.12508572868970558,
)
INV_SQRT_2PI = 1.0 / math.sqrt(2.0 * math.pi)
HALF_LOG2E = -0.5 / math.log(2.0)


def mm(a, b):
    return lax.dot_general(a, b, (((1,), (0,)), ((), ())), preferred_element_type=f32)


def mmt(a, b):
    return lax.dot_general(a, b, (((1,), (1,)), ((), ())), preferred_element_type=f32)


def tmm(a, b):
    return lax.dot_general(a, b, (((0,), (0,)), ((), ())), preferred_element_type=f32)


def loop(n, fn):
    def body(i, carry):
        fn(i)
        return carry

    lax.fori_loop(0, n, body, 0)


def al(i, step):
    return pl.ds(pl.multiple_of(i * step, step), step)


def centred(x):
    d = x.shape[-1]
    mu = jnp.sum(x, -1, keepdims=True) * (1.0 / d)
    xm = x - mu
    var = jnp.sum(xm * xm, -1, keepdims=True) * (1.0 / d)
    r = lax.rsqrt(var + EPS)
    return xm * r, r


def gelu_pair(v):
    d = 1.0 + TAIL_P * jnp.abs(v)
    t = pltpu.reciprocal(d, approx=True)
    t = t * (2.0 - d * t)
    e = jnp.exp2(HALF_LOG2E * (v * v))
    acc = TAIL[6] * t + TAIL[5]
    for k in range(4, -1, -1):
        acc = acc * t + TAIL[k]
    q = (acc * t) * e
    cdf = jnp.where(v < 0, q, 1.0 - q)
    return v * cdf, cdf + (v * e) * INV_SQRT_2PI


def fold8(x):
    return jnp.sum(x.reshape(x.shape[0] // 8, 8, x.shape[1]), 0)


class Dims:
    def __init__(self, tokens, w_up, n_t):
        self.samples, self.length, self.d = tokens.shape
        self.ns = self.samples // 2
        self.r = -(-self.length // 16) * 16
        self.rp = -(-self.r // 128) * 128
        self.rows = self.ns * self.r
        self.f = w_up.shape[1]
        self.ff = self.f * n_t
        self.n_t = n_t
        self.heads = self.d // HEAD_DIM
        self.pairs = self.heads // 2
        self.hw = self.d // n_t


class Links:
    def __init__(self, n_dp):
        self.n_dp = n_dp
        self.dp = lax.axis_index("dp")
        self.t = lax.axis_index("tensor")
        self.y, self.c = self.t // 2, lax.rem(self.t, 2)
        self.z, self.x = self.dp // 2, lax.rem(self.dp, 2)
        self.length = n_dp // 2
        self.sib = (self.dp, 2 * self.y + 1 - self.c)
        self.ypart = (self.dp, 2 * (1 - self.y) + self.c)
        self.t_sib = 2 * self.y + 1 - self.c
        self.t_y = 2 * (1 - self.y) + self.c
        self.t_ysib = 2 * (1 - self.y) + 1 - self.c
        g = lax.rem(self.dp, RING)
        half = RING // 2
        zz, xx = g // 2, lax.rem(g, 2)
        self.pos = jnp.where(xx == 0, zz, RING - 1 - zz)
        base = self.dp - g

        def at(pos):
            pos = lax.rem(pos + RING, RING)
            local = jnp.where(pos < half, 2 * pos, 2 * (RING - 1 - pos) + 1)
            return (base + local, self.t)

        self.step = 1 - 2 * self.c
        self.ahead, self.behind = at(self.pos + self.step), at(self.pos - self.step)

    def piece(self, offset):
        return lax.rem(self.pos + offset * self.step + RING, RING)


def rcopy(src, dst, ssem, rsem, dev):
    return pltpu.make_async_remote_copy(src_ref=src, dst_ref=dst, send_sem=ssem, recv_sem=rsem, device_id=dev, device_id_type=MESH)


def enter(devs):
    bar = pltpu.get_barrier_semaphore()
    for d in devs:
        pl.semaphore_signal(bar, inc=1, device_id=d, device_id_type=MESH)
    pl.semaphore_wait(bar, len(devs))


class Gather:
    def __init__(self, ln, src, out, direct, ssem, rsem, head=0):
        self.ln, self.src, self.out, self.direct, self.head = ln, src, out, direct, head
        self.ssem, self.rsem = ssem, rsem
        self.passed = self.passed_sib = False
        self.rows = src.shape[0]
        self.piece_rows = (self.rows - direct) // RING

    def at(self, ref, offset):
        return ref.at[pl.ds(pl.multiple_of(self.direct + self.ln.piece(offset) * self.piece_rows, 8), self.piece_rows)]

    def copy(self, src, dst, k, dev):
        return rcopy(src, dst, self.ssem.at[k], self.rsem.at[k], dev)

    def landed(self, view, k):
        rcopy(view, view, self.ssem.at[k], self.rsem.at[k], self.ln.sib).wait_recv()

    def spread_y(self):
        return self.copy(self.at(self.src, 0), self.at(self.out.at[self.ln.t], 0), 0, self.ln.ypart)

    def direct_y(self):
        d = pl.ds(self.head, self.direct - self.head)
        return self.copy(self.src.at[d], self.out.at[self.ln.t].at[d], 1, self.ln.ypart)

    def head_y(self):
        d = pl.ds(0, self.head)
        return self.copy(self.src.at[d], self.out.at[self.ln.t].at[d], 19, self.ln.ypart)

    def head_sib(self):
        v = self.out.at[self.ln.t_y].at[pl.ds(0, self.head)]
        return self.copy(v, v, 20, self.ln.sib)

    def head_landed(self):
        self.landed(self.out.at[self.ln.t_y].at[pl.ds(0, self.head)], 19)
        self.head_sib().start()

    def head_sib_landed(self):
        self.landed(self.out.at[self.ln.t_ysib].at[pl.ds(0, self.head)], 20)

    def whole_sib(self):
        return self.copy(self.src, self.out.at[self.ln.t], 2, self.ln.sib)

    def start_y(self):
        self.spread_y().start()
        self.direct_y().start()

    def start_sib(self):
        self.whole_sib().start()

    def wait_sib(self):
        self.landed(self.out.at[self.ln.t_sib], 2)

    def to_sib(self, offset):
        v = self.at(self.out.at[self.ln.t_y], offset)
        return self.copy(v, v, 11 + 4 + offset, self.ln.sib)

    def direct_sib(self):
        v = self.out.at[self.ln.t_y].at[pl.ds(self.head, self.direct - self.head)]
        return self.copy(v, v, 10, self.ln.sib)

    def ring_ahead(self, s):
        v = self.at(self.out.at[self.ln.t_y], -s)
        return self.copy(v, v, 3 + s, self.ln.ahead)

    def ring_behind(self, s):
        v = self.at(self.out.at[self.ln.t_y], s)
        return self.copy(v, v, 7 + s, self.ln.behind)

    def tick(self, i):
        ln, out = self.ln, self.out.at[self.ln.t_y]
        if i == 0:
            self.landed(self.at(out, 0), 0)
            self.ring_ahead(0).start()
            self.ring_behind(0).start()
            self.to_sib(0).start()
            return
        s = i - 1
        self.landed(self.at(out, -s - 1), 3 + s)
        if s < 3:
            self.ring_ahead(s + 1).start()
            self.landed(self.at(out, s + 1), 7 + s)
            if s < 2:
                self.ring_behind(s + 1).start()
        self.to_sib(-s - 1).start()
        if s < 3:
            self.to_sib(s + 1).start()

    def direct_landed(self):
        if not self.passed:
            self.passed = True
            self.landed(self.out.at[self.ln.t_y].at[pl.ds(self.head, self.direct - self.head)], 1)
            self.direct_sib().start()

    def direct_sib_landed(self):
        if not self.passed_sib:
            self.passed_sib = True
            self.landed(self.out.at[self.ln.t_ysib].at[pl.ds(self.head, self.direct - self.head)], 10)

    def finish(self):
        ln, out = self.ln, self.out.at[self.ln.t_ysib]
        for offset in range(-4, 4):
            v = out.at[pl.ds(pl.multiple_of(self.direct + lax.rem(ln.pos - offset * ln.step + RING, RING) * self.piece_rows, 8), self.piece_rows)]
            self.landed(v, 11 + 4 + offset)
        self.direct_sib_landed()

    def drain(self):
        cps = [self.head_y(), self.head_sib()] if self.head else []
        cps += [self.spread_y(), self.direct_y(), self.whole_sib(), self.direct_sib()]
        cps += [self.ring_ahead(s) for s in range(4)] + [self.ring_behind(s) for s in range(3)]
        cps += [self.to_sib(o) for o in range(-4, 4)]
        for cp in cps:
            cp.wait_send()


GATHER_SEMS = 21


def keep_of(meta, base, s, r0, n):
    rows = lax.broadcasted_iota(jnp.int32, (n, 1), 0) + r0
    return jnp.where(rows == 1, meta[base + s].astype(f32), 1.0)


def row_chunks(dm):
    out, r = [], 0
    while r < dm.r:
        n = min(CH, dm.r - r)
        out.append((r, n))
        r += n
    return out


def forward_kernel(dm, n_dp, *refs):
    (meta, wq, wk, wv, wo_s, wup_s, wdn_s, bup_r, bq_r, bv_r, g1_r, s1_r, g2_r, s2_r, bo_r, tokens, cotan) = refs[:17]
    (gu, gn_h, n32, p_hbm, o_wqkv, o_wo, o_wup, o_bias, o_tok, o_cot, o_normed, o_q8, o_kk, o_vv, o_mixt, o_n2, o_act, o_gp, o_mid, d_own, d_sib) = refs[17:38]
    (tok3, cot3, tok, cot, wqkv, wo, wup, normed, q8, kk, vv, mixt, n2, act, gp, mid, dwd, pbuf, tmp, bbuf, bqv, ga, ustage) = refs[38:61]
    psem, tsem, lsem, osem, ssa, rsa, ssu, rsu, ssn, rsn, ssd, rsd = refs[61:]
    R, D, NS, hw, f = dm.r, dm.d, dm.ns, dm.hw, dm.f
    ln = Links(n_dp)
    y, c, t = ln.y, ln.c, ln.t
    base = c * NS

    def row(ref):
        return ref[...].reshape(1, D)

    loads = [pltpu.make_async_copy(tokens, tok3, lsem.at[0]), pltpu.make_async_copy(cotan, cot3, lsem.at[1])]
    for cp in loads:
        cp.start()
    outs = []

    def put(src, dst):
        cp = pltpu.make_async_copy(src, dst, osem.at[len(outs)])
        cp.start()
        outs.append(cp)

    own_a = mid.at[pl.ds(0, 16 + 3 * hw)]
    mid[0:16, :] = jnp.zeros((16, D), f32)
    mid[0:1, 0:f] = bup_r[...].reshape(1, f)
    mid[1:2, 0:hw] = bq_r[...].reshape(1, hw)
    mid[1:2, hw : 2 * hw] = bv_r[...].reshape(1, hw)
    bbuf[t] = mid[0:16, :]
    for i, w in enumerate((wq, wk, wv)):
        mid[16 + i * hw : 16 + (i + 1) * hw, :] = w[...].astype(f32)
        wqkv[pl.ds(pl.multiple_of(i * D + t * hw, 16), hw), :] = w[...]
    wo[al(t, hw), :] = wo_s[...]
    g_a = Gather(ln, own_a, ga, 16 + hw, ssa, rsa)
    g_u = Gather(ln, ustage, gu, hw + D // 3, ssu, rsu, hw)
    g_n = Gather(ln, n32, gn_h, D // 4, ssn, rsn)
    enter((ln.ypart, ln.sib, ln.ahead, ln.behind))
    g_a.start_y()
    g_a.start_sib()
    ustage[0:hw, :] = wo_s[...].astype(f32)

    def widen(i):
        rs = al(i, 64)
        ustage[pl.ds(pl.multiple_of(hw + i * 64, 64), 64), :] = wup_s[rs, :].astype(f32)
        dwd[1, rs, :] = wdn_s[rs, :].astype(f32)
        wup[c, rs, :] = wup_s[rs, :]

    loop(D // 64, widen)
    put(dwd.at[1], n32)
    g_u.spread_y().start()
    outs[0].wait()
    g_n.spread_y().start()
    g_u.head_y().start()
    g_u.direct_y().start()
    g_n.direct_y().start()
    g_u.start_sib()
    g_n.start_sib()

    for cp in loads:
        cp.wait()
    g1, s1, g2, s2, bo = (row(r) for r in (g1_r, s1_r, g2_r, s2_r, bo_r))
    grp = dm.length // 32
    rest, pad = dm.length - grp * 32, R - grp * 32

    def selection(n_out, n_in):
        r = lax.broadcasted_iota(jnp.int32, (NS * n_out, n_in * 2 * NS), 0)
        col = lax.broadcasted_iota(jnp.int32, (NS * n_out, n_in * 2 * NS), 1)
        hit = (col == lax.rem(r, n_out) * (2 * NS) + base + r // n_out) & (lax.rem(r, n_out) < n_in)
        return jnp.where(hit, 1.0, 0.0).astype(bf16)

    sel = selection(32, 32)

    def regroup(g):
        for src, dst in ((tok3, tok), (cot3, cot)):
            v = src[al(g, 32)].astype(f32).reshape(32 * 2 * NS, D).astype(bf16)
            o = mm(sel, v).astype(bf16)
            for s in range(NS):
                dst[pl.ds(pl.multiple_of(s * R + g * 32, 16), 32), :] = o[s * 32 : (s + 1) * 32]

    loop(grp, regroup)
    if pad:
        sel_end = selection(pad, rest)
        for src, dst in ((tok3, tok), (cot3, cot)):
            v = src[grp * 32 : grp * 32 + rest].astype(f32).reshape(rest * 2 * NS, D).astype(bf16)
            o = mm(sel_end, v).astype(bf16)
            for s in range(NS):
                dst[s * R + grp * 32 : (s + 1) * R, :] = o[s * pad : (s + 1) * pad]
    put(tok, o_tok)
    put(cot, o_cot)

    def ln1(s):
        for r, n in row_chunks(dm):
            rs = pl.ds(pl.multiple_of(s * R + r, 16), n)
            x = tok[rs, :].astype(f32)
            if r == 0:
                x = x * keep_of(meta, base, s, r, n)
            xh, _ = centred(x)
            normed[rs, :] = (xh * g1 + s1).astype(bf16)

    loop(NS, ln1)
    put(normed, o_normed)

    def fetch(src, k):
        cp = pltpu.make_async_copy(src, tmp.at[k], tsem.at[k])
        cp.start()
        return cp

    def take_a(tp):
        bbuf[tp] = ga[tp, 0:16, :]
        for i in range(3):
            wqkv[pl.ds(pl.multiple_of(i * D + tp * hw, 16), hw), :] = ga[tp, 16 + i * hw : 16 + (i + 1) * hw, :].astype(bf16)

    lane = lax.broadcasted_iota(jnp.int32, (1, 128), 1)
    masks = (lane < HEAD_DIM, lane >= HEAD_DIM)
    hp = dm.pairs // 2
    tail = R - 16
    live = lax.broadcasted_iota(jnp.int32, (16, 1), 0) < dm.length - tail

    def project(hf):
        for i in range(2):
            b = bbuf[2 * hf + i]
            bqv[0:1, i * hw : (i + 1) * hw] = b[1:2, 0:hw]
            bqv[1:2, i * hw : (i + 1) * hw] = b[1:2, hw : 2 * hw]
        cs = al(hf, 2 * hw)

        def one(s):
            rs = al(s, R)
            n = normed[rs, :]
            w = [wqkv[pl.ds(pl.multiple_of(i * D + hf * 2 * hw, 128), 2 * hw), :] for i in range(3)]
            q8[rs, cs] = (mmt(n, w[0]) + bqv[0:1, : 2 * hw]).astype(bf16) * jnp.bfloat16(0.125)
            kk[rs, cs] = mmt(n, w[1]).astype(bf16)
            vv[rs, cs] = (mmt(n, w[2]) + bqv[1:2, : 2 * hw]).astype(bf16)

        loop(NS, one)

    def p_copy(hf, i):
        slot = lax.rem(i, 2)
        return pltpu.make_async_copy(pbuf.at[slot], p_hbm.at[(i // hp) * dm.pairs + hf * hp + lax.rem(i, hp)], psem.at[slot])

    def attend(hf, ticks):
        total = NS * hp

        def one(i):
            s, p = i // hp, hf * hp + lax.rem(i, hp)
            slot = lax.rem(i, 2)
            rs, cs = al(s, R), al(p, 128)
            for k, fn in ticks:
                pl.when(i == k)(fn)

            @pl.when(i >= 2)
            def _():
                p_copy(hf, i - 2).wait()

            q, k, v = q8[rs, cs], kk[rs, cs], vv[rs, cs]
            for h in range(2):
                st = mmt(jnp.where(masks[h], k, jnp.bfloat16(0)), q)
                sa = st[:tail]
                sb = jnp.where(live, st[tail:], -1e30)
                m = jnp.maximum(jnp.max(sa, 0, keepdims=True), jnp.max(sb, 0, keepdims=True))
                ea, eb = jnp.exp(sa - m), jnp.exp(sb - m)
                inv = 1.0 / (jnp.sum(ea, 0, keepdims=True) + jnp.sum(eb, 0, keepdims=True))
                pbuf[slot, h * R : h * R + tail, 0:R] = (ea * inv).astype(bf16)
                pbuf[slot, h * R + tail : (h + 1) * R, 0:R] = (eb * inv).astype(bf16)
                o = tmm(v, pbuf[slot, h * R : (h + 1) * R, 0:R])
                hr = pl.ds(pl.multiple_of(p * 128 + h * HEAD_DIM, HEAD_DIM), HEAD_DIM)
                mixt[s, hr, :] = o[h * HEAD_DIM : (h + 1) * HEAD_DIM].astype(bf16)
            p_copy(hf, i).start()

        loop(total, one)
        p_copy(hf, total - 2).wait()
        p_copy(hf, total - 1).wait()

    g_a.wait_sib()
    take_a(ln.t_sib)
    g_a.tick(0)
    project(y)
    g_a.tick(1)
    attend(y, [(3, lambda: g_a.tick(2)), (9, lambda: g_a.tick(3))])
    g_a.tick(4)
    g_a.direct_landed()
    g_a.finish()
    take_a(ln.t_y)
    take_a(ln.t_ysib)
    put(wqkv, o_wqkv)
    put(bbuf, o_bias)
    g_u.tick(0)
    project(1 - y)
    put(q8, o_q8)
    put(kk, o_kk)
    put(vv, o_vv)
    g_n.tick(0)

    def both(i):
        g_u.tick(i)
        g_n.tick(i)

    attend(1 - y, [(9, lambda: both(1))])
    put(mixt, o_mixt)
    g_a.drain()
    g_u.head_landed()
    wo_rows = [fetch(gu.at[tp, pl.ds(0, hw)], i) for i, tp in enumerate((ln.t_y,))]
    g_u.wait_sib()
    wo_rows.append(fetch(gu.at[ln.t_sib, pl.ds(0, hw)], 1))
    g_u.head_sib_landed()
    wo_rows.append(fetch(gu.at[ln.t_ysib, pl.ds(0, hw)], 2))
    for i, tp in enumerate((ln.t_y, ln.t_sib, ln.t_ysib)):
        wo_rows[i].wait()
        wo[al(tp, hw), :] = tmp[i].astype(bf16)
    put(wo, o_wo)
    ups = [fetch(gu.at[ln.t_sib, pl.ds((i + 1) * hw, hw)], i) for i in range(4)]

    def outp(s):
        rs = al(s, R)
        mid[rs, :] = tmm(mixt[s], wo[...])

    loop(NS, outp)

    def ln2(s):
        for r, n in row_chunks(dm):
            rs = pl.ds(pl.multiple_of(s * R + r, 16), n)
            x = tok[rs, :].astype(f32)
            if r == 0:
                x = x * keep_of(meta, base, s, r, n)
            m = x + (mid[rs, :] + bo)
            mid[rs, :] = m
            xh, _ = centred(m)
            n2[rs, :] = (xh * g2 + s2).astype(bf16)

    both(2)
    loop(NS, ln2)
    put(mid, o_mid)
    put(n2, o_n2)
    for i in range(4):
        ups[i].wait()
        wup[1 - c, i * hw : (i + 1) * hw, :] = tmp[i].astype(bf16)
    put(wup, o_wup)
    ft = f // 256
    tw = 384 if f % 384 == 0 else 256
    mt = f // tw

    def mlp(i):
        pl.when(i == NS * 3)(lambda: both(3))
        s, j = i // (2 * mt), lax.rem(i, 2 * mt)
        rs, sh, cs = al(s, R), j // mt, al(lax.rem(j, mt), tw)
        h = mm(n2[rs, :], wup[sh, :, cs]) + bbuf[2 * y + sh, 0:1, cs]
        a, g = gelu_pair(h)
        act[rs, al(j, tw)] = a.astype(bf16)
        gp[rs, al(j, tw)] = g.astype(bf16)

    loop(NS * 2 * mt, mlp)
    put(act, o_act)
    put(gp, o_gp)

    def dwdn(sh):
        def one(j):
            dwd[sh, al(j, 256), :] = tmm(act[:, al(sh * ft + j, 256)], cot[...])

        loop(ft, one)

    dwdn(1 - c)
    ex = rcopy(dwd.at[1 - c], d_sib, ssd.at[0], rsd.at[0], ln.sib)
    ex.start()
    both(4)
    dwdn(c)
    put(dwd.at[c], d_own)
    g_u.direct_landed()
    g_u.finish()
    g_n.direct_landed()
    g_n.wait_sib()
    g_n.finish()
    g_u.drain()
    g_n.drain()
    ex.wait()
    for cp in outs[1:]:
        cp.wait()


V = pl.BlockSpec(memory_space=pltpu.VMEM)
ANY = pl.BlockSpec(memory_space=pl.ANY)
SM = pl.BlockSpec(memory_space=pltpu.SMEM)


def forward_call(dm, n_dp, small, big):
    M, D, f = dm.rows, dm.d, dm.f
    sds, vm, dma = jax.ShapeDtypeStruct, pltpu.VMEM, pltpu.SemaphoreType.DMA
    row = sds((M, D), bf16)
    wide = sds((M, 2 * f), bf16)
    sq = sds((D, f), f32)
    outs = [sds((dm.n_t, D + dm.hw, f), f32), sds((dm.n_t, f, D), f32), sds((f, D), f32), sds((dm.ns * dm.pairs, 2 * dm.r, dm.rp), bf16), sds((3 * D, D), bf16), sds((D, D), bf16), sds((2, D, f), bf16), sds((dm.n_t, 16, D), f32)]
    outs += [row] * 6 + [sds((dm.ns, D, dm.r), bf16), row, wide, wide, sds((M, D), f32), sds((f, D), f32), sds((f, D), f32)]
    scratch = [vm((dm.length, 2 * dm.ns, D), bf16)] * 2 + [vm((M, D), bf16)] * 2 + [vm((3 * D, D), bf16), vm((D, D), bf16), vm((2, D, f), bf16)]
    scratch += [vm((M, D), bf16)] * 4 + [vm((dm.ns, D, dm.r), bf16), vm((M, D), bf16), vm((M, 2 * f), bf16), vm((M, 2 * f), bf16), vm((M, D), f32), vm((2, f, D), f32)]
    scratch += [vm((2, 2 * dm.r, dm.rp), bf16), vm((4, dm.hw, D), f32), vm((dm.n_t, 16, D), f32), vm((8, D), f32), vm((dm.n_t, 16 + 3 * dm.hw, D), f32), vm((dm.hw + D, D), f32)]
    scratch += [dma((2,)), dma((4,)), dma((2,)), dma((20,)), *([dma((GATHER_SEMS,))] * 6), dma((1,)), dma((1,))]

    def kern(*refs):
        forward_kernel(dm, n_dp, *refs)

    return pl.pallas_call(
        kern,
        out_shape=outs,
        in_specs=[SM] + [V] * (len(small) - 1) + [ANY] * len(big),
        out_specs=[ANY] * len(outs),
        scratch_shapes=scratch,
        compiler_params=pltpu.CompilerParams(vmem_limit_bytes=VMEM_LIMIT, collective_id=1, has_side_effects=True),
        name="forward",
    )(*small, *big)


class Reduce:
    KINDS = 7

    @staticmethod
    def scratch(n_arrays, n_sub, rows, width):
        pr, nq = rows // 4 // n_sub, n_arrays * n_sub
        vm, dma = pltpu.VMEM, pltpu.SemaphoreType.DMA
        return [vm((2, 2, 4 * pr, width), f32), vm((2, 7 * pr, width), f32), vm((nq, 5 * pr, width), f32), dma((2, 3, 2)), dma((2, 2)), dma((2, 11)), dma((nq, Reduce.KINDS))]

    def __init__(self, ln, head, own, sib, fin, height, n_arrays, n_sub, vin, vout, land, lsem, fsem, ssem, rsem):
        self.ln, self.head, self.own, self.sibling, self.fin = ln, head, own, sib, fin
        self.vin, self.vout, self.land, self.lsem, self.fsem, self.ssem, self.rsem = vin, vout, land, lsem, fsem, ssem, rsem
        self.n_sub, self.total = n_sub, n_sub * n_arrays
        self.pr = height // 4 // n_sub
        L, z, x = ln.length, ln.z, ln.x
        self.L = L
        self.waves = self.total + 2 * L
        up = 2 * x - 1
        self.k = ((1 - x) * (L - 1 - z) + x * z, x * (L - 1 - z) + (1 - x) * z)
        self.up = ((2 * (z + up) + x, ln.t), (2 * (z - up) + x, ln.t))
        self.down = (self.up[1], self.up[0])
        self.partner = (2 * z + 1 - x, ln.t)
        self.parts = ((2 * x, 2), (2 * (1 - x) + 1, 1), (2 * (1 - x), 1))

    def rows(self, q, job, part=0, n=None):
        first, count = self.parts[job]
        return pl.ds(pl.multiple_of((q * 4 + first + part) * self.pr, 8), (n or count) * self.pr)

    def view(self, ref, q, job, part=0, n=None):
        return ref.at[self.rows(q, job, part, n)]

    def box(self, q, part, n=1):
        return self.land.at[q, pl.ds(part * self.pr, n * self.pr)]

    def landed(self, view, q, kind):
        rcopy(view, view, self.ssem.at[0, 0], self.rsem.at[q, kind], self.ln.sib).wait_recv()

    def ok(self, q):
        return (q >= 0) & (q < self.total)

    def slabs(self, tau):
        return (tau - 1 - self.k[0], tau - 1 - self.k[1], tau)

    def loads(self, tau, job, views):
        par = lax.rem(tau, 2)
        n = self.parts[job][1] * self.pr
        at = pl.ds((0, 2, 3)[job] * self.pr, n)
        return [pltpu.make_async_copy(v, self.vin.at[par, i, at], self.lsem.at[par, job, i]) for i, v in enumerate(views)]

    def prefetch(self, tau):
        for job, q in enumerate(self.slabs(tau)):

            def start(refs):
                for cp in self.loads(tau, job, refs):
                    cp.start()

            @pl.when(self.ok(q))
            def _():
                pair = [self.view(r, q, job) for r in (self.own, self.sibling)]
                if self.head is None:
                    start(pair)
                    return
                pl.when(q < self.n_sub)(lambda: start([r.at[self.rows(q, job)] for r in self.head]))
                pl.when(q >= self.n_sub)(lambda: start(pair))

    def send(self, src, dst, slot, k, q, kind, dev):
        return rcopy(src, dst, self.ssem.at[slot, k], self.rsem.at[q, kind], dev)

    def wave(self, tau, start=True):
        L, pr = self.L, self.pr
        slot = lax.rem(tau, 2)
        q_both, q_one, q_leaf = self.slabs(tau)

        def run(*cps):
            for cp in cps:
                cp.start() if start else cp.wait_send()

        def out(part, n=1):
            return self.vout.at[slot, pl.ds(part * pr, n * pr)]

        def summed(job, q):
            for cp in self.loads(tau, job, [self.view(r, q, job) for r in (self.own, self.sibling)]):
                cp.wait()
            a = (0, 2, 3)[job] * pr
            n = self.parts[job][1] * pr
            return self.vin[slot, 0, a : a + n] + self.vin[slot, 1, a : a + n]

        @pl.when(self.ok(q_leaf))
        def _():
            o = out(3)
            if start:
                o[...] = summed(2, q_leaf)
            run(self.send(o, self.box(q_leaf, 3), slot, 0, q_leaf, 0, self.partner))

        q_met = tau - L - 1
        for i in range(2):
            n, part = (2, 0) if i == 0 else (1, 2)

            @pl.when(self.ok(q_met) & (self.k[i] == L - 1))
            def _():
                tot = out(4 + 2 * i, n)
                if start:
                    a = (part + n - 1) * pr
                    self.landed(self.box(q_met, 4), q_met, 3)
                    if i == 0:
                        tot[0:pr] = self.vout[1 - slot, 0:pr]
                    tot[(n - 1) * pr : n * pr] = self.vout[1 - slot, a : a + pr] + self.land[q_met, 4 * pr : 5 * pr]
                fv = self.view(self.fin, q_met, i)
                run(self.send(tot, fv, slot, 2 if i == 0 else 7, q_met, 4 if i == 0 else 6, self.down[i]))
                if i == 0:
                    run(self.send(out(4), self.view(self.fin, q_met, 0, 0, 1), slot, 3, q_met, 5, self.partner))
                cp = pltpu.make_async_copy(tot, fv, self.fsem.at[i, slot])
                cp.start() if start else cp.wait()

        for i in range(2):
            k = self.k[i]
            r = L - 1 - k
            q = tau - L - 1 - r

            @pl.when(self.ok(q) & (r > 0))
            def _():
                fv = self.view(self.fin, q, i)
                if start:
                    self.landed(fv, q, 4 if i == 0 else 6)

                @pl.when(k > 0)
                def _():
                    run(self.send(fv, fv, slot, 8 if i == 0 else 10, q, 4 if i == 0 else 6, self.down[i]))

                if i == 0:
                    fx = self.view(self.fin, q, 0, 0, 1)
                    run(self.send(fx, fx, slot, 9, q, 5, self.partner))

        for i, q in ((0, q_both), (1, q_one)):
            k = self.k[i]
            n, part = (2, 0) if i == 0 else (1, 2)

            @pl.when(self.ok(q))
            def _():
                o = out(part, n)
                if start:
                    v = summed(i, q)
                    if i == 0:
                        self.landed(self.box(q, 3), q, 0)
                        o[0:pr] = v[0:pr] + self.land[q, 3 * pr : 4 * pr]
                        o[pr : 2 * pr] = v[pr : 2 * pr]
                    else:
                        o[...] = v

                    @pl.when(k > 0)
                    def _():
                        self.landed(self.box(q, part, n), q, 1 + i)
                        o[...] += self.land[q, part * pr : (part + n) * pr]

                @pl.when(k < L - 1)
                def _():
                    run(self.send(o, self.box(q, part, n), slot, 1 if i == 0 else 5, q, 1 + i, self.up[i]))

                @pl.when(k == L - 1)
                def _():
                    run(self.send(out(part + n - 1), self.box(q, 4), slot, 4 if i == 0 else 6, q, 3, self.partner))

    def step(self, tau):
        self.wave(tau - 2, start=False)
        self.wave(tau)

    def steps(self, t0, t1):
        def body(tau, carry):
            self.prefetch(tau + 1)
            self.step(tau)
            return carry

        lax.fori_loop(t0, t1, body, 0)

    def finish(self):
        self.wave(self.waves - 2, start=False)
        self.wave(self.waves - 1, start=False)

        def body(q, carry):
            self.landed(self.view(self.fin, q, 2), q, 5)
            return carry

        lax.fori_loop(0, self.total, body, 0)


N_SUB = 4
PER = N_SUB // 4
P_AHEAD = 8


def backward_kernel(dm, n_dp, *refs):
    (meta, g1_r, g2_r, bd_r, wdn_s, gn_h, gu, p_hbm, i_wqkv, i_wo, i_wup, i_bias, i_tok, i_cot, i_normed, i_q8, i_kk, i_vv, i_mixt, i_n2, i_act, i_gp, i_mid, d_own, d_sib) = refs[:25]
    (fin, sm_out, lo32, gt32, own, sibl, sland) = refs[25:32]
    (wqkv, wo, wup, wdn, cot, mixt, n2, gp, act, mid, gn, dwa, acc, bbuf, small) = refs[32:47]
    psem, tsem, lsem, osem, xss, xrs, sss, srs = refs[47:55]
    red_a = refs[55:62]
    R, D, NS, hw, f = dm.r, dm.d, dm.ns, dm.hw, dm.f
    ln = Links(n_dp)
    y, c, t = ln.y, ln.c, ln.t
    base = c * NS
    nt, ft = D // 256, f // 256

    srcs = (i_gp, i_n2, i_cot, wdn_s, i_act, i_bias, i_mid, i_wup, i_wqkv, i_wo, i_mixt)
    dsts = (gp.at[:, pl.ds(0, 2 * f)], n2, cot, wdn.at[al(t, f)], act, bbuf, mid, wup.at[pl.ds(2 * y, 2)], wqkv, wo, mixt)
    ins = [pltpu.make_async_copy(a, b, lsem.at[i]) for i, (a, b) in enumerate(zip(srcs, dsts))]
    late = [pltpu.make_async_copy(a, gp.at[:, pl.ds(i * D, D)], lsem.at[11 + i]) for i, a in enumerate((i_q8, i_kk, i_vv, i_normed))]
    late.append(pltpu.make_async_copy(i_tok, n2, lsem.at[15]))
    for cp in ins:
        cp.start()
    bar = pltpu.get_barrier_semaphore()
    group = ln.dp - lax.rem(ln.dp, n_dp)
    for dev in (ln.ypart, ln.sib):
        pl.semaphore_signal(bar, inc=1, device_id=dev, device_id_type=MESH)

    def greet(i, carry):
        pl.semaphore_signal(bar, inc=1, device_id=(lax.rem(ln.dp + i, n_dp), t), device_id_type=MESH)
        return carry

    lax.fori_loop(1, n_dp, greet, 0)
    pl.semaphore_wait(bar, 2 + n_dp - 1)
    red = Reduce(ln, (d_own, d_sib), own, sibl, fin, D, 3, N_SUB, *red_a)
    def at(i):
        red.steps(i * PER, (i + 1) * PER)

    def stage(src, ref, r0, k):
        return pltpu.make_async_copy(src, ref.at[pl.ds(r0, D)], tsem.at[k])

    staged = [stage(gn_h.at[ln.t_sib], dwa, 0, 0), stage(gu.at[ln.t_y, pl.ds(hw, D)], dwa, D, 1), stage(gu.at[ln.t_ysib, pl.ds(hw, D)], gn, 0, 2)]
    for cp in staged:
        cp.start()

    def narrow(cp, ref, r0, dst):
        cp.wait()
        for r in range(0, D, 128):
            dst[r : r + 128, :] = ref[r0 + r : r0 + r + 128, :].astype(bf16)

    red.prefetch(0)
    at(0)
    narrow(staged[0], dwa, 0, wdn.at[al(ln.t_sib, f)])
    for cp in ins[:4]:
        cp.wait()
    acc[...] = jnp.zeros_like(acc)

    def grad_hidden(half):
        def one(i):
            s, sh = i // 2, lax.rem(i, 2)
            rs, cs = al(s, R), al(half * 2 + sh, f)
            hf = y if half == 0 else 1 - y
            ga = mmt(cot[rs, :], wdn[al(2 * hf + sh, f), :])
            gp[rs, cs] = (ga * gp[rs, cs].astype(f32)).astype(bf16)

        loop(NS * 2, one)

    grad_hidden(0)
    at(1)
    narrow(staged[1], dwa, D, wup.at[ln.t_y])
    narrow(staged[2], gn, 0, wup.at[ln.t_ysib])

    def dwup(i):
        sh, j = i // nt, lax.rem(i, nt)
        for n in range(ft):
            dwa[pl.ds(pl.multiple_of(i * 256, 256), 256), n * 256 : n * 256 + 256] = tmm(n2[:, al(j, 256)], gp[:, al(sh * ft + n, 256)])

    loop(2 * nt, dwup)
    up_own = pltpu.make_async_copy(dwa.at[al(c, D)], own.at[pl.ds(D, D)], osem.at[2])
    up_own.start()
    up_sib = rcopy(dwa.at[al(1 - c, D)], sibl.at[pl.ds(D, D)], xss.at[0], xrs.at[0], ln.sib)
    up_sib.start()
    ones = jnp.ones((8, dm.rows), bf16)
    for sh in range(2):
        acc[6 + sh, :, :f] = mm(ones, gp[:, sh * f : (sh + 1) * f]) * 0.125

    bd = bd_r[...].reshape(1, D)
    for cp in ins[4:]:
        cp.wait()

    def lo_own(s):
        rs = al(s, R)
        gn[rs, :] = mid[rs, :] + bd + mm(act[rs, :], wdn[al(y, 2 * f), :])

    loop(NS, lo_own)
    at(2)
    up_own.wait()
    up_sib.wait()
    staged = [stage(gn_h.at[ln.t_y], dwa, 0, 0), stage(gn_h.at[ln.t_ysib], dwa, D, 1)]
    for cp in staged:
        cp.start()
    tw = 384 if f % 384 == 0 else 256
    mt = f // tw

    def mlp(i):
        pl.when(i == NS * mt)(lambda: at(3))
        s, j = i // (2 * mt), lax.rem(i, 2 * mt)
        sh = 2 * (1 - y) + j // mt
        rs, cs = al(s, R), al(lax.rem(j, mt), tw)
        h = mm(n2[rs, :], wup[sh, :, cs]) + bbuf[sh, 0:1, cs]
        a, g = gelu_pair(h)
        act[rs, al(j, tw)] = a.astype(bf16)
        gp[rs, al(2 * mt + j, tw)] = g.astype(bf16)

    loop(NS * 2 * mt, mlp)
    at(4)
    narrow(staged[0], dwa, 0, wdn.at[al(ln.t_y, f)])
    narrow(staged[1], dwa, D, wdn.at[al(ln.t_ysib, f)])
    grad_hidden(1)

    def gnorm2(s):
        rs = al(s, R)
        tot = None
        for half in range(2):
            for i in range(2):
                sh = 2 * (y if half == 0 else 1 - y) + i
                k = half * 2 + i
                p = mmt(gp[rs, k * f : (k + 1) * f], wup[sh])
                tot = p if tot is None else tot + p
        lo = gn[rs, :] + mm(act[rs, :], wdn[al(1 - y, 2 * f), :])
        dwa[rs, :] = lo
        gn[rs, :] = tot

    loop(NS, gnorm2)
    at(5)
    total, hp = NS * dm.pairs, dm.pairs // 2

    def place(i):
        j = lax.rem(i, NS * hp)
        half = i // (NS * hp)
        hf = y + half * (1 - 2 * y)
        return j // hp, hf * hp + lax.rem(j, hp)

    def p_slot(i):
        k = lax.rem(i, P_AHEAD)
        return k // 2, pl.ds(pl.multiple_of(lax.rem(k, 2) * dm.rp, 128), dm.rp)

    def p_copy(i):
        s, p = place(i)
        k, cs = p_slot(i)
        return pltpu.make_async_copy(p_hbm.at[s * dm.pairs + p], wup.at[k, pl.ds(0, 2 * R), cs], psem.at[lax.rem(i, P_AHEAD)])

    for i in range(P_AHEAD - 1):
        p_copy(i).start()
    lo_copies = []
    for s in range(NS):
        v = dwa.at[pl.ds(s * R, R)]
        lo_copies.append((pltpu.make_async_copy(v, lo32.at[base + s], osem.at[3 + s]), rcopy(v, lo32.at[base + s], xss.at[1 + s], xrs.at[1 + s], ln.sib)))
        for cp in lo_copies[-1]:
            cp.start()
    for cp in late:
        cp.start()
    q8, kk, vv, normed = (gp.at[:, pl.ds(i * D, D)] for i in range(4))
    tok = n2
    g2 = g2_r[...].reshape(1, D)
    g1 = g1_r[...].reshape(1, D)

    def ln2b(i):
        rs = pl.ds(pl.multiple_of(i * CH, CH), CH)
        xh, r = centred(mid[rs, :])
        go = gn[rs, :]
        co = cot[rs, :].astype(f32)
        g = go * g2
        gx = g * xh
        gm = co + r * (g - jnp.sum(g, -1, keepdims=True) * (1.0 / D) - xh * (jnp.sum(gx, -1, keepdims=True) * (1.0 / D)))
        mid[rs, :] = gm
        gl = gm.astype(bf16)
        act[rs, 0:D] = gl
        acc[0] += fold8(co)
        acc[1] += fold8(gl.astype(f32))
        acc[4] += fold8(go * xh)
        acc[5] += fold8(go)

    loop(dm.rows // CH, ln2b)

    def gmixf(s):
        rs = al(s, R)
        act[rs, D : 2 * D] = mmt(act[rs, 0:D], wo[...]).astype(bf16)

    loop(NS, gmixf)
    at(6)
    own_h = al(y, 2 * hw)

    def over_samples(fn):
        tot = None
        for s in range(NS):
            p = fn(s)
            tot = p if tot is None else tot + p
        return tot

    for a, b in lo_copies:
        a.wait()
        b.wait()

    for n in range(nt):
        cc = slice(n * 256, n * 256 + 256)
        p = over_samples(lambda s: mm(mixt[s, own_h, :], act[s * R : s * R + R, cc]))
        for sh in range(2):
            dwa[sh * D + 3 * hw : sh * D + 4 * hw, cc] = p[sh * hw : (sh + 1) * hw]
    for cp in late:
        cp.wait()
    lane = lax.broadcasted_iota(jnp.int32, (1, 128), 1)
    masks = (lane < HEAD_DIM, lane >= HEAD_DIM)
    def attn(i):
        s, p = place(i)
        rs, cs = al(s, R), al(p, 128)
        slab, pc = p_slot(i)

        @pl.when(i + P_AHEAD - 1 < total)
        def _():
            p_copy(i + P_AHEAD - 1).start()

        p_copy(i).wait()
        q, k, v, do = q8[rs, cs], kk[rs, cs], vv[rs, cs], act[rs, pl.ds(pl.multiple_of(D + p * 128, 128), 128)]
        dv, dk = [], []
        for h in range(2):
            pt = wup[slab, h * R : (h + 1) * R, pc][:, :R]
            pf = pt.astype(f32)
            dp = mmt(jnp.where(masks[h], v, jnp.bfloat16(0)), do)
            dsum = jnp.sum(pf * dp, 0, keepdims=True)
            ds = (pf * (dp - dsum)).astype(bf16)
            dv.append(mm(pt, do))
            dk.append(mm(ds, q))
            o = tmm(k, ds)
            hr = pl.ds(pl.multiple_of(p * 128 + h * HEAD_DIM, HEAD_DIM), HEAD_DIM)
            mixt[s, hr, :] = (o[h * HEAD_DIM : (h + 1) * HEAD_DIM] * 0.125).astype(bf16)
        kk[rs, cs] = jnp.where(masks[0], dk[0], dk[1]).astype(bf16)
        vv[rs, cs] = jnp.where(masks[0], dv[0], dv[1]).astype(bf16)

    def attend(i0, i1, between):
        def one(i, carry):
            attn(i)
            for k, fn in between:
                pl.when(i == k)(fn)
            return carry

        lax.fori_loop(i0, i1, one, 0)

    half = NS * hp

    def seventh():
        red.steps(7 * PER, 8 * PER - 1)
        red.step(8 * PER - 1)

    attend(0, half, [(half // 2, seventh)])
    for n in range(nt):
        cc = slice(n * 256, n * 256 + 256)
        p = over_samples(lambda s: mm(mixt[s, own_h, :], normed[s * R : s * R + R, cc]))
        tk = tmm(kk[:, own_h], normed[:, cc])
        tv = tmm(vv[:, own_h], normed[:, cc])
        for sh in range(2):
            h = slice(sh * hw, (sh + 1) * hw)
            dwa[sh * D : sh * D + hw, cc] = p[h]
            dwa[sh * D + hw : sh * D + 2 * hw, cc] = tk[h]
            dwa[sh * D + 2 * hw : sh * D + 3 * hw, cc] = tv[h]
    a_own = pltpu.make_async_copy(dwa.at[al(c, D)], own.at[pl.ds(2 * D, D)], osem.at[2])
    a_own.start()
    a_sib = rcopy(dwa.at[al(1 - c, D)], sibl.at[pl.ds(2 * D, D)], xss.at[5], xrs.at[5], ln.sib)
    a_sib.start()
    onesr = jnp.ones((8, R), bf16)
    acc[8, :, 0 : 2 * hw] = over_samples(lambda s: mmt(onesr, mixt[s, own_h, :])) * 0.125
    acc[9, :, 0 : 2 * hw] = mm(ones, vv[:, own_h]) * 0.125
    third3 = NS * hp // 3
    attend(half, half + third3, [])
    a_own.wait()
    a_sib.wait()
    red.prefetch(8 * PER)
    at(8)
    attend(half + third3, total, [(half + 2 * third3, lambda: at(9))])
    at(10)

    def gnorm1(s):
        rs = al(s, R)
        gn[rs, :] = tmm(mixt[s], wqkv[0:D, :]) + mm(kk[rs, :], wqkv[D : 2 * D, :]) + mm(vv[rs, :], wqkv[2 * D : 3 * D, :])

    loop(NS, gnorm1)
    at(11)

    def ln1b(s):
        for r0, n in row_chunks(dm):
            rs = pl.ds(pl.multiple_of(s * R + r0, 16), n)
            x = tok[rs, :].astype(f32)
            keep = keep_of(meta, base, s, r0, n) if r0 == 0 else None
            xh, r = centred(x if keep is None else x * keep)
            go = gn[rs, :]
            g = go * g1
            gx = g * xh
            gi = r * (g - jnp.sum(g, -1, keepdims=True) * (1.0 / D) - xh * (jnp.sum(gx, -1, keepdims=True) * (1.0 / D)))
            o = mid[rs, :] + gi
            mid[rs, :] = o if keep is None else o * keep
            acc[2] += fold8(go * xh)
            acc[3] += fold8(go)

    loop(NS, ln1b)
    gt_copies = []
    for s in range(NS):
        v = mid.at[pl.ds(s * R, R)]
        gt_copies.append((pltpu.make_async_copy(v, gt32.at[base + s], osem.at[3 + s]), rcopy(v, gt32.at[base + s], xss.at[6 + s], xrs.at[6 + s], ln.sib)))
        for cp in gt_copies[-1]:
            cp.start()

    tot = jnp.sum(acc[...], 1)
    for sh in range(2):
        small[sh, 0:6, :] = tot[0:6]
        small[sh, 6:7, :] = tot[6 + sh : 7 + sh]
        small[sh, 7:8, 0:hw] = tot[8:9, sh * hw : (sh + 1) * hw]
        small[sh, 7:8, hw : 2 * hw] = tot[9:10, sh * hw : (sh + 1) * hw]
        small[sh, 7:8, 2 * hw :] = jnp.zeros((1, D - 2 * hw), f32)
    cp = rcopy(small.at[1 - c], small.at[2], xss.at[10], xrs.at[10], ln.sib)
    cp.start()
    cp.wait()
    small[2] = small[c] + small[2]
    mine = sland.at[al(ln.dp, 8)]
    kept = pltpu.make_async_copy(small.at[2], mine, osem.at[0])
    kept.start()

    def peer(i):
        d = lax.rem(ln.dp + i, n_dp)
        return rcopy(small.at[2], mine, sss.at[d], srs.at[ln.dp], (d, t))

    def spread(i, carry):
        peer(i).start()
        return carry

    lax.fori_loop(1, n_dp, spread, 0)

    red.steps(12 * PER, red.waves)
    red.finish()

    def gathered(i, carry):
        peer(i).wait_send()
        d = lax.rem(ln.dp + i, n_dp)
        theirs = sland.at[al(d, 8)]
        rcopy(theirs, theirs, sss.at[d], srs.at[d], (d, t)).wait_recv()
        return carry

    lax.fori_loop(1, n_dp, gathered, 0)
    kept.wait()
    back = pltpu.make_async_copy(sland, dwa.at[pl.ds(0, 8 * n_dp)], osem.at[0])
    back.start()
    back.wait()
    sm_out[...] = lax.fori_loop(1, n_dp, lambda i, v: v + dwa[al(i, 8), :], dwa[0:8, :])
    for a, b in gt_copies:
        a.wait()
        b.wait()


def backward_call(dm, n_dp, small, big):
    M, D, f = dm.rows, dm.d, dm.f
    sds, vm, dma = jax.ShapeDtypeStruct, pltpu.VMEM, pltpu.SemaphoreType.DMA
    st = sds((3 * D, D), f32)
    outs = [st, sds((8, D), f32), sds((dm.samples, dm.r, D), f32), sds((dm.samples, dm.r, D), f32), st, st, sds((8 * n_dp, D), f32)]
    row, wide = vm((M, D), bf16), vm((M, 2 * f), bf16)
    scratch = [vm((3 * D, D), bf16), vm((D, D), bf16), vm((dm.n_t, D, f), bf16), vm((dm.ff, D), bf16), row]
    scratch += [vm((dm.ns, D, dm.r), bf16), row, vm((M, dm.ff), bf16), wide, vm((M, D), f32), vm((M, D), f32), vm((2 * D, D), f32), vm((10, 8, D), f32)]
    scratch += [vm((dm.n_t, 16, D), f32), vm((3, 8, D), f32)]
    scratch += [dma((P_AHEAD,)), dma((3,)), dma((16,)), dma((7,)), dma((11,)), dma((11,)), dma((n_dp,)), dma((n_dp,))]
    scratch += Reduce.scratch(3, N_SUB, D, D)

    def kern(*refs):
        backward_kernel(dm, n_dp, *refs)

    return pl.pallas_call(
        kern,
        out_shape=outs,
        in_specs=[SM] + [V] * (len(small) - 1) + [ANY] * len(big),
        out_specs=[ANY, V] + [ANY] * 5,
        scratch_shapes=scratch,
        compiler_params=pltpu.CompilerParams(vmem_limit_bytes=VMEM_LIMIT, collective_id=2, has_side_effects=True),
        name="backward",
    )(*small, *big)


def shards(tokens, metadata, cotangent, w_query, w_key, w_value, w_out, b_query, b_value, b_out, w_up, b_up, w_down, b_down, gain_one, shift_one, gain_two, shift_two, n_dp, n_t):
    dm = Dims(tokens, w_up, n_t)
    D, hw, f = dm.d, dm.hw, dm.f
    small = (metadata, w_query.T, w_key.T, w_value.T, w_out, w_up, w_down, b_up, b_query, b_value, gain_one, shift_one, gain_two, shift_two, b_out)
    (gu, gnw, _, p, wqkv, wo, wu, bb, tok, cot, normed, q8, kk, vv, mixt, n2, act, gp, mid, d_own, d_sib) = forward_call(dm, n_dp, small, (tokens.transpose(1, 0, 2), cotangent.transpose(1, 0, 2)))
    small = (metadata, gain_one, gain_two, b_down)
    fin, sm, lo, gt, *_ = backward_call(dm, n_dp, small, (w_down, gnw, gu, p, wqkv, wo, wu, bb, tok, cot, normed, q8, kk, vv, mixt, n2, act, gp, mid, d_own, d_sib))
    a_ = fin[2 * D :]
    return (
        lo[:, : dm.length].astype(bf16),
        gt[:, : dm.length],
        a_[0:hw].T,
        a_[hw : 2 * hw].T,
        a_[2 * hw : 3 * hw].T,
        a_[3 * hw : 4 * hw],
        sm[7, :hw],
        sm[7, hw : 2 * hw],
        sm[1],
        fin[D : 2 * D],
        sm[6],
        fin[:D],
        sm[0],
        sm[2],
        sm[3],
        sm[4],
        sm[5],
    )


def solution(mesh):
    n_dp, n_t = mesh.shape["dp"], mesh.shape["tensor"]
    rows, cols, vec, rep = P("dp", None, None), P(None, "tensor"), P("tensor"), P()
    srow = P("tensor", None)

    def run(*args):
        return shards(*args, n_dp=n_dp, n_t=n_t)

    return jax.shard_map(
        run,
        mesh=mesh,
        in_specs=(rows, P("dp"), rows, cols, cols, cols, srow, vec, vec, rep, cols, vec, srow, rep, rep, rep, rep, rep),
        out_specs=(rows, rows, cols, cols, cols, srow, vec, vec, rep, cols, vec, srow, rep, rep, rep, rep, rep),
        check_vma=False,
    )
```

```python
import math

import jax
import jax.numpy as jnp
from jax import lax
from jax.experimental import pallas as pl
from jax.experimental.pallas import tpu as pltpu
from jax.sharding import PartitionSpec as P

HEAD_DIM = 64
EPS = 1e-05
MESH = pl.DeviceIdType.MESH
f32 = jnp.float32
bf16 = jnp.bfloat16
VMEM_LIMIT = 63 << 20
RING = 8
CH = 64
TAIL_P = 0.24
TAIL = (
    0.08952743306829739,
    0.15551359433427508,
    -0.15404885518029288,
    0.6255903019940591,
    -0.6460706945688248,
    0.5545739487327468,
    -0.12508572868970558,
)
INV_SQRT_2PI = 1.0 / math.sqrt(2.0 * math.pi)
HALF_LOG2E = -0.5 / math.log(2.0)


def mm(a, b):
    return lax.dot_general(a, b, (((1,), (0,)), ((), ())), preferred_element_type=f32)


def mmt(a, b):
    return lax.dot_general(a, b, (((1,), (1,)), ((), ())), preferred_element_type=f32)


def tmm(a, b):
    return lax.dot_general(a, b, (((0,), (0,)), ((), ())), preferred_element_type=f32)


def loop(n, fn):
    def body(i, carry):
        fn(i)
        return carry

    lax.fori_loop(0, n, body, 0)


def al(i, step):
    return pl.ds(pl.multiple_of(i * step, step), step)


def centred(x):
    d = x.shape[-1]
    mu = jnp.sum(x, -1, keepdims=True) * (1.0 / d)
    xm = x - mu
    var = jnp.sum(xm * xm, -1, keepdims=True) * (1.0 / d)
    r = lax.rsqrt(var + EPS)
    return xm * r, r


def gelu_pair(v):
    d = 1.0 + TAIL_P * jnp.abs(v)
    t = pltpu.reciprocal(d, approx=True)
    t = t * (2.0 - d * t)
    e = jnp.exp2(HALF_LOG2E * (v * v))
    acc = TAIL[6] * t + TAIL[5]
    for k in range(4, -1, -1):
        acc = acc * t + TAIL[k]
    q = (acc * t) * e
    cdf = jnp.where(v < 0, q, 1.0 - q)
    return v * cdf, cdf + (v * e) * INV_SQRT_2PI


def fold8(x):
    return jnp.sum(x.reshape(x.shape[0] // 8, 8, x.shape[1]), 0)


class Dims:
    def __init__(self, tokens, w_up, n_t):
        self.samples, self.length, self.d = tokens.shape
        self.ns = self.samples // 2
        self.r = -(-self.length // 16) * 16
        self.rp = -(-self.r // 128) * 128
        self.rows = self.ns * self.r
        self.f = w_up.shape[1]
        self.ff = self.f * n_t
        self.n_t = n_t
        self.heads = self.d // HEAD_DIM
        self.pairs = self.heads // 2
        self.hw = self.d // n_t


class Links:
    def __init__(self, n_dp):
        self.n_dp = n_dp
        self.dp = lax.axis_index("dp")
        self.t = lax.axis_index("tensor")
        self.y, self.c = self.t // 2, lax.rem(self.t, 2)
        self.z, self.x = self.dp // 2, lax.rem(self.dp, 2)
        self.length = n_dp // 2
        self.sib = (self.dp, 2 * self.y + 1 - self.c)
        self.ypart = (self.dp, 2 * (1 - self.y) + self.c)
        self.t_sib = 2 * self.y + 1 - self.c
        self.t_y = 2 * (1 - self.y) + self.c
        self.t_ysib = 2 * (1 - self.y) + 1 - self.c
        g = lax.rem(self.dp, RING)
        half = RING // 2
        zz, xx = g // 2, lax.rem(g, 2)
        self.pos = jnp.where(xx == 0, zz, RING - 1 - zz)
        base = self.dp - g

        def at(pos):
            pos = lax.rem(pos + RING, RING)
            local = jnp.where(pos < half, 2 * pos, 2 * (RING - 1 - pos) + 1)
            return (base + local, self.t)

        self.step = 1 - 2 * self.c
        self.ahead, self.behind = at(self.pos + self.step), at(self.pos - self.step)

    def piece(self, offset):
        return lax.rem(self.pos + offset * self.step + RING, RING)


def rcopy(src, dst, ssem, rsem, dev):
    return pltpu.make_async_remote_copy(src_ref=src, dst_ref=dst, send_sem=ssem, recv_sem=rsem, device_id=dev, device_id_type=MESH)


def enter(devs):
    bar = pltpu.get_barrier_semaphore()
    for d in devs:
        pl.semaphore_signal(bar, inc=1, device_id=d, device_id_type=MESH)
    pl.semaphore_wait(bar, len(devs))


class Gather:
    def __init__(self, ln, src, out, direct, ssem, rsem, head=0):
        self.ln, self.src, self.out, self.direct, self.head = ln, src, out, direct, head
        self.ssem, self.rsem = ssem, rsem
        self.passed = self.passed_sib = False
        self.rows = src.shape[0]
        self.piece_rows = (self.rows - direct) // RING

    def at(self, ref, offset):
        return ref.at[pl.ds(pl.multiple_of(self.direct + self.ln.piece(offset) * self.piece_rows, 8), self.piece_rows)]

    def copy(self, src, dst, k, dev):
        return rcopy(src, dst, self.ssem.at[k], self.rsem.at[k], dev)

    def landed(self, view, k):
        rcopy(view, view, self.ssem.at[k], self.rsem.at[k], self.ln.sib).wait_recv()

    def spread_y(self):
        return self.copy(self.at(self.src, 0), self.at(self.out.at[self.ln.t], 0), 0, self.ln.ypart)

    def direct_y(self):
        d = pl.ds(self.head, self.direct - self.head)
        return self.copy(self.src.at[d], self.out.at[self.ln.t].at[d], 1, self.ln.ypart)

    def head_y(self):
        d = pl.ds(0, self.head)
        return self.copy(self.src.at[d], self.out.at[self.ln.t].at[d], 19, self.ln.ypart)

    def head_sib(self):
        v = self.out.at[self.ln.t_y].at[pl.ds(0, self.head)]
        return self.copy(v, v, 20, self.ln.sib)

    def head_landed(self):
        self.landed(self.out.at[self.ln.t_y].at[pl.ds(0, self.head)], 19)
        self.head_sib().start()

    def head_sib_landed(self):
        self.landed(self.out.at[self.ln.t_ysib].at[pl.ds(0, self.head)], 20)

    def whole_sib(self):
        return self.copy(self.src, self.out.at[self.ln.t], 2, self.ln.sib)

    def start_y(self):
        self.spread_y().start()
        self.direct_y().start()

    def start_sib(self):
        self.whole_sib().start()

    def wait_sib(self):
        self.landed(self.out.at[self.ln.t_sib], 2)

    def to_sib(self, offset):
        v = self.at(self.out.at[self.ln.t_y], offset)
        return self.copy(v, v, 11 + 4 + offset, self.ln.sib)

    def direct_sib(self):
        v = self.out.at[self.ln.t_y].at[pl.ds(self.head, self.direct - self.head)]
        return self.copy(v, v, 10, self.ln.sib)

    def ring_ahead(self, s):
        v = self.at(self.out.at[self.ln.t_y], -s)
        return self.copy(v, v, 3 + s, self.ln.ahead)

    def ring_behind(self, s):
        v = self.at(self.out.at[self.ln.t_y], s)
        return self.copy(v, v, 7 + s, self.ln.behind)

    def tick(self, i):
        ln, out = self.ln, self.out.at[self.ln.t_y]
        if i == 0:
            self.landed(self.at(out, 0), 0)
            self.ring_ahead(0).start()
            self.ring_behind(0).start()
            self.to_sib(0).start()
            return
        s = i - 1
        self.landed(self.at(out, -s - 1), 3 + s)
        if s < 3:
            self.ring_ahead(s + 1).start()
            self.landed(self.at(out, s + 1), 7 + s)
            if s < 2:
                self.ring_behind(s + 1).start()
        self.to_sib(-s - 1).start()
        if s < 3:
            self.to_sib(s + 1).start()

    def direct_landed(self):
        if not self.passed:
            self.passed = True
            self.landed(self.out.at[self.ln.t_y].at[pl.ds(self.head, self.direct - self.head)], 1)
            self.direct_sib().start()

    def direct_sib_landed(self):
        if not self.passed_sib:
            self.passed_sib = True
            self.landed(self.out.at[self.ln.t_ysib].at[pl.ds(self.head, self.direct - self.head)], 10)

    def finish(self):
        ln, out = self.ln, self.out.at[self.ln.t_ysib]
        for offset in range(-4, 4):
            v = out.at[pl.ds(pl.multiple_of(self.direct + lax.rem(ln.pos - offset * ln.step + RING, RING) * self.piece_rows, 8), self.piece_rows)]
            self.landed(v, 11 + 4 + offset)
        self.direct_sib_landed()

    def drain(self):
        cps = [self.head_y(), self.head_sib()] if self.head else []
        cps += [self.spread_y(), self.direct_y(), self.whole_sib(), self.direct_sib()]
        cps += [self.ring_ahead(s) for s in range(4)] + [self.ring_behind(s) for s in range(3)]
        cps += [self.to_sib(o) for o in range(-4, 4)]
        for cp in cps:
            cp.wait_send()


GATHER_SEMS = 21


def keep_of(meta, base, s, r0, n):
    rows = lax.broadcasted_iota(jnp.int32, (n, 1), 0) + r0
    return jnp.where(rows == 1, meta[base + s].astype(f32), 1.0)


def row_chunks(dm):
    out, r = [], 0
    while r < dm.r:
        n = min(CH, dm.r - r)
        out.append((r, n))
        r += n
    return out


def forward_kernel(dm, n_dp, *refs):
    (meta, wq, wk, wv, wo_s, wup_s, wdn_s, bup_r, bq_r, bv_r, g1_r, s1_r, g2_r, s2_r, bo_r, tokens, cotan) = refs[:17]
    (gu, gn_h, n32, p_hbm, o_wqkv, o_wo, o_wup, o_bias, o_tok, o_cot, o_normed, o_q8, o_kk, o_vv, o_mixt, o_n2, o_act, o_gp, o_mid, d_own, d_sib) = refs[17:38]
    (tok3, cot3, tok, cot, wqkv, wo, wup, normed, q8, kk, vv, mixt, n2, act, gp, mid, dwd, pbuf, tmp, bbuf, bqv, ga, ustage) = refs[38:61]
    psem, tsem, lsem, osem, ssa, rsa, ssu, rsu, ssn, rsn, ssd, rsd = refs[61:]
    R, D, NS, hw, f = dm.r, dm.d, dm.ns, dm.hw, dm.f
    ln = Links(n_dp)
    y, c, t = ln.y, ln.c, ln.t
    base = c * NS

    def row(ref):
        return ref[...].reshape(1, D)

    loads = [pltpu.make_async_copy(tokens, tok3, lsem.at[0]), pltpu.make_async_copy(cotan, cot3, lsem.at[1])]
    for cp in loads:
        cp.start()
    outs = []

    def put(src, dst):
        cp = pltpu.make_async_copy(src, dst, osem.at[len(outs)])
        cp.start()
        outs.append(cp)

    own_a = mid.at[pl.ds(0, 16 + 3 * hw)]
    mid[0:16, :] = jnp.zeros((16, D), f32)
    mid[0:1, 0:f] = bup_r[...].reshape(1, f)
    mid[1:2, 0:hw] = bq_r[...].reshape(1, hw)
    mid[1:2, hw : 2 * hw] = bv_r[...].reshape(1, hw)
    bbuf[t] = mid[0:16, :]
    for i, w in enumerate((wq, wk, wv)):
        mid[16 + i * hw : 16 + (i + 1) * hw, :] = w[...].astype(f32)
        wqkv[pl.ds(pl.multiple_of(i * D + t * hw, 16), hw), :] = w[...]
    wo[al(t, hw), :] = wo_s[...]
    g_a = Gather(ln, own_a, ga, 16 + hw, ssa, rsa)
    g_u = Gather(ln, ustage, gu, hw + D // 3, ssu, rsu, hw)
    g_n = Gather(ln, n32, gn_h, D // 4, ssn, rsn)
    enter((ln.ypart, ln.sib, ln.ahead, ln.behind))
    g_a.start_y()
    g_a.start_sib()
    ustage[0:hw, :] = wo_s[...].astype(f32)

    def widen(i):
        rs = al(i, 64)
        ustage[pl.ds(pl.multiple_of(hw + i * 64, 64), 64), :] = wup_s[rs, :].astype(f32)
        dwd[1, rs, :] = wdn_s[rs, :].astype(f32)
        wup[c, rs, :] = wup_s[rs, :]

    loop(D // 64, widen)
    put(dwd.at[1], n32)
    g_u.spread_y().start()
    outs[0].wait()
    g_n.spread_y().start()
    g_u.head_y().start()
    g_u.direct_y().start()
    g_n.direct_y().start()
    g_u.start_sib()
    g_n.start_sib()

    for cp in loads:
        cp.wait()
    g1, s1, g2, s2, bo = (row(r) for r in (g1_r, s1_r, g2_r, s2_r, bo_r))
    grp = dm.length // 32
    rest, pad = dm.length - grp * 32, R - grp * 32

    def selection(n_out, n_in):
        r = lax.broadcasted_iota(jnp.int32, (NS * n_out, n_in * 2 * NS), 0)
        col = lax.broadcasted_iota(jnp.int32, (NS * n_out, n_in * 2 * NS), 1)
        hit = (col == lax.rem(r, n_out) * (2 * NS) + base + r // n_out) & (lax.rem(r, n_out) < n_in)
        return jnp.where(hit, 1.0, 0.0).astype(bf16)

    sel = selection(32, 32)

    def regroup(g):
        for src, dst in ((tok3, tok), (cot3, cot)):
            v = src[al(g, 32)].astype(f32).reshape(32 * 2 * NS, D).astype(bf16)
            o = mm(sel, v).astype(bf16)
            for s in range(NS):
                dst[pl.ds(pl.multiple_of(s * R + g * 32, 16), 32), :] = o[s * 32 : (s + 1) * 32]

    loop(grp, regroup)
    if pad:
        sel_end = selection(pad, rest)
        for src, dst in ((tok3, tok), (cot3, cot)):
            v = src[grp * 32 : grp * 32 + rest].astype(f32).reshape(rest * 2 * NS, D).astype(bf16)
            o = mm(sel_end, v).astype(bf16)
            for s in range(NS):
                dst[s * R + grp * 32 : (s + 1) * R, :] = o[s * pad : (s + 1) * pad]
    put(tok, o_tok)
    put(cot, o_cot)

    def ln1(s):
        for r, n in row_chunks(dm):
            rs = pl.ds(pl.multiple_of(s * R + r, 16), n)
            x = tok[rs, :].astype(f32)
            if r == 0:
                x = x * keep_of(meta, base, s, r, n)
            xh, _ = centred(x)
            normed[rs, :] = (xh * g1 + s1).astype(bf16)

    loop(NS, ln1)
    put(normed, o_normed)

    def fetch(src, k):
        cp = pltpu.make_async_copy(src, tmp.at[k], tsem.at[k])
        cp.start()
        return cp

    def take_a(tp):
        bbuf[tp] = ga[tp, 0:16, :]
        for i in range(3):
            wqkv[pl.ds(pl.multiple_of(i * D + tp * hw, 16), hw), :] = ga[tp, 16 + i * hw : 16 + (i + 1) * hw, :].astype(bf16)

    lane = lax.broadcasted_iota(jnp.int32, (1, 128), 1)
    masks = (lane < HEAD_DIM, lane >= HEAD_DIM)
    hp = dm.pairs // 2
    tail = R - 16
    live = lax.broadcasted_iota(jnp.int32, (16, 1), 0) < dm.length - tail

    def project(hf):
        for i in range(2):
            b = bbuf[2 * hf + i]
            bqv[0:1, i * hw : (i + 1) * hw] = b[1:2, 0:hw]
            bqv[1:2, i * hw : (i + 1) * hw] = b[1:2, hw : 2 * hw]
        cs = al(hf, 2 * hw)

        def one(s):
            rs = al(s, R)
            n = normed[rs, :]
            w = [wqkv[pl.ds(pl.multiple_of(i * D + hf * 2 * hw, 128), 2 * hw), :] for i in range(3)]
            q8[rs, cs] = (mmt(n, w[0]) + bqv[0:1, : 2 * hw]).astype(bf16) * jnp.bfloat16(0.125)
            kk[rs, cs] = mmt(n, w[1]).astype(bf16)
            vv[rs, cs] = (mmt(n, w[2]) + bqv[1:2, : 2 * hw]).astype(bf16)

        loop(NS, one)

    def p_copy(hf, i):
        slot = lax.rem(i, 2)
        return pltpu.make_async_copy(pbuf.at[slot], p_hbm.at[(i // hp) * dm.pairs + hf * hp + lax.rem(i, hp)], psem.at[slot])

    def attend(hf, ticks):
        total = NS * hp

        def one(i):
            s, p = i // hp, hf * hp + lax.rem(i, hp)
            slot = lax.rem(i, 2)
            rs, cs = al(s, R), al(p, 128)
            for k, fn in ticks:
                pl.when(i == k)(fn)

            @pl.when(i >= 2)
            def _():
                p_copy(hf, i - 2).wait()

            q, k, v = q8[rs, cs], kk[rs, cs], vv[rs, cs]
            for h in range(2):
                st = mmt(jnp.where(masks[h], k, jnp.bfloat16(0)), q)
                sa = st[:tail]
                sb = jnp.where(live, st[tail:], -1e30)
                m = jnp.maximum(jnp.max(sa, 0, keepdims=True), jnp.max(sb, 0, keepdims=True))
                ea, eb = jnp.exp(sa - m), jnp.exp(sb - m)
                inv = 1.0 / (jnp.sum(ea, 0, keepdims=True) + jnp.sum(eb, 0, keepdims=True))
                pbuf[slot, h * R : h * R + tail, 0:R] = (ea * inv).astype(bf16)
                pbuf[slot, h * R + tail : (h + 1) * R, 0:R] = (eb * inv).astype(bf16)
                o = tmm(v, pbuf[slot, h * R : (h + 1) * R, 0:R])
                hr = pl.ds(pl.multiple_of(p * 128 + h * HEAD_DIM, HEAD_DIM), HEAD_DIM)
                mixt[s, hr, :] = o[h * HEAD_DIM : (h + 1) * HEAD_DIM].astype(bf16)
            p_copy(hf, i).start()

        loop(total, one)
        p_copy(hf, total - 2).wait()
        p_copy(hf, total - 1).wait()

    g_a.wait_sib()
    take_a(ln.t_sib)
    g_a.tick(0)
    project(y)
    g_a.tick(1)
    attend(y, [(3, lambda: g_a.tick(2)), (9, lambda: g_a.tick(3))])
    g_a.tick(4)
    g_a.direct_landed()
    g_a.finish()
    take_a(ln.t_y)
    take_a(ln.t_ysib)
    put(wqkv, o_wqkv)
    put(bbuf, o_bias)
    g_u.tick(0)
    project(1 - y)
    put(q8, o_q8)
    put(kk, o_kk)
    put(vv, o_vv)
    g_n.tick(0)

    def both(i):
        g_u.tick(i)
        g_n.tick(i)

    attend(1 - y, [(9, lambda: both(1))])
    put(mixt, o_mixt)
    g_a.drain()
    g_u.head_landed()
    wo_rows = [fetch(gu.at[tp, pl.ds(0, hw)], i) for i, tp in enumerate((ln.t_y,))]
    g_u.wait_sib()
    wo_rows.append(fetch(gu.at[ln.t_sib, pl.ds(0, hw)], 1))
    g_u.head_sib_landed()
    wo_rows.append(fetch(gu.at[ln.t_ysib, pl.ds(0, hw)], 2))
    for i, tp in enumerate((ln.t_y, ln.t_sib, ln.t_ysib)):
        wo_rows[i].wait()
        wo[al(tp, hw), :] = tmp[i].astype(bf16)
    put(wo, o_wo)
    ups = [fetch(gu.at[ln.t_sib, pl.ds((i + 1) * hw, hw)], i) for i in range(4)]

    def outp(s):
        rs = al(s, R)
        mid[rs, :] = tmm(mixt[s], wo[...])

    loop(NS, outp)

    def ln2(s):
        for r, n in row_chunks(dm):
            rs = pl.ds(pl.multiple_of(s * R + r, 16), n)
            x = tok[rs, :].astype(f32)
            if r == 0:
                x = x * keep_of(meta, base, s, r, n)
            m = x + (mid[rs, :] + bo)
            mid[rs, :] = m
            xh, _ = centred(m)
            n2[rs, :] = (xh * g2 + s2).astype(bf16)

    both(2)
    loop(NS, ln2)
    put(mid, o_mid)
    put(n2, o_n2)
    for i in range(4):
        ups[i].wait()
        wup[1 - c, i * hw : (i + 1) * hw, :] = tmp[i].astype(bf16)
    put(wup, o_wup)
    ft = f // 256
    tw = 384 if f % 384 == 0 else 256
    mt = f // tw

    def mlp(i):
        pl.when(i == NS * 3)(lambda: both(3))
        s, j = i // (2 * mt), lax.rem(i, 2 * mt)
        rs, sh, cs = al(s, R), j // mt, al(lax.rem(j, mt), tw)
        h = mm(n2[rs, :], wup[sh, :, cs]) + bbuf[2 * y + sh, 0:1, cs]
        a, g = gelu_pair(h)
        act[rs, al(j, tw)] = a.astype(bf16)
        gp[rs, al(j, tw)] = g.astype(bf16)

    loop(NS * 2 * mt, mlp)
    put(act, o_act)
    put(gp, o_gp)

    def dwdn(sh):
        def one(j):
            dwd[sh, al(j, 256), :] = tmm(act[:, al(sh * ft + j, 256)], cot[...])

        loop(ft, one)

    dwdn(1 - c)
    ex = rcopy(dwd.at[1 - c], d_sib, ssd.at[0], rsd.at[0], ln.sib)
    ex.start()
    both(4)
    dwdn(c)
    put(dwd.at[c], d_own)
    g_u.direct_landed()
    g_u.finish()
    g_n.direct_landed()
    g_n.wait_sib()
    g_n.finish()
    g_u.drain()
    g_n.drain()
    ex.wait()
    for cp in outs[1:]:
        cp.wait()


V = pl.BlockSpec(memory_space=pltpu.VMEM)
ANY = pl.BlockSpec(memory_space=pl.ANY)
SM = pl.BlockSpec(memory_space=pltpu.SMEM)


def forward_call(dm, n_dp, small, big):
    M, D, f = dm.rows, dm.d, dm.f
    sds, vm, dma = jax.ShapeDtypeStruct, pltpu.VMEM, pltpu.SemaphoreType.DMA
    row = sds((M, D), bf16)
    wide = sds((M, 2 * f), bf16)
    sq = sds((D, f), f32)
    outs = [sds((dm.n_t, D + dm.hw, f), f32), sds((dm.n_t, f, D), f32), sds((f, D), f32), sds((dm.ns * dm.pairs, 2 * dm.r, dm.rp), bf16), sds((3 * D, D), bf16), sds((D, D), bf16), sds((2, D, f), bf16), sds((dm.n_t, 16, D), f32)]
    outs += [row] * 6 + [sds((dm.ns, D, dm.r), bf16), row, wide, wide, sds((M, D), f32), sds((f, D), f32), sds((f, D), f32)]
    scratch = [vm((dm.length, 2 * dm.ns, D), bf16)] * 2 + [vm((M, D), bf16)] * 2 + [vm((3 * D, D), bf16), vm((D, D), bf16), vm((2, D, f), bf16)]
    scratch += [vm((M, D), bf16)] * 4 + [vm((dm.ns, D, dm.r), bf16), vm((M, D), bf16), vm((M, 2 * f), bf16), vm((M, 2 * f), bf16), vm((M, D), f32), vm((2, f, D), f32)]
    scratch += [vm((2, 2 * dm.r, dm.rp), bf16), vm((4, dm.hw, D), f32), vm((dm.n_t, 16, D), f32), vm((8, D), f32), vm((dm.n_t, 16 + 3 * dm.hw, D), f32), vm((dm.hw + D, D), f32)]
    scratch += [dma((2,)), dma((4,)), dma((2,)), dma((20,)), *([dma((GATHER_SEMS,))] * 6), dma((1,)), dma((1,))]

    def kern(*refs):
        forward_kernel(dm, n_dp, *refs)

    return pl.pallas_call(
        kern,
        out_shape=outs,
        in_specs=[SM] + [V] * (len(small) - 1) + [ANY] * len(big),
        out_specs=[ANY] * len(outs),
        scratch_shapes=scratch,
        compiler_params=pltpu.CompilerParams(vmem_limit_bytes=VMEM_LIMIT, collective_id=1, has_side_effects=True),
        name="forward",
    )(*small, *big)


class Reduce:
    KINDS = 9

    @staticmethod
    def scratch(n_arrays, n_sub, rows, width):
        pr, nq = rows // 4 // n_sub, n_arrays * n_sub
        vm, dma = pltpu.VMEM, pltpu.SemaphoreType.DMA
        return [vm((2, 2, 4 * pr, width), f32), vm((2, 7 * pr, width), f32), vm((nq, 7 * pr, width), f32), dma((2, 3, 2)), dma((2, 2)), dma((2, 13)), dma((nq, Reduce.KINDS))]

    def __init__(self, ln, head, own, sib, fin, height, n_arrays, n_sub, vin, vout, land, lsem, fsem, ssem, rsem):
        self.ln, self.head, self.own, self.sibling, self.fin = ln, head, own, sib, fin
        self.vin, self.vout, self.land, self.lsem, self.fsem, self.ssem, self.rsem = vin, vout, land, lsem, fsem, ssem, rsem
        self.n_sub, self.total = n_sub, n_sub * n_arrays
        self.pr = height // 4 // n_sub
        L, z, x = ln.length, ln.z, ln.x
        self.L = L
        self.K = L // 2
        self.waves = self.total + 2 * self.K + 2
        rows = (L // 2 - 1 + x, L // 2 - x)
        self.root = [z == r for r in rows]
        self.from_above = [z == r + 1 for r in rows]
        self.dist = [jnp.abs(z - r) for r in rows]
        below = [(z < r).astype(jnp.int32) for r in rows]
        at_root = [(z == r).astype(jnp.int32) for r in rows]
        self.k = [o * self.K + (1 - o) * (b * z + (1 - b) * (L - 1 - z)) for o, b in zip(at_root, below)]
        self.up = [(2 * (z + 2 * b - 1) + x, ln.t) for b in below]
        self.down = [(2 * (z - 2 * b + 1) + x, ln.t) for b in below]
        self.lower, self.higher = (2 * (z - 1) + x, ln.t), (2 * (z + 1) + x, ln.t)
        self.has_lower, self.has_higher = z > 0, z < L - 1
        self.partner = (2 * z + 1 - x, ln.t)
        self.parts = ((2 * x, 2), (2 * (1 - x) + 1, 1), (2 * (1 - x), 1))

    def rows(self, q, job, part=0, n=None):
        first, count = self.parts[job]
        return pl.ds(pl.multiple_of((q * 4 + first + part) * self.pr, 8), (n or count) * self.pr)

    def view(self, ref, q, job, part=0, n=None):
        return ref.at[self.rows(q, job, part, n)]

    def box(self, q, part, n=1):
        return self.land.at[q, pl.ds(part * self.pr, n * self.pr)]

    def landed(self, view, q, kind):
        rcopy(view, view, self.ssem.at[0, 0], self.rsem.at[q, kind], self.ln.sib).wait_recv()

    def ok(self, q):
        return (q >= 0) & (q < self.total)

    def slabs(self, tau):
        return (tau - 1 - self.k[0], tau - 1 - self.k[1], tau)

    def loads(self, tau, job, views):
        par = lax.rem(tau, 2)
        n = self.parts[job][1] * self.pr
        at = pl.ds((0, 2, 3)[job] * self.pr, n)
        return [pltpu.make_async_copy(v, self.vin.at[par, i, at], self.lsem.at[par, job, i]) for i, v in enumerate(views)]

    def prefetch(self, tau):
        for job, q in enumerate(self.slabs(tau)):

            def start(refs):
                for cp in self.loads(tau, job, refs):
                    cp.start()

            @pl.when(self.ok(q))
            def _():
                pair = [self.view(r, q, job) for r in (self.own, self.sibling)]
                if self.head is None:
                    start(pair)
                    return
                pl.when(q < self.n_sub)(lambda: start([r.at[self.rows(q, job)] for r in self.head]))
                pl.when(q >= self.n_sub)(lambda: start(pair))

    def send(self, src, dst, slot, k, q, kind, dev):
        return rcopy(src, dst, self.ssem.at[slot, k], self.rsem.at[q, kind], dev)

    def wave(self, tau, start=True):
        L, pr = self.L, self.pr
        slot = lax.rem(tau, 2)
        q_both, q_one, q_leaf = self.slabs(tau)

        def run(*cps):
            for cp in cps:
                cp.start() if start else cp.wait_send()

        def out(part, n=1):
            return self.vout.at[slot, pl.ds(part * pr, n * pr)]

        def summed(job, q):
            for cp in self.loads(tau, job, [self.view(r, q, job) for r in (self.own, self.sibling)]):
                cp.wait()
            a = (0, 2, 3)[job] * pr
            n = self.parts[job][1] * pr
            return self.vin[slot, 0, a : a + n] + self.vin[slot, 1, a : a + n]

        @pl.when(self.ok(q_leaf))
        def _():
            o = out(3)
            if start:
                o[...] = summed(2, q_leaf)
            run(self.send(o, self.box(q_leaf, 3), slot, 0, q_leaf, 0, self.partner))

        q_met = tau - self.K - 2
        for i in range(2):
            n, part = (2, 0) if i == 0 else (1, 2)

            @pl.when(self.ok(q_met) & self.root[i])
            def _():
                tot = out(4 + 2 * i, n)
                if start:
                    a = (part + n - 1) * pr
                    self.landed(self.box(q_met, 4), q_met, 3)
                    if i == 0:
                        tot[0:pr] = self.vout[1 - slot, 0:pr]
                    tot[(n - 1) * pr : n * pr] = self.vout[1 - slot, a : a + pr] + self.land[q_met, 4 * pr : 5 * pr]
                fv = self.view(self.fin, q_met, i)
                pl.when(self.has_lower)(lambda: run(self.send(tot, fv, slot, 2 if i == 0 else 7, q_met, 4 if i == 0 else 6, self.lower)))
                pl.when(self.has_higher)(lambda: run(self.send(tot, fv, slot, 11 + i, q_met, 4 if i == 0 else 6, self.higher)))
                if i == 0:
                    run(self.send(out(4), self.view(self.fin, q_met, 0, 0, 1), slot, 3, q_met, 5, self.partner))
                cp = pltpu.make_async_copy(tot, fv, self.fsem.at[i, slot])
                cp.start() if start else cp.wait()

        for i in range(2):
            k = self.k[i]
            q = tau - self.K - 2 - self.dist[i]

            @pl.when(self.ok(q) & ~self.root[i])
            def _():
                fv = self.view(self.fin, q, i)
                if start:
                    self.landed(fv, q, 4 if i == 0 else 6)

                @pl.when(k > 0)
                def _():
                    run(self.send(fv, fv, slot, 8 if i == 0 else 10, q, 4 if i == 0 else 6, self.down[i]))

                if i == 0:
                    fx = self.view(self.fin, q, 0, 0, 1)
                    run(self.send(fx, fx, slot, 9, q, 5, self.partner))

        for i, q in ((0, q_both), (1, q_one)):
            k = self.k[i]
            n, part = (2, 0) if i == 0 else (1, 2)

            @pl.when(self.ok(q))
            def _():
                o = out(part, n)
                if start:
                    v = summed(i, q)
                    if i == 0:
                        self.landed(self.box(q, 3), q, 0)
                        o[0:pr] = v[0:pr] + self.land[q, 3 * pr : 4 * pr]
                        o[pr : 2 * pr] = v[pr : 2 * pr]
                    else:
                        o[...] = v

                    root = self.root[i]

                    @pl.when((~root & (k > 0)) | (root & self.has_lower))
                    def _():
                        self.landed(self.box(q, part, n), q, 1 + i)
                        o[...] += self.land[q, part * pr : (part + n) * pr]

                    @pl.when(root & self.has_higher)
                    def _():
                        self.landed(self.box(q, 5, n), q, 7 + i)
                        o[...] += self.land[q, 5 * pr : (5 + n) * pr]

                up = 1 if i == 0 else 5
                pl.when(~self.root[i] & ~self.from_above[i])(lambda: run(self.send(o, self.box(q, part, n), slot, up, q, 1 + i, self.up[i])))
                pl.when(self.from_above[i])(lambda: run(self.send(o, self.box(q, 5, n), slot, up, q, 7 + i, self.up[i])))

                @pl.when(self.root[i])
                def _():
                    run(self.send(out(part + n - 1), self.box(q, 4), slot, 4 if i == 0 else 6, q, 3, self.partner))

    def step(self, tau):
        self.wave(tau - 2, start=False)
        self.wave(tau)

    def steps(self, t0, t1):
        def body(tau, carry):
            self.prefetch(tau + 1)
            self.step(tau)
            return carry

        lax.fori_loop(t0, t1, body, 0)

    def finish(self):
        self.wave(self.waves - 2, start=False)
        self.wave(self.waves - 1, start=False)

        def body(q, carry):
            self.landed(self.view(self.fin, q, 2), q, 5)
            return carry

        lax.fori_loop(0, self.total, body, 0)


N_SUB = 4
PER = N_SUB // 4
P_AHEAD = 8


def backward_kernel(dm, n_dp, *refs):
    (meta, g1_r, g2_r, bd_r, wdn_s, gn_h, gu, p_hbm, i_wqkv, i_wo, i_wup, i_bias, i_tok, i_cot, i_normed, i_q8, i_kk, i_vv, i_mixt, i_n2, i_act, i_gp, i_mid, d_own, d_sib) = refs[:25]
    (fin, sm_out, lo32, gt32, own, sibl, sland) = refs[25:32]
    (wqkv, wo, wup, wdn, cot, mixt, n2, gp, act, mid, gn, dwa, acc, bbuf, small) = refs[32:47]
    psem, tsem, lsem, osem, xss, xrs, sss, srs = refs[47:55]
    red_a = refs[55:62]
    R, D, NS, hw, f = dm.r, dm.d, dm.ns, dm.hw, dm.f
    ln = Links(n_dp)
    y, c, t = ln.y, ln.c, ln.t
    base = c * NS
    nt, ft = D // 256, f // 256

    srcs = (i_gp, i_n2, i_cot, wdn_s, i_act, i_bias, i_mid, i_wup, i_wqkv, i_wo, i_mixt)
    dsts = (gp.at[:, pl.ds(0, 2 * f)], n2, cot, wdn.at[al(t, f)], act, bbuf, mid, wup.at[pl.ds(2 * y, 2)], wqkv, wo, mixt)
    ins = [pltpu.make_async_copy(a, b, lsem.at[i]) for i, (a, b) in enumerate(zip(srcs, dsts))]
    late = [pltpu.make_async_copy(a, gp.at[:, pl.ds(i * D, D)], lsem.at[11 + i]) for i, a in enumerate((i_q8, i_kk, i_vv, i_normed))]
    late.append(pltpu.make_async_copy(i_tok, n2, lsem.at[15]))
    for cp in ins:
        cp.start()
    bar = pltpu.get_barrier_semaphore()
    group = ln.dp - lax.rem(ln.dp, n_dp)
    for dev in (ln.ypart, ln.sib):
        pl.semaphore_signal(bar, inc=1, device_id=dev, device_id_type=MESH)

    def greet(i, carry):
        pl.semaphore_signal(bar, inc=1, device_id=(lax.rem(ln.dp + i, n_dp), t), device_id_type=MESH)
        return carry

    lax.fori_loop(1, n_dp, greet, 0)
    pl.semaphore_wait(bar, 2 + n_dp - 1)
    red = Reduce(ln, (d_own, d_sib), own, sibl, fin, D, 3, N_SUB, *red_a)
    def at(i):
        red.steps(i * PER, (i + 1) * PER)

    def stage(src, ref, r0, k):
        return pltpu.make_async_copy(src, ref.at[pl.ds(r0, D)], tsem.at[k])

    staged = [stage(gn_h.at[ln.t_sib], dwa, 0, 0), stage(gu.at[ln.t_y, pl.ds(hw, D)], dwa, D, 1), stage(gu.at[ln.t_ysib, pl.ds(hw, D)], gn, 0, 2)]
    for cp in staged:
        cp.start()

    def narrow(cp, ref, r0, dst):
        cp.wait()
        for r in range(0, D, 128):
            dst[r : r + 128, :] = ref[r0 + r : r0 + r + 128, :].astype(bf16)

    red.prefetch(0)
    at(0)
    narrow(staged[0], dwa, 0, wdn.at[al(ln.t_sib, f)])
    for cp in ins[:4]:
        cp.wait()
    acc[...] = jnp.zeros_like(acc)

    def grad_hidden(half):
        def one(i):
            s, sh = i // 2, lax.rem(i, 2)
            rs, cs = al(s, R), al(half * 2 + sh, f)
            hf = y if half == 0 else 1 - y
            ga = mmt(cot[rs, :], wdn[al(2 * hf + sh, f), :])
            gp[rs, cs] = (ga * gp[rs, cs].astype(f32)).astype(bf16)

        loop(NS * 2, one)

    grad_hidden(0)
    at(1)
    narrow(staged[1], dwa, D, wup.at[ln.t_y])
    narrow(staged[2], gn, 0, wup.at[ln.t_ysib])

    def dwup(i):
        sh, j = i // nt, lax.rem(i, nt)
        for n in range(ft):
            dwa[pl.ds(pl.multiple_of(i * 256, 256), 256), n * 256 : n * 256 + 256] = tmm(n2[:, al(j, 256)], gp[:, al(sh * ft + n, 256)])

    loop(2 * nt, dwup)
    up_own = pltpu.make_async_copy(dwa.at[al(c, D)], own.at[pl.ds(D, D)], osem.at[2])
    up_own.start()
    up_sib = rcopy(dwa.at[al(1 - c, D)], sibl.at[pl.ds(D, D)], xss.at[0], xrs.at[0], ln.sib)
    up_sib.start()
    ones = jnp.ones((8, dm.rows), bf16)
    for sh in range(2):
        acc[6 + sh, :, :f] = mm(ones, gp[:, sh * f : (sh + 1) * f]) * 0.125

    bd = bd_r[...].reshape(1, D)
    for cp in ins[4:]:
        cp.wait()

    def lo_own(s):
        rs = al(s, R)
        gn[rs, :] = mid[rs, :] + bd + mm(act[rs, :], wdn[al(y, 2 * f), :])

    loop(NS, lo_own)
    at(2)
    up_own.wait()
    up_sib.wait()
    staged = [stage(gn_h.at[ln.t_y], dwa, 0, 0), stage(gn_h.at[ln.t_ysib], dwa, D, 1)]
    for cp in staged:
        cp.start()
    tw = 384 if f % 384 == 0 else 256
    mt = f // tw

    def mlp(i):
        pl.when(i == NS * mt)(lambda: at(3))
        s, j = i // (2 * mt), lax.rem(i, 2 * mt)
        sh = 2 * (1 - y) + j // mt
        rs, cs = al(s, R), al(lax.rem(j, mt), tw)
        h = mm(n2[rs, :], wup[sh, :, cs]) + bbuf[sh, 0:1, cs]
        a, g = gelu_pair(h)
        act[rs, al(j, tw)] = a.astype(bf16)
        gp[rs, al(2 * mt + j, tw)] = g.astype(bf16)

    loop(NS * 2 * mt, mlp)
    at(4)
    narrow(staged[0], dwa, 0, wdn.at[al(ln.t_y, f)])
    narrow(staged[1], dwa, D, wdn.at[al(ln.t_ysib, f)])
    grad_hidden(1)

    def gnorm2(s):
        rs = al(s, R)
        tot = None
        for half in range(2):
            for i in range(2):
                sh = 2 * (y if half == 0 else 1 - y) + i
                k = half * 2 + i
                p = mmt(gp[rs, k * f : (k + 1) * f], wup[sh])
                tot = p if tot is None else tot + p
        lo = gn[rs, :] + mm(act[rs, :], wdn[al(1 - y, 2 * f), :])
        dwa[rs, :] = lo
        gn[rs, :] = tot

    loop(NS, gnorm2)
    at(5)
    total, hp = NS * dm.pairs, dm.pairs // 2

    def place(i):
        j = lax.rem(i, NS * hp)
        half = i // (NS * hp)
        hf = y + half * (1 - 2 * y)
        return j // hp, hf * hp + lax.rem(j, hp)

    def p_slot(i):
        k = lax.rem(i, P_AHEAD)
        return k // 2, pl.ds(pl.multiple_of(lax.rem(k, 2) * dm.rp, 128), dm.rp)

    def p_copy(i):
        s, p = place(i)
        k, cs = p_slot(i)
        return pltpu.make_async_copy(p_hbm.at[s * dm.pairs + p], wup.at[k, pl.ds(0, 2 * R), cs], psem.at[lax.rem(i, P_AHEAD)])

    for i in range(P_AHEAD - 1):
        p_copy(i).start()
    lo_copies = []
    for s in range(NS):
        v = dwa.at[pl.ds(s * R, R)]
        lo_copies.append((pltpu.make_async_copy(v, lo32.at[base + s], osem.at[3 + s]), rcopy(v, lo32.at[base + s], xss.at[1 + s], xrs.at[1 + s], ln.sib)))
        for cp in lo_copies[-1]:
            cp.start()
    for cp in late:
        cp.start()
    q8, kk, vv, normed = (gp.at[:, pl.ds(i * D, D)] for i in range(4))
    tok = n2
    g2 = g2_r[...].reshape(1, D)
    g1 = g1_r[...].reshape(1, D)

    def ln2b(i):
        rs = pl.ds(pl.multiple_of(i * CH, CH), CH)
        xh, r = centred(mid[rs, :])
        go = gn[rs, :]
        co = cot[rs, :].astype(f32)
        g = go * g2
        gx = g * xh
        gm = co + r * (g - jnp.sum(g, -1, keepdims=True) * (1.0 / D) - xh * (jnp.sum(gx, -1, keepdims=True) * (1.0 / D)))
        mid[rs, :] = gm
        gl = gm.astype(bf16)
        act[rs, 0:D] = gl
        acc[0] += fold8(co)
        acc[1] += fold8(gl.astype(f32))
        acc[4] += fold8(go * xh)
        acc[5] += fold8(go)

    loop(dm.rows // CH, ln2b)

    def gmixf(s):
        rs = al(s, R)
        act[rs, D : 2 * D] = mmt(act[rs, 0:D], wo[...]).astype(bf16)

    loop(NS, gmixf)
    own_h = al(y, 2 * hw)

    def over_samples(fn):
        tot = None
        for s in range(NS):
            p = fn(s)
            tot = p if tot is None else tot + p
        return tot

    for a, b in lo_copies:
        a.wait()
        b.wait()

    for n in range(nt):
        cc = slice(n * 256, n * 256 + 256)
        p = over_samples(lambda s: mm(mixt[s, own_h, :], act[s * R : s * R + R, cc]))
        for sh in range(2):
            dwa[sh * D + 3 * hw : sh * D + 4 * hw, cc] = p[sh * hw : (sh + 1) * hw]
    for cp in late:
        cp.wait()
    lane = lax.broadcasted_iota(jnp.int32, (1, 128), 1)
    masks = (lane < HEAD_DIM, lane >= HEAD_DIM)
    def attn(i):
        s, p = place(i)
        rs, cs = al(s, R), al(p, 128)
        slab, pc = p_slot(i)

        @pl.when(i + P_AHEAD - 1 < total)
        def _():
            p_copy(i + P_AHEAD - 1).start()

        p_copy(i).wait()
        q, k, v, do = q8[rs, cs], kk[rs, cs], vv[rs, cs], act[rs, pl.ds(pl.multiple_of(D + p * 128, 128), 128)]
        dv, dk = [], []
        for h in range(2):
            pt = wup[slab, h * R : (h + 1) * R, pc][:, :R]
            pf = pt.astype(f32)
            dp = mmt(jnp.where(masks[h], v, jnp.bfloat16(0)), do)
            dsum = jnp.sum(pf * dp, 0, keepdims=True)
            ds = (pf * (dp - dsum)).astype(bf16)
            dv.append(mm(pt, do))
            dk.append(mm(ds, q))
            o = tmm(k, ds)
            hr = pl.ds(pl.multiple_of(p * 128 + h * HEAD_DIM, HEAD_DIM), HEAD_DIM)
            mixt[s, hr, :] = (o[h * HEAD_DIM : (h + 1) * HEAD_DIM] * 0.125).astype(bf16)
        kk[rs, cs] = jnp.where(masks[0], dk[0], dk[1]).astype(bf16)
        vv[rs, cs] = jnp.where(masks[0], dv[0], dv[1]).astype(bf16)

    def attend(i0, i1, between):
        def one(i, carry):
            attn(i)
            for k, fn in between:
                pl.when(i == k)(fn)
            return carry

        lax.fori_loop(i0, i1, one, 0)

    half = NS * hp

    def seventh():
        red.steps(7 * PER, 8 * PER - 1)
        red.step(8 * PER - 1)

    attend(0, half, [(half // 2, lambda: at(6))])
    for n in range(nt):
        cc = slice(n * 256, n * 256 + 256)
        p = over_samples(lambda s: mm(mixt[s, own_h, :], normed[s * R : s * R + R, cc]))
        tk = tmm(kk[:, own_h], normed[:, cc])
        tv = tmm(vv[:, own_h], normed[:, cc])
        for sh in range(2):
            h = slice(sh * hw, (sh + 1) * hw)
            dwa[sh * D : sh * D + hw, cc] = p[h]
            dwa[sh * D + hw : sh * D + 2 * hw, cc] = tk[h]
            dwa[sh * D + 2 * hw : sh * D + 3 * hw, cc] = tv[h]
    a_own = pltpu.make_async_copy(dwa.at[al(c, D)], own.at[pl.ds(2 * D, D)], osem.at[2])
    a_own.start()
    a_sib = rcopy(dwa.at[al(1 - c, D)], sibl.at[pl.ds(2 * D, D)], xss.at[5], xrs.at[5], ln.sib)
    a_sib.start()
    seventh()
    onesr = jnp.ones((8, R), bf16)
    acc[8, :, 0 : 2 * hw] = over_samples(lambda s: mmt(onesr, mixt[s, own_h, :])) * 0.125
    acc[9, :, 0 : 2 * hw] = mm(ones, vv[:, own_h]) * 0.125
    third3 = NS * hp // 3
    attend(half, half + third3, [])
    a_own.wait()
    a_sib.wait()
    red.prefetch(8 * PER)
    at(8)
    attend(half + third3, total, [(half + 2 * third3, lambda: at(9))])
    at(10)

    def gnorm1(s):
        rs = al(s, R)
        gn[rs, :] = tmm(mixt[s], wqkv[0:D, :]) + mm(kk[rs, :], wqkv[D : 2 * D, :]) + mm(vv[rs, :], wqkv[2 * D : 3 * D, :])

    loop(NS, gnorm1)
    at(11)

    def ln1b(s):
        for r0, n in row_chunks(dm):
            rs = pl.ds(pl.multiple_of(s * R + r0, 16), n)
            x = tok[rs, :].astype(f32)
            keep = keep_of(meta, base, s, r0, n) if r0 == 0 else None
            xh, r = centred(x if keep is None else x * keep)
            go = gn[rs, :]
            g = go * g1
            gx = g * xh
            gi = r * (g - jnp.sum(g, -1, keepdims=True) * (1.0 / D) - xh * (jnp.sum(gx, -1, keepdims=True) * (1.0 / D)))
            o = mid[rs, :] + gi
            mid[rs, :] = o if keep is None else o * keep
            acc[2] += fold8(go * xh)
            acc[3] += fold8(go)

    loop(NS, ln1b)
    gt_copies = []
    for s in range(NS):
        v = mid.at[pl.ds(s * R, R)]
        gt_copies.append((pltpu.make_async_copy(v, gt32.at[base + s], osem.at[3 + s]), rcopy(v, gt32.at[base + s], xss.at[6 + s], xrs.at[6 + s], ln.sib)))
        for cp in gt_copies[-1]:
            cp.start()

    tot = jnp.sum(acc[...], 1)
    for sh in range(2):
        small[sh, 0:6, :] = tot[0:6]
        small[sh, 6:7, :] = tot[6 + sh : 7 + sh]
        small[sh, 7:8, 0:hw] = tot[8:9, sh * hw : (sh + 1) * hw]
        small[sh, 7:8, hw : 2 * hw] = tot[9:10, sh * hw : (sh + 1) * hw]
        small[sh, 7:8, 2 * hw :] = jnp.zeros((1, D - 2 * hw), f32)
    cp = rcopy(small.at[1 - c], small.at[2], xss.at[10], xrs.at[10], ln.sib)
    cp.start()
    cp.wait()
    small[2] = small[c] + small[2]
    mine = sland.at[al(ln.dp, 8)]
    kept = pltpu.make_async_copy(small.at[2], mine, osem.at[0])
    kept.start()

    def peer(i):
        d = lax.rem(ln.dp + i, n_dp)
        return rcopy(small.at[2], mine, sss.at[d], srs.at[ln.dp], (d, t))

    def spread(i, carry):
        peer(i).start()
        return carry

    lax.fori_loop(1, n_dp, spread, 0)

    red.steps(12 * PER, red.waves)
    red.finish()

    def gathered(i, carry):
        peer(i).wait_send()
        d = lax.rem(ln.dp + i, n_dp)
        theirs = sland.at[al(d, 8)]
        rcopy(theirs, theirs, sss.at[d], srs.at[d], (d, t)).wait_recv()
        return carry

    lax.fori_loop(1, n_dp, gathered, 0)
    kept.wait()
    back = pltpu.make_async_copy(sland, dwa.at[pl.ds(0, 8 * n_dp)], osem.at[0])
    back.start()
    back.wait()
    sm_out[...] = lax.fori_loop(1, n_dp, lambda i, v: v + dwa[al(i, 8), :], dwa[0:8, :])
    for a, b in gt_copies:
        a.wait()
        b.wait()


def backward_call(dm, n_dp, small, big):
    M, D, f = dm.rows, dm.d, dm.f
    sds, vm, dma = jax.ShapeDtypeStruct, pltpu.VMEM, pltpu.SemaphoreType.DMA
    st = sds((3 * D, D), f32)
    outs = [st, sds((8, D), f32), sds((dm.samples, dm.r, D), f32), sds((dm.samples, dm.r, D), f32), st, st, sds((8 * n_dp, D), f32)]
    row, wide = vm((M, D), bf16), vm((M, 2 * f), bf16)
    scratch = [vm((3 * D, D), bf16), vm((D, D), bf16), vm((dm.n_t, D, f), bf16), vm((dm.ff, D), bf16), row]
    scratch += [vm((dm.ns, D, dm.r), bf16), row, vm((M, dm.ff), bf16), wide, vm((M, D), f32), vm((M, D), f32), vm((2 * D, D), f32), vm((10, 8, D), f32)]
    scratch += [vm((dm.n_t, 16, D), f32), vm((3, 8, D), f32)]
    scratch += [dma((P_AHEAD,)), dma((3,)), dma((16,)), dma((7,)), dma((11,)), dma((11,)), dma((n_dp,)), dma((n_dp,))]
    scratch += Reduce.scratch(3, N_SUB, D, D)

    def kern(*refs):
        backward_kernel(dm, n_dp, *refs)

    return pl.pallas_call(
        kern,
        out_shape=outs,
        in_specs=[SM] + [V] * (len(small) - 1) + [ANY] * len(big),
        out_specs=[ANY, V] + [ANY] * 5,
        scratch_shapes=scratch,
        compiler_params=pltpu.CompilerParams(vmem_limit_bytes=VMEM_LIMIT, collective_id=2, has_side_effects=True),
        name="backward",
    )(*small, *big)


def shards(tokens, metadata, cotangent, w_query, w_key, w_value, w_out, b_query, b_value, b_out, w_up, b_up, w_down, b_down, gain_one, shift_one, gain_two, shift_two, n_dp, n_t):
    dm = Dims(tokens, w_up, n_t)
    D, hw, f = dm.d, dm.hw, dm.f
    small = (metadata, w_query.T, w_key.T, w_value.T, w_out, w_up, w_down, b_up, b_query, b_value, gain_one, shift_one, gain_two, shift_two, b_out)
    (gu, gnw, _, p, wqkv, wo, wu, bb, tok, cot, normed, q8, kk, vv, mixt, n2, act, gp, mid, d_own, d_sib) = forward_call(dm, n_dp, small, (tokens.transpose(1, 0, 2), cotangent.transpose(1, 0, 2)))
    small = (metadata, gain_one, gain_two, b_down)
    fin, sm, lo, gt, *_ = backward_call(dm, n_dp, small, (w_down, gnw, gu, p, wqkv, wo, wu, bb, tok, cot, normed, q8, kk, vv, mixt, n2, act, gp, mid, d_own, d_sib))
    a_ = fin[2 * D :]
    return (
        lo[:, : dm.length].astype(bf16),
        gt[:, : dm.length],
        a_[0:hw].T,
        a_[hw : 2 * hw].T,
        a_[2 * hw : 3 * hw].T,
        a_[3 * hw : 4 * hw],
        sm[7, :hw],
        sm[7, hw : 2 * hw],
        sm[1],
        fin[D : 2 * D],
        sm[6],
        fin[:D],
        sm[0],
        sm[2],
        sm[3],
        sm[4],
        sm[5],
    )


def solution(mesh):
    n_dp, n_t = mesh.shape["dp"], mesh.shape["tensor"]
    rows, cols, vec, rep = P("dp", None, None), P(None, "tensor"), P("tensor"), P()
    srow = P("tensor", None)

    def run(*args):
        return shards(*args, n_dp=n_dp, n_t=n_t)

    return jax.shard_map(
        run,
        mesh=mesh,
        in_specs=(rows, P("dp"), rows, cols, cols, cols, srow, vec, vec, rep, cols, vec, srow, rep, rep, rep, rep, rep),
        out_specs=(rows, rows, cols, cols, cols, srow, vec, vec, rep, cols, vec, srow, rep, rep, rep, rep, rep),
        check_vma=False,
    )
```
